16 devices in a mesh: data: 16 (over z, y, x, core).
Axes of the slice: x: 2, y: 2, z: 2, core: 2. Of those that a mesh axis runs over, the one named last changes fastest.
Arguments:
- x_in: bfloat16 [128, 48, 512], P('data')
- targets: int32 [128, 48], P('data')
- w_lstm: bfloat16 [8, 1024, 2048], replicated
- b_lstm: float32 [8, 2048], replicated
- w_vocab: bfloat16 [512, 32000], replicated
Outputs:
- output 1: float32 [8, 1024, 2048], replicated
- output 2: float32 [8, 2048], replicated
- output 3: float32 [512, 32000], replicated
- output 4: float32 [128, 48, 512], P('data')
All inputs are finite; a program needn't handle non-finite values.
Results may differ from the reference program's by a relative error of at most 0.00726.
Values are sent between devices in bfloat16 or wider.
A program may use at most 1 GiB of HBM per device.

```python
import jax
import jax.numpy as jnp
from jax import lax

LAYERS = 8
HIDDEN = 512
VOCAB_SIZE = 32000
SEQ_LEN = 48
BATCH_DEV = 8
GROUP_SIZE = 16
BATCH = BATCH_DEV * GROUP_SIZE


def setup_inputs(seed: int = 0) -> dict:
    key_list = jax.random.split(jax.random.key(seed), 5)
    x_in = jax.random.normal(key_list[0], (BATCH, SEQ_LEN, HIDDEN), jnp.float32).astype(jnp.bfloat16)
    targets = jax.random.randint(key_list[1], (BATCH, SEQ_LEN), 0, VOCAB_SIZE, jnp.int32)
    w_lstm = jax.random.normal(key_list[2], (LAYERS, 2 * HIDDEN, 4 * HIDDEN), jnp.float32) * (2 * HIDDEN) ** -0.5
    forget_shift = jnp.concatenate([jnp.zeros((HIDDEN,), jnp.float32), jnp.ones((HIDDEN,), jnp.float32), jnp.zeros((2 * HIDDEN,), jnp.float32)])
    b_lstm = 0.5 * jax.random.normal(key_list[3], (LAYERS, 4 * HIDDEN), jnp.float32) + forget_shift
    w_vocab = jax.random.normal(key_list[4], (HIDDEN, VOCAB_SIZE), jnp.float32) * HIDDEN ** -0.5
    return {'x_in': x_in, 'targets': targets, 'w_lstm': w_lstm.astype(jnp.bfloat16), 'b_lstm': b_lstm, 'w_vocab': w_vocab.astype(jnp.bfloat16)}


def lstm_forward(seq_in, w_layer, b_layer):
    seq_len, num_rows, hidden = seq_in.shape
    w_rec = w_layer[hidden:]
    z_in = jnp.dot(seq_in.reshape(seq_len * num_rows, hidden), w_layer[:hidden], preferred_element_type=jnp.float32)
    z_in = z_in.reshape(seq_len, num_rows, 4 * hidden) + b_layer

    def time_step(carry_in, z_step):
        h_low, c_prev = carry_in
        z_all = z_step + jnp.dot(h_low, w_rec, preferred_element_type=jnp.float32)
        gate_i = jax.nn.sigmoid(z_all[:, :hidden])
        gate_f = jax.nn.sigmoid(z_all[:, hidden:2 * hidden])
        gate_g = jnp.tanh(z_all[:, 2 * hidden:3 * hidden])
        gate_o = jax.nn.sigmoid(z_all[:, 3 * hidden:])
        c_new = gate_f * c_prev + gate_i * gate_g
        tanh_c = jnp.tanh(c_new)
        h_new = gate_o * tanh_c
        gate_all = jnp.concatenate([gate_i, gate_f, gate_g, gate_o], axis=-1)
        return (h_new.astype(jnp.bfloat16), c_new), (h_new, h_low, gate_all, c_prev, tanh_c)

    init_state = (jnp.zeros((num_rows, hidden), jnp.bfloat16), jnp.zeros((num_rows, hidden), jnp.float32))
    final_state, stored = lax.scan(time_step, init_state, z_in)
    h_seq, h_prev, gate_seq, c_prev_seq, tanh_seq = stored
    u_seq = jnp.concatenate([seq_in, h_prev], axis=-1)
    next_in = (seq_in.astype(jnp.float32) + h_seq).astype(jnp.bfloat16)
    return next_in, (u_seq, gate_seq, c_prev_seq, tanh_seq)


def lstm_backward(d_out, stored, w_layer):
    u_seq, gate_seq, c_prev_seq, tanh_seq = stored
    seq_len, num_rows, hidden = d_out.shape
    w_rec_t = w_layer[hidden:].T

    def time_step(carry_in, step_in):
        dh_rec, dc_next = carry_in
        d_ext, gate_all, cell_prev, tanh_c = step_in
        gate_i = gate_all[:, :hidden]
        gate_f = gate_all[:, hidden:2 * hidden]
        gate_g = gate_all[:, 2 * hidden:3 * hidden]
        gate_o = gate_all[:, 3 * hidden:]
        grad_h = d_ext + dh_rec
        dc_tot = dc_next + grad_h * gate_o * (1.0 - tanh_c * tanh_c)
        dz_all = jnp.concatenate([
            dc_tot * gate_g * gate_i * (1.0 - gate_i),
            dc_tot * cell_prev * gate_f * (1.0 - gate_f),
            dc_tot * gate_i * (1.0 - gate_g * gate_g),
            grad_h * tanh_c * gate_o * (1.0 - gate_o)], axis=-1)
        dz_low = dz_all.astype(jnp.bfloat16)
        dh_prev = jnp.dot(dz_low, w_rec_t, preferred_element_type=jnp.float32)
        return (dh_prev, dc_tot * gate_f), (dz_low, jnp.sum(dz_all, axis=0))

    init_state = (jnp.zeros((num_rows, hidden), jnp.float32), jnp.zeros((num_rows, hidden), jnp.float32))
    final_state, outs_seq = lax.scan(time_step, init_state, (d_out, gate_seq, c_prev_seq, tanh_seq), reverse=True)
    dz_seq, db_steps = outs_seq
    dz_flat = dz_seq.reshape(seq_len * num_rows, 4 * hidden)
    dw_layer = jnp.dot(u_seq.reshape(seq_len * num_rows, 2 * hidden).T, dz_flat, preferred_element_type=jnp.float32)
    dx_part = jnp.dot(dz_flat, w_layer[:hidden].T, preferred_element_type=jnp.float32)
    d_in = d_out + dx_part.reshape(seq_len, num_rows, hidden)
    return dw_layer, jnp.sum(db_steps, axis=0), d_in


def head_backward(top_in, tgt_seq, w_vocab):
    seq_len, num_rows, hidden = top_in.shape
    top_flat = top_in.reshape(seq_len * num_rows, hidden)
    logits = jnp.dot(top_flat, w_vocab, preferred_element_type=jnp.float32)
    prob_all = jax.nn.softmax(logits, axis=-1)
    is_target = jnp.arange(w_vocab.shape[1])[None, :] == tgt_seq.reshape(-1)[:, None]
    d_logits = jnp.where(is_target, prob_all - 1.0, prob_all).astype(jnp.bfloat16)
    dw_vocab = jnp.dot(top_flat.T, d_logits, preferred_element_type=jnp.float32)
    d_top = jnp.dot(d_logits, w_vocab.T, preferred_element_type=jnp.float32)
    return d_top.reshape(seq_len, num_rows, hidden), dw_vocab


def shard_grads(x_rows, tgt_rows, w_lstm, b_lstm, w_vocab):
    num_layers = w_lstm.shape[0]
    seq_in = jnp.swapaxes(x_rows, 0, 1)
    saved_acts = []
    for layer_idx in range(num_layers):
        seq_in, stored = lstm_forward(seq_in, w_lstm[layer_idx], b_lstm[layer_idx])
        saved_acts.append(stored)
    d_seq, dw_vocab = head_backward(seq_in, jnp.swapaxes(tgt_rows, 0, 1), w_vocab)
    dw_list = []
    db_list = []
    for layer_idx in reversed(range(num_layers)):
        dw_layer, db_layer, d_seq = lstm_backward(d_seq, saved_acts[layer_idx], w_lstm[layer_idx])
        dw_list.insert(0, dw_layer)
        db_list.insert(0, db_layer)
    return jnp.stack(dw_list), jnp.stack(db_list), dw_vocab, jnp.swapaxes(d_seq, 0, 1)


def reference(x_in, targets, w_lstm, b_lstm, w_vocab):
    x_groups = x_in.reshape(GROUP_SIZE, BATCH_DEV, SEQ_LEN, HIDDEN)
    tgt_groups = targets.reshape(GROUP_SIZE, BATCH_DEV, SEQ_LEN)

    def shard_step(totals, group_in):
        dw_part, db_part, dv_part, dx_part = shard_grads(group_in[0], group_in[1], w_lstm, b_lstm, w_vocab)
        return (totals[0] + dw_part, totals[1] + db_part, totals[2] + dv_part), dx_part

    init_totals = (jnp.zeros(w_lstm.shape, jnp.float32), jnp.zeros(b_lstm.shape, jnp.float32), jnp.zeros(w_vocab.shape, jnp.float32))
    totals, dx_groups = lax.scan(shard_step, init_totals, (x_groups, tgt_groups))
    return totals[0], totals[1], totals[2], dx_groups.reshape(BATCH, SEQ_LEN, HIDDEN)
```

```python
import functools

import jax
import jax.numpy as jnp
from jax import lax
from jax.experimental import pallas as pl
from jax.experimental.pallas import tpu as pltpu
from jax.sharding import PartitionSpec as P

T = 48
R = 8
S = 8
Q = S * R
H = 512
HB = 256
G4 = 4 * H
L = 8
V = 32000
LANE = 128
NDEV = 16
F32 = jnp.float32
BF16 = jnp.bfloat16
MESH = pl.DeviceIdType.MESH
MIB = 1024 * 1024
ANY = pl.BlockSpec(memory_space=pl.ANY)
VMEM = pl.BlockSpec(memory_space=pltpu.VMEM)
DMA = pltpu.SemaphoreType.DMA


def dot(a, b):
    return jnp.dot(a, b, preferred_element_type=F32)


def dot_tt(a, b):
    return lax.dot_general(a, b, (((1,), (1,)), ((), ())), preferred_element_type=F32)


def place():
    me = lax.axis_index("data")
    return me // S * S, lax.rem(me, S)


def plane_barrier(base, stage):
    barrier = pltpu.get_barrier_semaphore()
    for i in range(1, S):
        pl.semaphore_signal(barrier, inc=1, device_id=(base + lax.rem(stage + i, S),), device_id_type=MESH)
    pl.semaphore_wait(barrier, S - 1)


def rows_of(v):
    return v.reshape(Q, v.shape[-1])


def groups_of(v):
    return v.reshape(S, R, v.shape[-1])


def fwd_kernel(x_hbm, w_hbm, b_ref, gates_hbm, cp_hbm, hp_hbm, xs_hbm, xl_hbm,
               w, xbuf, xout, z0, z1, q0, q1, c0, c1, h0, h1, wsem, insem, recv, send, lastsem, osem):
    base, stage = place()
    first, last = stage == 0, stage == S - 1
    nxt = base + lax.rem(stage + 1, S)
    plane_barrier(base, stage)

    wcopy = pltpu.make_async_copy(w_hbm.at[stage], w, wsem.at[0])
    wcopy.start()

    def feed(t):
        return pltpu.make_async_remote_copy(x_hbm.at[t], xbuf.at[t, stage], insem, recv.at[t],
                                            device_id=(base,), device_id_type=MESH)

    def step_out(t):
        return pltpu.make_async_remote_copy(xout.at[t], xbuf.at[t], send, recv.at[t], device_id=(nxt,), device_id_type=MESH)

    def final_out(t, i):
        if i == S - 1:
            return pltpu.make_async_copy(xout.at[t, i], xl_hbm.at[t], lastsem)
        return pltpu.make_async_remote_copy(xout.at[t, i], xl_hbm.at[t], send, lastsem, device_id=(base + i,), device_id_type=MESH)

    def arrived(t):
        step_out(t).wait_recv()

    def pass_on(t):
        @pl.when(jnp.logical_not(last))
        def _():
            step_out(t).start()

        @pl.when(last)
        def _():
            for i in range(S):
                final_out(t, i).start()

    @pl.when(first)
    def _():
        lax.fori_loop(0, T, lambda t, _: (pltpu.make_async_copy(x_hbm.at[t], xbuf.at[t, 0], recv.at[t]).start(), 0)[1], 0)

    @pl.when(jnp.logical_not(first))
    def _():
        lax.fori_loop(0, T, lambda t, _: (feed(t).start(), 0)[1], 0)

    bias = b_ref[pl.ds(stage, 1), :]

    def project(zref, t):
        xt = rows_of(xbuf[t].astype(F32)).astype(BF16)
        for n in range(0, G4, HB):
            zref[:, n:n + HB] = dot(xt, w[0:H, n:n + HB]) + bias[:, n:n + HB]

    wcopy.wait()
    arrived(0)
    project(z0, 0)

    bufs = ((z0, z1, q0, c0, h0), (z1, z0, q1, c1, h1))

    def saves(u, t):
        _, _, qb, cb, hb = bufs[u]
        return (pltpu.make_async_copy(qb, gates_hbm.at[t], osem.at[u, 0]), pltpu.make_async_copy(cb, cp_hbm.at[t], osem.at[u, 1]),
                pltpu.make_async_copy(hb, hp_hbm.at[t], osem.at[u, 2]))

    def two(p, state):
        for u in range(2):
            t = 2 * p + u
            zc, zn, qb, cb, hb = bufs[u]

            @pl.when(p > 0)
            def _():
                for cp in saves(u, t):
                    cp.wait()

            @pl.when(t + 1 < T)
            def _():
                arrived(t + 1)

            ha, hc, ca, cc = state
            hlow = jnp.concatenate([ha, hc], axis=1).astype(BF16)
            hb[...] = hlow
            cb[:, 0:HB] = ca
            cb[:, HB:H] = cc
            nh, nc = [], []
            for q in range(2):
                zz = []
                for g in range(4):
                    cols = slice(g * H + q * HB, g * H + q * HB + HB)
                    zz.append(zc[:, cols] + dot(hlow, w[H:2 * H, cols]))
                gi, gf, gg, go = jax.nn.sigmoid(zz[0]), jax.nn.sigmoid(zz[1]), jnp.tanh(zz[2]), jax.nn.sigmoid(zz[3])
                cn = gf * (ca, cc)[q] + gi * gg
                nh.append(go * jnp.tanh(cn))
                nc.append(cn)
                for g, val in enumerate((gi, gf, gg, go)):
                    qb[:, g * H + q * HB:g * H + q * HB + HB] = val
            project(zn, jnp.minimum(t + 1, T - 1))
            xt = rows_of(xbuf[t].astype(F32))
            xout[t] = groups_of(xt + jnp.concatenate(nh, axis=1)).astype(BF16)
            state = (nh[0], nh[1], nc[0], nc[1])
            for cp in saves(u, t):
                cp.start()

            @pl.when(t > 0)
            def _():
                pass_on(t - 1)

        return state

    zero = jnp.zeros((Q, HB), F32)
    lax.fori_loop(0, T // 2, two, (zero,) * 4)
    keep = pltpu.make_async_copy(xbuf, xs_hbm, wsem.at[0])
    keep.start()
    pass_on(T - 1)
    for u in range(2):
        for cp in saves(u, T - 2 + u):
            cp.wait()
    keep.wait()

    @pl.when(jnp.logical_not(first))
    def _():
        pltpu.make_async_remote_copy(x_hbm, xl_hbm, insem, lastsem, device_id=(base,), device_id_type=MESH).wait_send()

    @pl.when(jnp.logical_not(last))
    def _():
        pltpu.make_async_remote_copy(xout, xbuf, send, recv.at[0], device_id=(nxt,), device_id_type=MESH).wait_send()

    @pl.when(last)
    def _():
        others = (slice(None), slice(0, S - 1))
        pltpu.make_async_remote_copy(xout.at[others], xbuf.at[others], send, recv.at[0], device_id=(nxt,), device_id_type=MESH).wait_send()

    pltpu.make_async_copy(x_hbm, xl_hbm, lastsem).wait()


def forward(x, w, b):
    return pl.pallas_call(
        fwd_kernel,
        out_shape=(jax.ShapeDtypeStruct((T, Q, G4), F32), jax.ShapeDtypeStruct((T, Q, H), F32),
                   jax.ShapeDtypeStruct((T, Q, H), BF16), jax.ShapeDtypeStruct((T, S, R, H), BF16),
                   jax.ShapeDtypeStruct((T, R, H), BF16)),
        in_specs=[ANY, ANY, VMEM],
        out_specs=(ANY,) * 5,
        scratch_shapes=[pltpu.VMEM((2 * H, G4), BF16), pltpu.VMEM((T, S, R, H), BF16), pltpu.VMEM((T, S, R, H), BF16)]
        + [pltpu.VMEM((Q, G4), F32)] * 4 + [pltpu.VMEM((Q, H), F32)] * 2 + [pltpu.VMEM((Q, H), BF16)] * 2
        + [DMA((1,)), DMA, DMA((T,)), DMA, DMA, DMA((2, 3))],
        compiler_params=pltpu.CompilerParams(vmem_limit_bytes=32 * MIB, collective_id=0, has_side_effects=True),
        cost_estimate=pl.CostEstimate(flops=60_000_000_000, bytes_accessed=80_000_000, transcendentals=0),
        name="lstm_fwd",
    )(x, w, b)


def bwd_kernel(d_hbm, gates_hbm, cp_hbm, hp_hbm, xs_hbm, w_hbm, own_hbm, give_hbm, db_ref, dx_hbm,
               w, wt, dbuf, dout, dall, ut, q0, q1, c0, c1, h0, h1, x0, x1, r0, r1,
               wsem, insem, recv, send, lastsem, isem, osem):
    base, stage = place()
    plane = base // S
    first, last = stage == 0, stage == S - 1
    prv = base + lax.rem(stage + S - 1, S)
    top = base + S - 1
    plane_barrier(base, stage)

    wcopy = pltpu.make_async_copy(w_hbm.at[stage], w, wsem.at[0])
    wcopy.start()

    def feed(t):
        return pltpu.make_async_remote_copy(d_hbm.at[t], dbuf.at[t, stage], insem, recv.at[t],
                                            device_id=(top,), device_id_type=MESH)

    def step_out(t):
        return pltpu.make_async_remote_copy(dout.at[t], dbuf.at[t], send, recv.at[t], device_id=(prv,), device_id_type=MESH)

    def final_out(t, i):
        if i == 0:
            return pltpu.make_async_copy(dout.at[t, i], dx_hbm.at[t], lastsem)
        return pltpu.make_async_remote_copy(dout.at[t, i], dx_hbm.at[t], send, lastsem, device_id=(base + i,), device_id_type=MESH)

    def pass_on(t):
        @pl.when(jnp.logical_not(first))
        def _():
            step_out(t).start()

        @pl.when(first)
        def _():
            for i in range(S):
                final_out(t, i).start()

    @pl.when(last)
    def _():
        lax.fori_loop(0, T, lambda t, _: (pltpu.make_async_copy(d_hbm.at[T - 1 - t], dbuf.at[T - 1 - t, S - 1], recv.at[T - 1 - t]).start(), 0)[1], 0)

    @pl.when(jnp.logical_not(last))
    def _():
        lax.fori_loop(0, T, lambda t, _: (feed(T - 1 - t).start(), 0)[1], 0)

    bufs = ((q0, c0, h0, x0), (q1, c1, h1, x1))

    def loads(u, p):
        qb, cb, hb, xb = bufs[u]
        t = 2 * p + u
        return (pltpu.make_async_copy(gates_hbm.at[t], qb, isem.at[u, 0]), pltpu.make_async_copy(cp_hbm.at[t], cb, isem.at[u, 1]),
                pltpu.make_async_copy(hp_hbm.at[t], hb, isem.at[u, 2]), pltpu.make_async_copy(xs_hbm.at[t], xb, isem.at[u, 3]))

    for u in range(2):
        for cp in loads(u, T // 2 - 1):
            cp.start()
    db_ref[...] = jnp.zeros(db_ref.shape, F32)
    wcopy.wait()

    def turn(n, _):
        cols = pl.ds(pl.multiple_of(n * HB, HB), HB)
        wt[cols, :] = w[:, cols].T
        return 0

    lax.fori_loop(0, G4 // HB, turn, 0)

    def two(k, state):
        p = T // 2 - 1 - k
        us = []
        for u in (1, 0):
            t = 2 * p + u
            qb, cb, hb, xb = bufs[u]
            for cp in loads(u, p):
                cp.wait()
            step_out(t).wait_recv()
            ea, ec, da, dc_ = state
            dext = rows_of(dbuf[t])
            parts = [[None, None] for _ in range(4)]
            nd = []
            for q in range(2):
                gi, gf, gg, go = (qb[:, g * H + q * HB:g * H + q * HB + HB] for g in range(4))
                hq = slice(q * HB, q * HB + HB)
                cprev = cb[:, hq]
                th = jnp.tanh(gf * cprev + gi * gg)
                e = dext[:, hq] + (ea, ec)[q]
                dc = (da, dc_)[q] + e * (go * (1.0 - th * th))
                parts[0][q] = dc * (gg * gi * (1.0 - gi))
                parts[1][q] = dc * (cprev * gf * (1.0 - gf))
                parts[2][q] = dc * (gi * (1.0 - gg * gg))
                parts[3][q] = e * (th * go * (1.0 - go))
                nd.append(dc * gf)
            trows = pl.ds(pl.multiple_of(t * Q, Q), Q)
            lows = []
            for i, v in enumerate(v for ps in parts for v in ps):
                cols = slice(i * HB, i * HB + HB)
                low = v.astype(BF16)
                dall[trows, cols] = low
                lows.append(low)
                db_ref[:, cols] += jnp.sum(v.reshape(Q // R, R, HB), axis=0)
            lowz = jnp.concatenate(lows, axis=1)
            ne = [dot(lowz, wt[:, H + q * HB:H + q * HB + HB]) for q in range(2)]
            for q in range(2):
                hq = slice(q * HB, q * HB + HB)
                dout[t, :, :, hq] = groups_of(dext[:, hq] + dot(lowz, wt[:, hq]))
            state = (ne[0], ne[1], nd[0], nd[1])
            us.append((rows_of(xb[...].astype(F32)), hb[...].astype(F32)))

            @pl.when(p > 0)
            def _():
                for cp in loads(u, p - 1):
                    cp.start()

            @pl.when(t < T - 1)
            def _():
                pass_on(t + 1)

        tcols = pl.ds(pl.multiple_of(p * 2 * Q, 2 * Q), 2 * Q)
        for j in range(2):
            ut[j * H:j * H + H, tcols] = jnp.concatenate([us[1][j], us[0][j]], axis=0).T.astype(BF16)

        return state

    zero = jnp.zeros((Q, HB), F32)
    lax.fori_loop(0, T // 2, two, (zero,) * 4)
    pass_on(0)

    accs = (r0, r1)

    def weight(n, _):
        cols = pl.ds(pl.multiple_of(n * HB, HB), HB)
        for half, (dst, at) in enumerate(((give_hbm, 1 - plane), (own_hbm, plane))):
            out = pltpu.make_async_copy(accs[half], dst.at[:, cols], osem.at[half])

            @pl.when(n > 0)
            def _():
                out.wait()

            for m in range(0, H, HB):
                urows = pl.ds(pl.multiple_of(at * H + m, HB), HB)
                accs[half][m:m + HB, :] = dot(ut[urows, :], dall[:, cols])
            out.start()
        return 0

    lax.fori_loop(0, G4 // HB, weight, 0)
    for half, dst in enumerate((give_hbm, own_hbm)):
        pltpu.make_async_copy(accs[half], dst.at[:, 0:HB], osem.at[half]).wait()

    @pl.when(jnp.logical_not(last))
    def _():
        pltpu.make_async_remote_copy(d_hbm, dx_hbm, insem, lastsem, device_id=(top,), device_id_type=MESH).wait_send()

    @pl.when(jnp.logical_not(first))
    def _():
        pltpu.make_async_remote_copy(dout, dbuf, send, recv.at[0], device_id=(prv,), device_id_type=MESH).wait_send()

    @pl.when(first)
    def _():
        others = (slice(None), slice(1, S))
        pltpu.make_async_remote_copy(dout.at[others], dbuf.at[others], send, recv.at[0], device_id=(prv,), device_id_type=MESH).wait_send()

    pltpu.make_async_copy(d_hbm, dx_hbm, lastsem).wait()


def backward(d_top, gates, cprev, hprev, xs, w):
    return pl.pallas_call(
        bwd_kernel,
        out_shape=(jax.ShapeDtypeStruct((H, G4), F32), jax.ShapeDtypeStruct((H, G4), F32), jax.ShapeDtypeStruct((R, G4), F32),
                   jax.ShapeDtypeStruct((T, R, H), F32)),
        in_specs=[ANY] * 6,
        out_specs=(ANY, ANY, VMEM, ANY),
        scratch_shapes=[pltpu.VMEM((2 * H, G4), BF16), pltpu.VMEM((G4, 2 * H), BF16), pltpu.VMEM((T, S, R, H), F32),
                        pltpu.VMEM((T, S, R, H), F32), pltpu.VMEM((T * Q, G4), BF16), pltpu.VMEM((2 * H, T * Q), BF16)]
        + [pltpu.VMEM((Q, G4), F32)] * 2 + [pltpu.VMEM((Q, H), F32)] * 2 + [pltpu.VMEM((Q, H), BF16)] * 2
        + [pltpu.VMEM((S, R, H), BF16)] * 2 + [pltpu.VMEM((H, HB), F32)] * 2
        + [DMA((1,)), DMA, DMA((T,)), DMA, DMA, DMA((2, 4)), DMA((2,))],
        compiler_params=pltpu.CompilerParams(vmem_limit_bytes=56 * MIB, collective_id=1, has_side_effects=True),
        cost_estimate=pl.CostEstimate(flops=110_000_000_000, bytes_accessed=80_000_000, transcendentals=0),
        name="lstm_bwd",
    )(d_top, gates, cprev, hprev, xs, w)


VB = 1280
NVB = V // VB
N = T * R
NW = 4
RB = 64


def head_kernel(x_ref, t_ref, w_hbm, dx_ref, lse_ref, lg, g0, g1, wv, mx, sm, tb, wsem):
    def wcopy(b):
        buf = lax.rem(b, NW)
        return pltpu.make_async_copy(w_hbm.at[:, pl.ds(pl.multiple_of(lax.rem(b, NVB) * VB, VB), VB)], wv.at[buf], wsem.at[buf])

    for b in range(NW - 1):
        wcopy(b).start()
    mx[...] = jnp.full(mx.shape, -jnp.inf, F32)
    sm[...] = jnp.zeros(sm.shape, F32)
    dx_ref[...] = jnp.zeros(dx_ref.shape, F32)

    def logits(b):
        wcopy(b).wait()
        wcopy(b + NW - 1).start()
        for c in range(0, VB, HB):
            lg[b, :, c:c + HB] = dot(x_ref[...], wv[lax.rem(b, NW), :, c:c + HB])

    def sums(b):
        for r in range(0, N, RB):
            rows = slice(r, r + RB)
            m_old = mx[rows, :]
            m_new = m_old
            for c in range(0, VB, LANE):
                m_new = jnp.maximum(m_new, lg[b, rows, c:c + LANE])
            acc = sm[rows, :] * jnp.exp(m_old - m_new)
            for c in range(0, VB, LANE):
                acc = acc + jnp.exp(lg[b, rows, c:c + LANE] - m_new)
            mx[rows, :] = m_new
            sm[rows, :] = acc

    logits(0)

    def first(b, _):
        logits(b)
        sums(b - 1)
        return 0

    lax.fori_loop(1, NVB, first, 0)
    sums(NVB - 1)
    for r in range(0, N, LANE):
        rows = slice(r, r + LANE)
        top = jnp.max(mx[rows, :], axis=1, keepdims=True)
        tot = jnp.sum(sm[rows, :] * jnp.exp(mx[rows, :] - top), axis=1, keepdims=True)
        lse = top + jnp.log(tot)
        lse_ref[rows, :] = lse
        mx[rows, :] = jnp.broadcast_to(lse, (LANE, LANE))
        tb[rows, :] = jnp.broadcast_to(t_ref[rows, :], (LANE, LANE))

    def grads(b, gb, c):
        ids = b * VB + c + lax.broadcasted_iota(jnp.int32, (RB, LANE), 1)
        for r in range(0, N, RB):
            rows = slice(r, r + RB)
            lse = mx[rows, :]
            tgt = tb[rows, :] - ids
            for h in (0, LANE):
                p = jnp.exp(lg[b, rows, c + h:c + h + LANE] - lse)
                gb[rows, c + h:c + h + LANE] = jnp.where(tgt == h, p - 1.0, p).astype(BF16)

    def apply(b, gb, c):
        return dot_tt(gb[:, c:c + HB], wv[lax.rem(b + NVB, NW), :, c:c + HB])

    for c in range(0, VB, HB):
        grads(0, g0, c)

    def second(h, _):
        for b, gb, gn in ((2 * h, g0, g1), (2 * h + 1, g1, g0)):
            wcopy(b + NVB).wait()

            @pl.when(b + NW - 1 < NVB)
            def _():
                wcopy(b + NVB + NW - 1).start()

            total = jnp.zeros((N, H), F32)
            for c in range(0, VB, HB):
                total = total + apply(b, gb, c)
                grads(b + 1, gn, c)
            dx_ref[...] += total
        return 0

    lax.fori_loop(0, NVB // 2, second, 0)
    wcopy(2 * NVB - 1).wait()
    for c in range(0, VB, HB):
        dx_ref[...] += apply(NVB - 1, g0, c)


def head(x, tgt, w_vocab):
    return pl.pallas_call(
        head_kernel,
        out_shape=(jax.ShapeDtypeStruct((N, H), F32), jax.ShapeDtypeStruct((N, 1), F32)),
        in_specs=[VMEM, VMEM, ANY],
        out_specs=(VMEM, VMEM),
        scratch_shapes=[pltpu.VMEM((NVB, N, VB), F32), pltpu.VMEM((N, VB), BF16), pltpu.VMEM((N, VB), BF16), pltpu.VMEM((NW, H, VB), BF16),
                        pltpu.VMEM((N, LANE), F32), pltpu.VMEM((N, LANE), F32), pltpu.VMEM((N, LANE), jnp.int32), DMA((NW,))],
        compiler_params=pltpu.CompilerParams(vmem_limit_bytes=60 * MIB),
        cost_estimate=pl.CostEstimate(flops=40_000_000_000, bytes_accessed=70_000_000, transcendentals=0),
        name="head",
    )(x, tgt, w_vocab)


TB = 768
NTOK = NDEV * N
NK = NTOK // TB
NOWN = (NVB + 1) // 2


def dwv_kernel(lo, hi, x_hbm, st_ref, w_hbm, *rest):
    dw_hbm, xv, xtv, wv, lg0, lg1, g0, g1, acc, wsem, xsem, osem, ssem, rsem = rest[-14:]
    core = lax.rem(lax.axis_index("data"), 2)
    peer = lax.axis_index("data") + 1 - 2 * core

    barrier = pltpu.get_barrier_semaphore()
    pl.semaphore_signal(barrier, inc=1, device_id=(peer,), device_id_type=MESH)

    def block(i, side):
        return lo + i + side * (NVB - 1 - 2 * (lo + i))

    def cols(b):
        return pl.ds(pl.multiple_of(b * VB, VB), VB)

    def wcopy(i):
        buf = lax.rem(i, 2)
        return pltpu.make_async_copy(w_hbm.at[:, cols(block(i, core))], wv.at[buf], wsem.at[buf])

    def keep(i):
        buf = lax.rem(i, 2)
        return pltpu.make_async_copy(acc.at[buf], dw_hbm.at[:, cols(block(i, core))], osem.at[buf])

    def send(i, side):
        buf = lax.rem(i, 2)
        return pltpu.make_async_remote_copy(acc.at[buf], dw_hbm.at[:, cols(block(i, side))], ssem.at[buf], rsem.at[i],
                                            device_id=(peer,), device_id_type=MESH)

    def shared(i):
        return lo + i < NOWN - 1

    def done(i):
        keep(i).start()

        @pl.when(shared(i))
        def _():
            send(i, core).start()

    def drained(i):
        keep(i).wait()

        @pl.when(shared(i))
        def _():
            send(i, core).wait_send()

    n = hi - lo
    wcopy(0).start()
    cx = pltpu.make_async_copy(x_hbm, xv, xsem.at[0])
    cx.start()
    cx.wait()

    def turn(k, _):
        rows = pl.ds(pl.multiple_of(k * HB, HB), HB)
        xtv[:, rows] = xv[rows, :].T
        return 0

    lax.fori_loop(0, NTOK // HB, turn, 0)
    pl.semaphore_wait(barrier, 1)

    def body(h, _):
        it = 2 * h
        i0, k0 = it // NK, lax.rem(it, NK)
        k2 = lax.rem(it + NK - 2, NK)
        i2 = jnp.maximum(it - 2, 0) // NK

        @pl.when((k0 == 0) & (i0 < n))
        def _():
            wcopy(i0).wait()

            @pl.when(i0 < n - 1)
            def _():
                wcopy(i0 + 1).start()

        @pl.when((k2 == 0) & (i2 >= 2))
        def _():
            drained(i2 - 2)

        for u, (lnew, lold, gnew, gold) in enumerate(((lg0, lg1, g1, g0), (lg1, lg0, g0, g1))):
            k1 = lax.rem(it + u + NK - 1, NK)
            i1 = jnp.maximum(it + u - 1, 0) // NK
            rows0 = pl.ds(pl.multiple_of((k0 + u) * TB, TB), TB)
            rows2 = pl.ds(pl.multiple_of((k2 + u) * TB, TB), TB)
            ids = (block(i1, core) * VB + lax.broadcasted_iota(jnp.int32, (RB, LANE), 1)).astype(F32)
            for c in range(0, VB, HB):
                lnew[:, c:c + HB] = dot(xv[rows0, :], wv[lax.rem(i0, 2), :, c:c + HB])
                acc_c = acc.at[lax.rem(i2, 2), :, c:c + HB]
                old = acc_c[...]
                acc_c[...] = (jnp.where(k2 == 0, 0.0, old) if u == 0 else old) + dot(xtv[:, rows2], gold[:, c:c + HB])
            for r in range(0, TB, RB):
                here = pl.ds(pl.multiple_of(k1 * TB + r, RB), RB)
                lse = jnp.broadcast_to(st_ref[here, 0:1], (RB, LANE))
                tgt = jnp.broadcast_to(st_ref[here, LANE - 1:LANE], (RB, LANE)) - ids
                for c in range(0, VB, LANE):
                    p = jnp.exp(lold[r:r + RB, c:c + LANE] - lse)
                    gnew[r:r + RB, c:c + LANE] = jnp.where(tgt == c, p - 1.0, p).astype(BF16)

        @pl.when((k2 == 0) & (i2 >= 1))
        def _():
            done(i2 - 1)

        return 0

    lax.fori_loop(0, n * NK // 2 + 1, body, 0)
    done(n - 1)
    drained(n - 2)
    drained(n - 1)
    for i in range(min(n, NOWN - 1 - lo)):
        send(i, 1 - core).wait_recv()


def grad_vocab(lo, hi, x_all, stats, w_vocab, before=()):
    return pl.pallas_call(
        functools.partial(dwv_kernel, lo, hi),
        out_shape=jax.ShapeDtypeStruct((H, V), F32),
        in_specs=[ANY, VMEM, ANY] + [ANY] * len(before),
        out_specs=ANY,
        input_output_aliases={3: 0} if before else {},
        scratch_shapes=[pltpu.VMEM((NTOK, H), BF16), pltpu.VMEM((H, NTOK), BF16), pltpu.VMEM((2, H, VB), BF16)]
        + [pltpu.VMEM((TB, VB), F32)] * 2 + [pltpu.VMEM((TB, VB), BF16)] * 2
        + [pltpu.VMEM((2, H, VB), F32), DMA((2,)), DMA((1,)), DMA((2,)), DMA((2,)), DMA((hi - lo,))],
        compiler_params=pltpu.CompilerParams(vmem_limit_bytes=48 * MIB, collective_id=2 + (lo > 0), has_side_effects=True),
        cost_estimate=pl.CostEstimate(flops=(hi - lo) * 20_000_000_000, bytes_accessed=100_000_000, transcendentals=0),
        name="dwv",
    )(x_all, stats, w_vocab, *before)


SPLIT = 5


def solution(mesh):
    def local_grads(x_rows, tgt_rows, w_lstm, b_lstm, w_vocab):
        tgt = jnp.swapaxes(tgt_rows, 0, 1).reshape(N, 1)
        gates, cprev, hprev, xs, top = forward(jnp.swapaxes(x_rows, 0, 1), w_lstm, b_lstm)
        top = top.reshape(N, H)
        d_top, lse = head(top, tgt, w_vocab)
        half = (N, LANE // 2)
        stats = jnp.concatenate([jnp.broadcast_to(lse, half), jnp.broadcast_to(tgt.astype(F32), half)], axis=1)
        x_all = lax.all_gather(top, 'data', axis=0, tiled=True)
        stats = lax.all_gather(stats, 'data', axis=0, tiled=True)
        own, give, db, dx = backward(d_top.reshape(T, R, H), gates, cprev, hprev, xs, w_lstm)
        got = lax.ppermute(give, 'data', [(i, (i + S) % NDEV) for i in range(NDEV)])
        dwv = grad_vocab(0, SPLIT, x_all, stats, w_vocab)
        db = lax.all_gather(db, 'data', axis=0).reshape(NDEV // S, S, R, G4)
        own, dwv = lax.optimization_barrier((own, dwv))
        part, dwv = lax.optimization_barrier((own + got, dwv))
        parts = lax.all_gather(part, 'data', axis=0).reshape(NDEV // S, S, H, G4)
        dwv = grad_vocab(SPLIT, NOWN, x_all, stats, w_vocab, (dwv,))
        dw = jnp.swapaxes(parts, 0, 1).reshape(L, 2 * H, G4)
        db = jnp.sum(db, axis=(0, 2))
        return dw, db, dwv, jnp.swapaxes(dx, 0, 1)

    return jax.shard_map(local_grads, mesh=mesh, in_specs=(P('data'), P('data'), P(), P(), P()), out_specs=(P(), P(), P(), P('data')), check_vma=False)
```

```python
import functools

import jax
import jax.numpy as jnp
from jax import lax
from jax.experimental import pallas as pl
from jax.experimental.pallas import tpu as pltpu
from jax.sharding import PartitionSpec as P

T = 48
R = 8
S = 8
Q = S * R
H = 512
HB = 256
G4 = 4 * H
L = 8
V = 32000
LANE = 128
NDEV = 16
CH = 4
NR = 6
F32 = jnp.float32
BF16 = jnp.bfloat16
MESH = pl.DeviceIdType.MESH
MIB = 1024 * 1024
ANY = pl.BlockSpec(memory_space=pl.ANY)
VMEM = pl.BlockSpec(memory_space=pltpu.VMEM)
HBM = pl.BlockSpec(memory_space=pltpu.HBM)
DMA = pltpu.SemaphoreType.DMA


def dot(a, b):
    return jnp.dot(a, b, preferred_element_type=F32)


def dot_tt(a, b):
    return lax.dot_general(a, b, (((1,), (1,)), ((), ())), preferred_element_type=F32)


def place():
    me = lax.axis_index("data")
    return me // S * S, lax.rem(me, S)


def plane_signal(base, stage):
    barrier = pltpu.get_barrier_semaphore()
    for i in range(1, S):
        pl.semaphore_signal(barrier, inc=1, device_id=(base + lax.rem(stage + i, S),), device_id_type=MESH)


def plane_wait():
    pl.semaphore_wait(pltpu.get_barrier_semaphore(), S - 1)


def rows_of(v):
    return v.reshape(Q, v.shape[-1])


def groups_of(v):
    return v.reshape(S, R, v.shape[-1])


def fwd_kernel(x_hbm, w_hbm, b_ref, gates_hbm, cp_hbm, hp_hbm, xs_hbm, xl_hbm,
               w, xbuf, xout, gates, cprev, hprev, z0, z1, wsem, insem, recv, send, lastsem, osem):
    base, stage = place()
    first, last = stage == 0, stage == S - 1
    nxt = base + lax.rem(stage + 1, S)
    plane_signal(base, stage)
    wcopy = pltpu.make_async_copy(w_hbm.at[stage], w, wsem.at[0])
    wcopy.start()
    plane_wait()

    def feed(k):
        ts = pl.ds(k * CH, CH)

        @pl.when(first)
        def _():
            pltpu.make_async_copy(x_hbm.at[ts], xbuf.at[ts, 0], recv.at[k * CH]).start()

        @pl.when(jnp.logical_not(first))
        def _():
            pltpu.make_async_remote_copy(x_hbm.at[ts], xbuf.at[ts, stage], insem, recv.at[k * CH],
                                         device_id=(base,), device_id_type=MESH).start()

        return 0

    def step_out(t):
        return pltpu.make_async_remote_copy(xout.at[t], xbuf.at[t], send, recv.at[t], device_id=(nxt,), device_id_type=MESH)

    def final_out(t, i):
        ts = pl.ds(t, CH)
        if i == S - 1:
            return pltpu.make_async_copy(xout.at[ts, i], xl_hbm.at[ts], lastsem)
        return pltpu.make_async_remote_copy(xout.at[ts, i], xl_hbm.at[ts], send, lastsem, device_id=(base + i,), device_id_type=MESH)

    def arrived(t):
        @pl.when(jnp.logical_not(first))
        def _():
            step_out(t).wait_recv()

        @pl.when(first & (lax.rem(t, CH) == 0))
        def _():
            ts = pl.ds(t, CH)
            pltpu.make_async_remote_copy(xout.at[ts], xbuf.at[ts], send, recv.at[t], device_id=(nxt,), device_id_type=MESH).wait_recv()

    def pass_on(t):
        @pl.when(jnp.logical_not(last))
        def _():
            step_out(t).start()

        @pl.when(last & (lax.rem(t, CH) == CH - 1))
        def _():
            for i in range(S):
                final_out(t - CH + 1, i).start()

    lax.fori_loop(0, T // CH, lambda k, _: feed(k), 0)
    bias = b_ref[pl.ds(stage, 1), :]

    def project(zref, t):
        xt = rows_of(xbuf[t].astype(F32)).astype(BF16)
        for n in range(0, G4, HB):
            zref[:, n:n + HB] = dot(xt, w[0:H, n:n + HB]) + bias[:, n:n + HB]

    wcopy.wait()
    arrived(jnp.int32(0))
    project(z0, 0)

    kept = ((gates, gates_hbm), (cprev, cp_hbm), (hprev, hp_hbm), (xbuf, xs_hbm))

    def save(t):
        for i, (src, dst) in enumerate(kept):
            pltpu.make_async_copy(src.at[t], dst.at[t], osem.at[i]).start()

    def two(p, state):
        for u in range(2):
            t = 2 * p + u
            zc, zn = ((z0, z1), (z1, z0))[u]

            @pl.when(t > 0)
            def _():
                pass_on(t - 1)
                save(t - 1)

            @pl.when(t + 1 < T)
            def _():
                arrived(t + 1)

            ha, hc, ca, cc = state
            hlow = jnp.concatenate([ha, hc], axis=1).astype(BF16)
            hprev[t] = hlow
            cprev[t, :, 0:HB] = ca
            cprev[t, :, HB:H] = cc
            nh, nc = [], []
            for q in range(2):
                zz = []
                for g in range(4):
                    cols = slice(g * H + q * HB, g * H + q * HB + HB)
                    zz.append(zc[:, cols] + dot(hlow, w[H:2 * H, cols]))
                gi, gf, gg, go = jax.nn.sigmoid(zz[0]), jax.nn.sigmoid(zz[1]), jnp.tanh(zz[2]), jax.nn.sigmoid(zz[3])
                cn = gf * (ca, cc)[q] + gi * gg
                nh.append(go * jnp.tanh(cn))
                nc.append(cn)
                for g, val in enumerate((gi, gf, gg, go)):
                    gates[t, :, g * H + q * HB:g * H + q * HB + HB] = val
            project(zn, jnp.minimum(t + 1, T - 1))
            xt = rows_of(xbuf[t].astype(F32))
            xout[t] = groups_of(xt + jnp.concatenate(nh, axis=1)).astype(BF16)
            state = (nh[0], nh[1], nc[0], nc[1])
        return state

    zero = jnp.zeros((Q, HB), F32)
    lax.fori_loop(0, T // 2, two, (zero,) * 4)
    pass_on(jnp.int32(T - 1))
    save(T - 1)
    for i, (src, dst) in enumerate(kept):
        pltpu.make_async_copy(src, dst, osem.at[i]).wait()

    @pl.when(jnp.logical_not(first))
    def _():
        pltpu.make_async_remote_copy(x_hbm, xl_hbm, insem, lastsem, device_id=(base,), device_id_type=MESH).wait_send()

    @pl.when(jnp.logical_not(last))
    def _():
        pltpu.make_async_remote_copy(xout, xbuf, send, recv.at[0], device_id=(nxt,), device_id_type=MESH).wait_send()

    @pl.when(last)
    def _():
        others = (slice(None), slice(0, S - 1))
        pltpu.make_async_remote_copy(xout.at[others], xbuf.at[others], send, recv.at[0], device_id=(nxt,), device_id_type=MESH).wait_send()

    pltpu.make_async_copy(x_hbm, xl_hbm, lastsem).wait()


def forward(x, w, b):
    return pl.pallas_call(
        fwd_kernel,
        out_shape=(jax.ShapeDtypeStruct((T, Q, G4), F32), jax.ShapeDtypeStruct((T, Q, H), F32),
                   jax.ShapeDtypeStruct((T, Q, H), BF16), jax.ShapeDtypeStruct((T, S, R, H), BF16),
                   jax.ShapeDtypeStruct((T, R, H), BF16)),
        in_specs=[ANY, ANY, VMEM],
        out_specs=(HBM,) * 5,
        scratch_shapes=[pltpu.VMEM((2 * H, G4), BF16), pltpu.VMEM((T, S, R, H), BF16), pltpu.VMEM((T, S, R, H), BF16),
                        pltpu.VMEM((T, Q, G4), F32), pltpu.VMEM((T, Q, H), F32), pltpu.VMEM((T, Q, H), BF16)]
        + [pltpu.VMEM((Q, G4), F32)] * 2 + [DMA((1,)), DMA, DMA((T,)), DMA, DMA, DMA((4,))],
        compiler_params=pltpu.CompilerParams(vmem_limit_bytes=52 * MIB, collective_id=0, has_side_effects=True),
        cost_estimate=pl.CostEstimate(flops=60_000_000_000, bytes_accessed=80_000_000, transcendentals=0),
        name="lstm_fwd",
    )(x, w, b)


def bwd_kernel(d_hbm, gates_hbm, cp_hbm, hp_hbm, xs_hbm, w_hbm, own0, own1, give0, give1, db_ref, dx_hbm,
               w, wt, dbuf, dout, dall, ut, gin, cin, hin, xin, acc,
               wsem, insem, recv, send, lastsem, isem, osem):
    base, stage = place()
    plane = base // S
    first, last = stage == 0, stage == S - 1
    prv = base + lax.rem(stage + S - 1, S)
    top = base + S - 1
    plane_signal(base, stage)
    wcopy = pltpu.make_async_copy(w_hbm.at[stage], w, wsem.at[0])
    wcopy.start()

    def feed(k):
        t = T - CH - k * CH
        ts = pl.ds(t, CH)

        @pl.when(last)
        def _():
            pltpu.make_async_copy(d_hbm.at[ts], dbuf.at[ts, S - 1], recv.at[t]).start()

        @pl.when(jnp.logical_not(last))
        def _():
            pltpu.make_async_remote_copy(d_hbm.at[ts], dbuf.at[ts, stage], insem, recv.at[t],
                                         device_id=(top,), device_id_type=MESH).start()

        return 0

    def step_out(t):
        return pltpu.make_async_remote_copy(dout.at[t], dbuf.at[t], send, recv.at[t], device_id=(prv,), device_id_type=MESH)

    def final_out(t, i):
        ts = pl.ds(t, CH)
        if i == 0:
            return pltpu.make_async_copy(dout.at[ts, i], dx_hbm.at[ts], lastsem)
        return pltpu.make_async_remote_copy(dout.at[ts, i], dx_hbm.at[ts], send, lastsem, device_id=(base + i,), device_id_type=MESH)

    def arrived(t):
        @pl.when(jnp.logical_not(last))
        def _():
            step_out(t).wait_recv()

        @pl.when(last & (lax.rem(t, CH) == CH - 1))
        def _():
            ts = pl.ds(t - CH + 1, CH)
            pltpu.make_async_remote_copy(dout.at[ts], dbuf.at[ts], send, recv.at[t - CH + 1], device_id=(prv,), device_id_type=MESH).wait_recv()

    def pass_on(t):
        @pl.when(jnp.logical_not(first))
        def _():
            step_out(t).start()

        @pl.when(first & (lax.rem(t, CH) == 0))
        def _():
            for i in range(S):
                final_out(t, i).start()

    def loads(t):
        k = lax.rem(t, NR)
        return [pltpu.make_async_copy(src.at[t], dst.at[k], isem.at[k, i])
                for i, (src, dst) in enumerate(((gates_hbm, gin), (cp_hbm, cin), (hp_hbm, hin), (xs_hbm, xin)))]

    for t in range(T - NR, T):
        for cp in loads(t):
            cp.start()
    plane_wait()
    lax.fori_loop(0, T // CH, lambda k, _: feed(k), 0)
    db_ref[...] = jnp.zeros(db_ref.shape, F32)
    wcopy.wait()

    def turn(n, _):
        cols = pl.ds(pl.multiple_of(n * HB, HB), HB)
        wt[cols, :] = w[:, cols].T
        return 0

    lax.fori_loop(0, G4 // HB, turn, 0)

    def two(n, state):
        p = T // 2 - 1 - n
        us = []
        for u in (1, 0):
            t = 2 * p + u
            k = lax.rem(t, NR)
            for cp in loads(t):
                cp.wait()

            @pl.when(t < T - 1)
            def _():
                pass_on(t + 1)

            arrived(t)
            ea, ec, da, dc_ = state
            dext = rows_of(dbuf[t])
            parts = [[None, None] for _ in range(4)]
            nd = []
            for q in range(2):
                gi, gf, gg, go = (gin[k, :, g * H + q * HB:g * H + q * HB + HB] for g in range(4))
                hq = slice(q * HB, q * HB + HB)
                cprev = cin[k, :, hq]
                th = jnp.tanh(gf * cprev + gi * gg)
                e = dext[:, hq] + (ea, ec)[q]
                dc = (da, dc_)[q] + e * (go * (1.0 - th * th))
                parts[0][q] = dc * (gg * gi * (1.0 - gi))
                parts[1][q] = dc * (cprev * gf * (1.0 - gf))
                parts[2][q] = dc * (gi * (1.0 - gg * gg))
                parts[3][q] = e * (th * go * (1.0 - go))
                nd.append(dc * gf)
            trows = pl.ds(pl.multiple_of(t * Q, Q), Q)
            lows = []
            for i, v in enumerate(v for ps in parts for v in ps):
                cols = slice(i * HB, i * HB + HB)
                low = v.astype(BF16)
                dall[trows, cols] = low
                lows.append(low)
                db_ref[:, cols] += jnp.sum(v.reshape(Q // R, R, HB), axis=0)
            lowz = jnp.concatenate(lows, axis=1)
            ne = [dot(lowz, wt[:, H + q * HB:H + q * HB + HB]) for q in range(2)]
            for q in range(2):
                hq = slice(q * HB, q * HB + HB)
                dout[t, :, :, hq] = groups_of(dext[:, hq] + dot(lowz, wt[:, hq]))
            state = (ne[0], ne[1], nd[0], nd[1])
            us.append((rows_of(xin[k].astype(F32)), hin[k].astype(F32)))

            @pl.when(t >= NR)
            def _():
                for cp in loads(t - NR):
                    cp.start()

        tcols = pl.ds(pl.multiple_of(p * 2 * Q, 2 * Q), 2 * Q)
        for j in range(2):
            ut[j * H:j * H + H, tcols] = jnp.concatenate([us[1][j], us[0][j]], axis=0).T.astype(BF16)

        return state

    zero = jnp.zeros((Q, HB), F32)
    lax.fori_loop(0, T // 2, two, (zero,) * 4)
    pass_on(jnp.int32(0))

    quarters = ((give0, 0, 1 - plane), (give1, HB, 1 - plane), (own0, 0, plane), (own1, HB, plane))

    def weight(n, _):
        cols = pl.ds(pl.multiple_of(n * HB, HB), HB)
        for i, (dst, m, at) in enumerate(quarters):
            out = pltpu.make_async_copy(acc.at[i], dst.at[:, cols], osem.at[i])

            @pl.when(n > 0)
            def _():
                out.wait()

            acc[i] = dot(ut[pl.ds(pl.multiple_of(at * H + m, HB), HB), :], dall[:, cols])
            out.start()
        return 0

    lax.fori_loop(0, G4 // HB, weight, 0)
    for i, (dst, _, _) in enumerate(quarters):
        pltpu.make_async_copy(acc.at[i], dst.at[:, 0:HB], osem.at[i]).wait()

    @pl.when(jnp.logical_not(last))
    def _():
        pltpu.make_async_remote_copy(d_hbm, dx_hbm, insem, lastsem, device_id=(top,), device_id_type=MESH).wait_send()

    @pl.when(jnp.logical_not(first))
    def _():
        pltpu.make_async_remote_copy(dout, dbuf, send, recv.at[0], device_id=(prv,), device_id_type=MESH).wait_send()

    @pl.when(first)
    def _():
        others = (slice(None), slice(1, S))
        pltpu.make_async_remote_copy(dout.at[others], dbuf.at[others], send, recv.at[0], device_id=(prv,), device_id_type=MESH).wait_send()

    pltpu.make_async_copy(d_hbm, dx_hbm, lastsem).wait()


def backward(d_top, gates, cprev, hprev, xs, w):
    return pl.pallas_call(
        bwd_kernel,
        out_shape=(jax.ShapeDtypeStruct((HB, G4), F32),) * 4 + (jax.ShapeDtypeStruct((R, G4), F32), jax.ShapeDtypeStruct((T, R, H), F32)),
        in_specs=[ANY] * 6,
        out_specs=(HBM,) * 4 + (VMEM, HBM),
        scratch_shapes=[pltpu.VMEM((2 * H, G4), BF16), pltpu.VMEM((G4, 2 * H), BF16), pltpu.VMEM((T, S, R, H), F32),
                        pltpu.VMEM((T, S, R, H), F32), pltpu.VMEM((T * Q, G4), BF16), pltpu.VMEM((2 * H, T * Q), BF16)]
        + [pltpu.VMEM((NR, Q, G4), F32), pltpu.VMEM((NR, Q, H), F32), pltpu.VMEM((NR, Q, H), BF16), pltpu.VMEM((NR, S, R, H), BF16)]
        + [pltpu.VMEM((4, HB, HB), F32)]
        + [DMA((1,)), DMA, DMA((T,)), DMA, DMA, DMA((NR, 4)), DMA((4,))],
        compiler_params=pltpu.CompilerParams(vmem_limit_bytes=56 * MIB, collective_id=1, has_side_effects=True),
        cost_estimate=pl.CostEstimate(flops=110_000_000_000, bytes_accessed=80_000_000, transcendentals=0),
        name="lstm_bwd",
    )(d_top, gates, cprev, hprev, xs, w)


VB = 1280
NVB = V // VB
N = T * R
NW = 4
RB = 64


def head_kernel(x_ref, t_ref, w_hbm, dx_ref, lse_ref, lg, g0, g1, wv, mx, sm, tb, wsem):
    def wcopy(b):
        buf = lax.rem(b, NW)
        return pltpu.make_async_copy(w_hbm.at[:, pl.ds(pl.multiple_of(lax.rem(b, NVB) * VB, VB), VB)], wv.at[buf], wsem.at[buf])

    for b in range(NW - 1):
        wcopy(b).start()

    def ready(b):
        for i in range(2):
            wcopy(b + i).wait()
            wcopy(b + i + 2).start()

    mx[...] = jnp.full(mx.shape, -jnp.inf, F32)
    sm[...] = jnp.zeros(sm.shape, F32)
    dx_ref[...] = jnp.zeros(dx_ref.shape, F32)

    def logits(b):
        for c in range(0, VB, HB):
            lg[b, :, c:c + HB] = dot(x_ref[...], wv[lax.rem(b, NW), :, c:c + HB])

    def sums(b):
        for r in range(0, N, RB):
            rows = slice(r, r + RB)
            m_old = mx[rows, :]
            m_new = m_old
            for c in range(0, VB, LANE):
                m_new = jnp.maximum(m_new, lg[b, rows, c:c + LANE])
            acc = sm[rows, :] * jnp.exp(m_old - m_new)
            for c in range(0, VB, LANE):
                acc = acc + jnp.exp(lg[b, rows, c:c + LANE] - m_new)
            mx[rows, :] = m_new
            sm[rows, :] = acc

    wcopy(0).wait()
    logits(0)

    def first(h, _):
        b = 2 * h + 1
        ready(b)
        for i in range(2):
            logits(b + i)
            sums(b + i - 1)
        return 0

    lax.fori_loop(0, NVB // 2, first, 0)
    sums(NVB - 1)
    for r in range(0, N, LANE):
        rows = slice(r, r + LANE)
        top = jnp.max(mx[rows, :], axis=1, keepdims=True)
        tot = jnp.sum(sm[rows, :] * jnp.exp(mx[rows, :] - top), axis=1, keepdims=True)
        lse = top + jnp.log(tot)
        lse_ref[rows, :] = lse
        mx[rows, :] = jnp.broadcast_to(lse, (LANE, LANE))
        tb[rows, :] = jnp.broadcast_to(t_ref[rows, :], (LANE, LANE))

    def grads(b, gb, c):
        ids = b * VB + c + lax.broadcasted_iota(jnp.int32, (RB, LANE), 1)
        for r in range(0, N, RB):
            rows = slice(r, r + RB)
            lse = mx[rows, :]
            tgt = tb[rows, :] - ids
            for h in (0, LANE):
                p = jnp.exp(lg[b, rows, c + h:c + h + LANE] - lse)
                gb[rows, c + h:c + h + LANE] = jnp.where(tgt == h, p - 1.0, p).astype(BF16)

    def apply(b, gb, c):
        return dot_tt(gb[:, c:c + HB], wv[lax.rem(b + NVB, NW), :, c:c + HB])

    for c in range(0, VB, HB):
        grads(0, g0, c)

    def second(h, _):
        for i in range(2):
            b = 2 * h + NVB + i
            wcopy(b).wait()

            @pl.when(b + 2 < 2 * NVB)
            def _():
                wcopy(b + 2).start()

        for b, gb, gn in ((2 * h, g0, g1), (2 * h + 1, g1, g0)):
            total = jnp.zeros((N, H), F32)
            for c in range(0, VB, HB):
                total = total + apply(b, gb, c)
                grads(b + 1, gn, c)
            dx_ref[...] += total
        return 0

    lax.fori_loop(0, NVB // 2, second, 0)
    wcopy(2 * NVB - 1).wait()
    for c in range(0, VB, HB):
        dx_ref[...] += apply(NVB - 1, g0, c)


def head(x, tgt, w_vocab):
    return pl.pallas_call(
        head_kernel,
        out_shape=(jax.ShapeDtypeStruct((N, H), F32), jax.ShapeDtypeStruct((N, 1), F32)),
        in_specs=[VMEM, VMEM, ANY],
        out_specs=(VMEM, VMEM),
        scratch_shapes=[pltpu.VMEM((NVB, N, VB), F32), pltpu.VMEM((N, VB), BF16), pltpu.VMEM((N, VB), BF16), pltpu.VMEM((NW, H, VB), BF16),
                        pltpu.VMEM((N, LANE), F32), pltpu.VMEM((N, LANE), F32), pltpu.VMEM((N, LANE), jnp.int32), DMA((NW,))],
        compiler_params=pltpu.CompilerParams(vmem_limit_bytes=60 * MIB),
        cost_estimate=pl.CostEstimate(flops=40_000_000_000, bytes_accessed=70_000_000, transcendentals=0),
        name="head",
    )(x, tgt, w_vocab)


TB = 768
NTOK = NDEV * N
NK = NTOK // TB
UN = 2
NOWN = (NVB + 1) // 2


def dwv_kernel(lo, hi, x_hbm, st_ref, w_hbm, *rest):
    dw_hbm, xv, xtv, wv, g0, g1, acc, lse, tgt, wsem, xsem, osem, ssem, rsem = rest[-14:]
    core = lax.rem(lax.axis_index("data"), 2)
    peer = lax.axis_index("data") + 1 - 2 * core

    barrier = pltpu.get_barrier_semaphore()
    pl.semaphore_signal(barrier, inc=1, device_id=(peer,), device_id_type=MESH)

    def block(i, side):
        return lo + i + side * (NVB - 1 - 2 * (lo + i))

    def cols(b):
        return pl.ds(pl.multiple_of(b * VB, VB), VB)

    def wcopy(i):
        buf = lax.rem(i, 2)
        return pltpu.make_async_copy(w_hbm.at[:, cols(block(i, core))], wv.at[buf], wsem.at[buf])

    def keep(i):
        buf = lax.rem(i, 2)
        return pltpu.make_async_copy(acc.at[buf], dw_hbm.at[:, cols(block(i, core))], osem.at[buf])

    def send(i, side):
        buf = lax.rem(i, 2)
        return pltpu.make_async_remote_copy(acc.at[buf], dw_hbm.at[:, cols(block(i, side))], ssem.at[buf], rsem.at[i],
                                            device_id=(peer,), device_id_type=MESH)

    def shared(i):
        return lo + i < NOWN - 1

    def done(i):
        keep(i).start()

        @pl.when(shared(i))
        def _():
            send(i, core).start()

    def drained(i):
        keep(i).wait()

        @pl.when(shared(i))
        def _():
            send(i, core).wait_send()

    n = hi - lo
    wcopy(0).start()
    cx = pltpu.make_async_copy(x_hbm, xv, xsem.at[0])
    cx.start()
    cx.wait()

    def turn(k, _):
        for c in range(0, TB, HB):
            rows = pl.ds(pl.multiple_of(k * TB + c, HB), HB)
            xtv[k, :, c:c + HB] = xv[rows, :].T
            lse[rows, :] = jnp.broadcast_to(st_ref[rows, 0:1], (HB, LANE))
            tgt[rows, :] = jnp.broadcast_to(st_ref[rows, LANE - 1:LANE], (HB, LANE))
        return 0

    lax.fori_loop(0, NK, turn, 0)
    pl.semaphore_wait(barrier, 1)

    def weight(it, gold, cols, reset=False):
        k, i = lax.rem(it + NK, NK), jnp.maximum(it, 0) // NK
        acc_c = acc.at[lax.rem(i, 2), :, cols]
        old = acc_c[...]
        acc_c[...] = (jnp.where(k == 0, 0.0, old) if reset else old) + dot(xtv[k], gold[:, cols])

    def step(it, u):
        gnew, gold = ((g0, g1), (g1, g0))[u % 2]
        k, i = lax.rem(it, NK) + u, it // NK
        base = pl.multiple_of(k * TB, TB)
        lane = lax.broadcasted_iota(jnp.int32, (R, LANE), 1) + block(i, core) * VB
        for c in range(0, VB, HB):
            lgt = dot(xv[pl.ds(base, TB), :], wv[lax.rem(i, 2), :, c:c + HB])
            weight(it + u - 1, gold, slice(c, c + HB), u == 1)
            ids = [jnp.tile((lane + (c + h)).astype(F32), (RB // R, 1)) for h in (0, LANE)]
            for r in range(0, TB, RB):
                here = pl.ds(pl.multiple_of(base + r, RB), RB)
                for h in (0, LANE):
                    p = jnp.exp(lgt[r:r + RB, h:h + LANE] - lse[here, :])
                    gnew[r:r + RB, c + h:c + h + LANE] = jnp.where(tgt[here, :] == ids[h // LANE], p - 1.0, p).astype(BF16)

    def body(h, _):
        it = UN * h
        i0, k0 = it // NK, lax.rem(it, NK)

        @pl.when(k0 == 0)
        def _():
            wcopy(i0).wait()

            @pl.when(i0 < n - 1)
            def _():
                wcopy(i0 + 1).start()

        @pl.when((k0 == 0) & (i0 >= 2))
        def _():
            drained(i0 - 2)

        for u in range(UN):
            step(it, u)

        @pl.when((k0 == UN) & (i0 >= 1))
        def _():
            done(i0 - 1)

        return 0

    lax.fori_loop(0, n * NK // UN, body, 0)

    def last(c, _):
        weight(jnp.int32(n * NK - 1), g1, pl.ds(pl.multiple_of(c * HB, HB), HB))
        return 0

    lax.fori_loop(0, VB // HB, last, 0)
    drained(n - 2)
    done(n - 1)
    drained(n - 1)
    for i in range(min(n, NOWN - 1 - lo)):
        send(i, 1 - core).wait_recv()


def grad_vocab(lo, hi, x_all, stats, w_vocab, before=()):
    return pl.pallas_call(
        functools.partial(dwv_kernel, lo, hi),
        out_shape=jax.ShapeDtypeStruct((H, V), F32),
        in_specs=[ANY, VMEM, ANY] + [ANY] * len(before),
        out_specs=ANY,
        input_output_aliases={3: 0} if before else {},
        scratch_shapes=[pltpu.VMEM((NTOK, H), BF16), pltpu.VMEM((NK, H, TB), BF16), pltpu.VMEM((2, H, VB), BF16)]
        + [pltpu.VMEM((TB, VB), BF16)] * 2
        + [pltpu.VMEM((2, H, VB), F32)] + [pltpu.VMEM((NTOK, LANE), F32)] * 2
        + [DMA((2,)), DMA((1,)), DMA((2,)), DMA((2,)), DMA((hi - lo,))],
        compiler_params=pltpu.CompilerParams(vmem_limit_bytes=48 * MIB, collective_id=2 + lo, has_side_effects=True),
        cost_estimate=pl.CostEstimate(flops=(hi - lo) * 20_000_000_000, bytes_accessed=100_000_000, transcendentals=0),
        name="dwv",
    )(x_all, stats, w_vocab, *before)


NC = 8


def copy_ring(n, src, dst, buf, isem, osem):
    def fetch(i):
        k = lax.rem(i, NC)
        return pltpu.make_async_copy(src(i), buf.at[k], isem.at[k])

    def put(i):
        k = lax.rem(i, NC)
        return pltpu.make_async_copy(buf.at[k], dst(i), osem.at[k])

    for i in range(NC // 2):
        fetch(i).start()

    def body(i, _):
        fetch(i).wait()
        put(i).start()

        @pl.when(i >= NC // 2)
        def _():
            put(i - NC // 2).wait()

        @pl.when(i + NC // 2 < n)
        def _():
            fetch(i + NC // 2).start()

        return 0

    lax.fori_loop(0, n, body, 0)
    for i in range(n - NC // 2, n):
        put(i).wait()


def copy_call(kernel, out, block, args, name):
    return pl.pallas_call(
        kernel,
        out_shape=jax.ShapeDtypeStruct(out, F32),
        in_specs=[ANY] * len(args),
        out_specs=ANY,
        input_output_aliases={1: 0} if len(args) > 1 else {},
        scratch_shapes=[pltpu.VMEM((NC,) + block, F32), DMA((NC,)), DMA((NC,))],
        compiler_params=pltpu.CompilerParams(vmem_limit_bytes=24 * MIB),
        cost_estimate=pl.CostEstimate(flops=20_000_000_000, bytes_accessed=130_000_000, transcendentals=0),
        name=name,
    )(*args)


def copy_dwv(v):
    rows = 2 * R

    def kernel(src, dst, *scratch):
        def at(ref):
            return lambda i: ref.at[pl.ds(pl.multiple_of(i * rows, rows), rows)]

        copy_ring(H // rows, at(src), at(dst), *scratch)

    return copy_call(kernel, (H, V), (rows, V), (v,), "copy_dwv")


def place_dw(quarter, parts, *before):
    def kernel(src, *rest):
        dst, scratch = rest[-4], rest[-3:]

        def target(i):
            return dst.at[lax.rem(i, S), pl.ds(pl.multiple_of(i // S * H + quarter * HB, HB), HB)]

        copy_ring(NDEV, lambda i: src.at[i], target, *scratch)

    return copy_call(kernel, (L, 2 * H, G4), (HB, G4), (parts,) + before, "place_dw")


SPLITS = (0, 2, 4, NOWN)


def solution(mesh):
    def local_grads(x_rows, tgt_rows, w_lstm, b_lstm, w_vocab):
        tgt = jnp.swapaxes(tgt_rows, 0, 1).reshape(N, 1)
        gates, cprev, hprev, xs, top = forward(jnp.swapaxes(x_rows, 0, 1), w_lstm, b_lstm)
        top = top.reshape(N, H)
        d_top, lse = head(top, tgt, w_vocab)
        half = (N, LANE // 2)
        stats = jnp.concatenate([jnp.broadcast_to(lse, half), jnp.broadcast_to(tgt.astype(F32), half)], axis=1)
        x_all = lax.all_gather(top, 'data', axis=0, tiled=True)
        stats = lax.all_gather(stats, 'data', axis=0, tiled=True)
        d_top, x_all = lax.optimization_barrier((d_top, x_all))
        *halves, db, dx = backward(d_top.reshape(T, R, H), gates, cprev, hprev, xs, w_lstm)
        db = lax.all_gather(db, 'data', axis=0).reshape(NDEV // S, S, R, G4)
        swap = [(i, (i + S) % NDEV) for i in range(NDEV)]
        dwv, gathered = (), []
        for i in range(2):
            own, give = halves[i], halves[2 + i]
            if i:
                give, part = lax.optimization_barrier((give, part))
            got = lax.ppermute(give, 'data', swap)
            dwv = grad_vocab(SPLITS[i], SPLITS[i + 1], x_all, stats, w_vocab, dwv)
            own, dwv = lax.optimization_barrier((own, dwv))
            part, dwv = lax.optimization_barrier((own + got, dwv))
            gathered.append(lax.all_gather(part, 'data', axis=0))
            dwv = (dwv,)
        dwv = copy_dwv(grad_vocab(SPLITS[2], SPLITS[3], x_all, stats, w_vocab, dwv))
        dw = place_dw(1, gathered[1], place_dw(0, gathered[0]))
        db = jnp.sum(db, axis=(0, 2))
        return dw, db, dwv, jnp.swapaxes(dx, 0, 1)

    return jax.shard_map(local_grads, mesh=mesh, in_specs=(P('data'), P('data'), P(), P(), P()), out_specs=(P(), P(), P(), P('data')), check_vma=False)
```

```python
import functools

import jax
import jax.numpy as jnp
from jax import lax
from jax.experimental import pallas as pl
from jax.experimental.pallas import tpu as pltpu
from jax.sharding import PartitionSpec as P

T = 48
R = 8
S = 8
Q = S * R
H = 512
HB = 256
G4 = 4 * H
L = 8
V = 32000
LANE = 128
NDEV = 16
CH = 4
NR = 6
F32 = jnp.float32
BF16 = jnp.bfloat16
MESH = pl.DeviceIdType.MESH
MIB = 1024 * 1024
ANY = pl.BlockSpec(memory_space=pl.ANY)
VMEM = pl.BlockSpec(memory_space=pltpu.VMEM)
HBM = pl.BlockSpec(memory_space=pltpu.HBM)
DMA = pltpu.SemaphoreType.DMA


def dot(a, b):
    return jnp.dot(a, b, preferred_element_type=F32)


def dot_tt(a, b):
    return lax.dot_general(a, b, (((1,), (1,)), ((), ())), preferred_element_type=F32)


def gray(k):
    chip, core = k // 2, k % 2
    hi, lo = chip // 2, chip % 2
    return 2 * (chip + hi - 2 * hi * lo) + core


LAST = gray(S - 1)


def place():
    me = lax.axis_index("data")
    index = lax.rem(me, S)
    return me - index, index, gray(index)


def plane_signal(base, index):
    barrier = pltpu.get_barrier_semaphore()
    for i in range(1, S):
        pl.semaphore_signal(barrier, inc=1, device_id=(base + lax.rem(index + i, S),), device_id_type=MESH)


def plane_wait():
    pl.semaphore_wait(pltpu.get_barrier_semaphore(), S - 1)


def rows_of(v):
    return v.reshape(Q, v.shape[-1])


def groups_of(v):
    return v.reshape(S, R, v.shape[-1])


def fwd_kernel(x_hbm, w_hbm, b_ref, gates_hbm, cp_hbm, hp_hbm, xs_hbm, xl_hbm,
               w, xbuf, xout, gates, cprev, hprev, z0, z1, wsem, insem, recv, send, lastsem, osem):
    base, index, stage = place()
    first, last = stage == 0, stage == S - 1
    nxt = base + gray(lax.rem(stage + 1, S))
    plane_signal(base, index)
    wcopy = pltpu.make_async_copy(w_hbm.at[stage], w, wsem.at[0])
    wcopy.start()
    plane_wait()

    def feed(k):
        ts = pl.ds(k * CH, CH)

        @pl.when(first)
        def _():
            pltpu.make_async_copy(x_hbm.at[ts], xbuf.at[ts, 0], recv.at[k * CH]).start()

        @pl.when(jnp.logical_not(first))
        def _():
            pltpu.make_async_remote_copy(x_hbm.at[ts], xbuf.at[ts, index], insem, recv.at[k * CH],
                                         device_id=(base,), device_id_type=MESH).start()

        return 0

    def step_out(t):
        return pltpu.make_async_remote_copy(xout.at[t], xbuf.at[t], send, recv.at[t], device_id=(nxt,), device_id_type=MESH)

    def final_out(t, i):
        ts = pl.ds(t, CH)
        if i == LAST:
            return pltpu.make_async_copy(xout.at[ts, i], xl_hbm.at[ts], lastsem)
        return pltpu.make_async_remote_copy(xout.at[ts, i], xl_hbm.at[ts], send, lastsem, device_id=(base + i,), device_id_type=MESH)

    def arrived(t):
        @pl.when(jnp.logical_not(first))
        def _():
            step_out(t).wait_recv()

        @pl.when(first & (lax.rem(t, CH) == 0))
        def _():
            ts = pl.ds(t, CH)
            pltpu.make_async_remote_copy(xout.at[ts], xbuf.at[ts], send, recv.at[t], device_id=(nxt,), device_id_type=MESH).wait_recv()

    def pass_on(t):
        @pl.when(jnp.logical_not(last))
        def _():
            step_out(t).start()

        @pl.when(last & (lax.rem(t, CH) == CH - 1))
        def _():
            for i in range(S):
                final_out(t - CH + 1, i).start()

    lax.fori_loop(0, T // CH, lambda k, _: feed(k), 0)
    bias = b_ref[pl.ds(stage, 1), :]

    def project(zref, t):
        xt = rows_of(xbuf[t].astype(F32)).astype(BF16)
        for n in range(0, G4, HB):
            zref[:, n:n + HB] = dot(xt, w[0:H, n:n + HB]) + bias[:, n:n + HB]

    wcopy.wait()
    arrived(jnp.int32(0))
    project(z0, 0)

    kept = ((gates, gates_hbm), (cprev, cp_hbm), (hprev, hp_hbm), (xbuf, xs_hbm))

    def save(t):
        for i, (src, dst) in enumerate(kept):
            pltpu.make_async_copy(src.at[t], dst.at[t], osem.at[i]).start()

    def two(p, state):
        for u in range(2):
            t = 2 * p + u
            zc, zn = ((z0, z1), (z1, z0))[u]

            @pl.when(t > 0)
            def _():
                pass_on(t - 1)
                save(t - 1)

            @pl.when(t + 1 < T)
            def _():
                arrived(t + 1)

            ha, hc, ca, cc = state
            hlow = jnp.concatenate([ha, hc], axis=1).astype(BF16)
            hprev[t] = hlow
            cprev[t, :, 0:HB] = ca
            cprev[t, :, HB:H] = cc
            nh, nc = [], []
            for q in range(2):
                zz = []
                for g in range(4):
                    cols = slice(g * H + q * HB, g * H + q * HB + HB)
                    zz.append(zc[:, cols] + dot(hlow, w[H:2 * H, cols]))
                gi, gf, gg, go = jax.nn.sigmoid(zz[0]), jax.nn.sigmoid(zz[1]), jnp.tanh(zz[2]), jax.nn.sigmoid(zz[3])
                cn = gf * (ca, cc)[q] + gi * gg
                nh.append(go * jnp.tanh(cn))
                nc.append(cn)
                for g, val in enumerate((gi, gf, gg, go)):
                    gates[t, :, g * H + q * HB:g * H + q * HB + HB] = val
            project(zn, jnp.minimum(t + 1, T - 1))
            xt = rows_of(xbuf[t].astype(F32))
            xout[t] = groups_of(xt + jnp.concatenate(nh, axis=1)).astype(BF16)
            state = (nh[0], nh[1], nc[0], nc[1])
        return state

    zero = jnp.zeros((Q, HB), F32)
    lax.fori_loop(0, T // 2, two, (zero,) * 4)
    pass_on(jnp.int32(T - 1))
    save(T - 1)
    for i, (src, dst) in enumerate(kept):
        pltpu.make_async_copy(src, dst, osem.at[i]).wait()

    @pl.when(jnp.logical_not(first))
    def _():
        pltpu.make_async_remote_copy(x_hbm, xl_hbm, insem, lastsem, device_id=(base,), device_id_type=MESH).wait_send()

    @pl.when(jnp.logical_not(last))
    def _():
        pltpu.make_async_remote_copy(xout, xbuf, send, recv.at[0], device_id=(nxt,), device_id_type=MESH).wait_send()

    @pl.when(last)
    def _():
        others = (slice(None), slice(0, S - 1))
        pltpu.make_async_remote_copy(xout.at[others], xbuf.at[others], send, recv.at[0], device_id=(nxt,), device_id_type=MESH).wait_send()

    pltpu.make_async_copy(x_hbm, xl_hbm, lastsem).wait()


def forward(x, w, b):
    return pl.pallas_call(
        fwd_kernel,
        out_shape=(jax.ShapeDtypeStruct((T, Q, G4), F32), jax.ShapeDtypeStruct((T, Q, H), F32),
                   jax.ShapeDtypeStruct((T, Q, H), BF16), jax.ShapeDtypeStruct((T, S, R, H), BF16),
                   jax.ShapeDtypeStruct((T, R, H), BF16)),
        in_specs=[ANY, ANY, VMEM],
        out_specs=(HBM,) * 5,
        scratch_shapes=[pltpu.VMEM((2 * H, G4), BF16), pltpu.VMEM((T, S, R, H), BF16), pltpu.VMEM((T, S, R, H), BF16),
                        pltpu.VMEM((T, Q, G4), F32), pltpu.VMEM((T, Q, H), F32), pltpu.VMEM((T, Q, H), BF16)]
        + [pltpu.VMEM((Q, G4), F32)] * 2 + [DMA((1,)), DMA, DMA((T,)), DMA, DMA, DMA((4,))],
        compiler_params=pltpu.CompilerParams(vmem_limit_bytes=52 * MIB, collective_id=0, has_side_effects=True),
        cost_estimate=pl.CostEstimate(flops=60_000_000_000, bytes_accessed=80_000_000, transcendentals=0),
        name="lstm_fwd",
    )(x, w, b)


def bwd_kernel(d_hbm, gates_hbm, cp_hbm, hp_hbm, xs_hbm, w_hbm, own0, own1, give0, give1, db_ref, dx_hbm,
               w, wt, dbuf, dout, dall, ut, acc, gin, cin, hin, xin,
               wsem, insem, recv, send, lastsem, isem, osem):
    base, index, stage = place()
    plane = base // S
    first, last = stage == 0, stage == S - 1
    prv = base + gray(lax.rem(stage + S - 1, S))
    top = base + LAST
    plane_signal(base, index)
    wcopy = pltpu.make_async_copy(w_hbm.at[stage], w, wsem.at[0])
    wcopy.start()

    def feed(k):
        t = T - CH - k * CH
        ts = pl.ds(t, CH)

        @pl.when(last)
        def _():
            pltpu.make_async_copy(d_hbm.at[ts], dbuf.at[ts, LAST], recv.at[t]).start()

        @pl.when(jnp.logical_not(last))
        def _():
            pltpu.make_async_remote_copy(d_hbm.at[ts], dbuf.at[ts, index], insem, recv.at[t],
                                         device_id=(top,), device_id_type=MESH).start()

        return 0

    def step_out(t):
        return pltpu.make_async_remote_copy(dout.at[t], dbuf.at[t], send, recv.at[t], device_id=(prv,), device_id_type=MESH)

    def final_out(t, i):
        ts = pl.ds(t, CH)
        if i == 0:
            return pltpu.make_async_copy(dout.at[ts, i], dx_hbm.at[ts], lastsem)
        return pltpu.make_async_remote_copy(dout.at[ts, i], dx_hbm.at[ts], send, lastsem, device_id=(base + i,), device_id_type=MESH)

    def arrived(t):
        @pl.when(jnp.logical_not(last))
        def _():
            step_out(t).wait_recv()

        @pl.when(last & (lax.rem(t, CH) == CH - 1))
        def _():
            ts = pl.ds(t - CH + 1, CH)
            pltpu.make_async_remote_copy(dout.at[ts], dbuf.at[ts], send, recv.at[t - CH + 1], device_id=(prv,), device_id_type=MESH).wait_recv()

    def pass_on(t):
        @pl.when(jnp.logical_not(first))
        def _():
            step_out(t).start()

        @pl.when(first & (lax.rem(t, CH) == 0))
        def _():
            for i in range(S):
                final_out(t, i).start()

    def loads(t):
        k = lax.rem(t, NR)
        return [pltpu.make_async_copy(src.at[t], dst.at[k], isem.at[k, i])
                for i, (src, dst) in enumerate(((gates_hbm, gin), (cp_hbm, cin), (hp_hbm, hin), (xs_hbm, xin)))]

    for t in range(T - NR, T):
        for cp in loads(t):
            cp.start()
    plane_wait()
    lax.fori_loop(0, T // CH, lambda k, _: feed(k), 0)
    db_ref[...] = jnp.zeros(db_ref.shape, F32)
    acc[...] = jnp.zeros(acc.shape, F32)
    wcopy.wait()

    def turn(n, _):
        cols = pl.ds(pl.multiple_of(n * HB, HB), HB)
        wt[cols, :] = w[:, cols].T
        return 0

    lax.fori_loop(0, G4 // HB, turn, 0)

    def weight():
        for n in range(0, G4, HB):
            acc[:, n:n + HB] += dot(ut[...], dall[:, n:n + HB])

    def two(n, state):
        p = T // 2 - 1 - n
        us = []
        for u in (1, 0):
            t = 2 * p + u
            k = lax.rem(t, NR)
            for cp in loads(t):
                cp.wait()

            @pl.when(t < T - 1)
            def _():
                pass_on(t + 1)

            if u == 1:
                @pl.when((p < T // 2 - 1) & (lax.rem(p, CH // 2) == CH // 2 - 1))
                def _():
                    weight()

            arrived(t)
            ea, ec, da, dc_ = state
            dext = rows_of(dbuf[t])
            parts = [[None, None] for _ in range(4)]
            nd = []
            for q in range(2):
                gi, gf, gg, go = (gin[k, :, g * H + q * HB:g * H + q * HB + HB] for g in range(4))
                hq = slice(q * HB, q * HB + HB)
                cprev = cin[k, :, hq]
                th = jnp.tanh(gf * cprev + gi * gg)
                e = dext[:, hq] + (ea, ec)[q]
                dc = (da, dc_)[q] + e * (go * (1.0 - th * th))
                parts[0][q] = dc * (gg * gi * (1.0 - gi))
                parts[1][q] = dc * (cprev * gf * (1.0 - gf))
                parts[2][q] = dc * (gi * (1.0 - gg * gg))
                parts[3][q] = e * (th * go * (1.0 - go))
                nd.append(dc * gf)
            trows = pl.ds(pl.multiple_of(lax.rem(t, CH) * Q, Q), Q)
            lows = []
            for i, v in enumerate(v for ps in parts for v in ps):
                cols = slice(i * HB, i * HB + HB)
                low = v.astype(BF16)
                dall[trows, cols] = low
                lows.append(low)
                db_ref[:, cols] += jnp.sum(v.reshape(Q // R, R, HB), axis=0)
            lowz = jnp.concatenate(lows, axis=1)
            ne = [dot(lowz, wt[:, H + q * HB:H + q * HB + HB]) for q in range(2)]
            for q in range(2):
                hq = slice(q * HB, q * HB + HB)
                dout[t, :, :, hq] = groups_of(dext[:, hq] + dot(lowz, wt[:, hq]))
            state = (ne[0], ne[1], nd[0], nd[1])
            us.append((rows_of(xin[k].astype(F32)), hin[k].astype(F32)))

            @pl.when(t >= NR)
            def _():
                for cp in loads(t - NR):
                    cp.start()

        tcols = pl.ds(pl.multiple_of(lax.rem(p, CH // 2) * 2 * Q, 2 * Q), 2 * Q)
        for j in range(2):
            ut[j * H:j * H + H, tcols] = jnp.concatenate([us[1][j], us[0][j]], axis=0).T.astype(BF16)

        return state

    zero = jnp.zeros((Q, HB), F32)
    lax.fori_loop(0, T // 2, two, (zero,) * 4)
    pass_on(jnp.int32(0))

    weight()
    outs = []
    for i, (dst, m, at) in enumerate(((give0, 0, 1 - plane), (give1, HB, 1 - plane), (own0, 0, plane), (own1, HB, plane))):
        outs.append(pltpu.make_async_copy(acc.at[pl.ds(pl.multiple_of(at * H + m, HB), HB)], dst, osem.at[i]))
        outs[i].start()
    for out in outs:
        out.wait()

    @pl.when(jnp.logical_not(last))
    def _():
        pltpu.make_async_remote_copy(d_hbm, dx_hbm, insem, lastsem, device_id=(top,), device_id_type=MESH).wait_send()

    @pl.when(jnp.logical_not(first))
    def _():
        pltpu.make_async_remote_copy(dout, dbuf, send, recv.at[0], device_id=(prv,), device_id_type=MESH).wait_send()

    @pl.when(first)
    def _():
        others = (slice(None), slice(1, S))
        pltpu.make_async_remote_copy(dout.at[others], dbuf.at[others], send, recv.at[0], device_id=(prv,), device_id_type=MESH).wait_send()

    pltpu.make_async_copy(d_hbm, dx_hbm, lastsem).wait()


def backward(d_top, gates, cprev, hprev, xs, w):
    return pl.pallas_call(
        bwd_kernel,
        out_shape=(jax.ShapeDtypeStruct((HB, G4), F32),) * 4 + (jax.ShapeDtypeStruct((R, G4), F32), jax.ShapeDtypeStruct((T, R, H), F32)),
        in_specs=[ANY] * 6,
        out_specs=(HBM,) * 4 + (VMEM, HBM),
        scratch_shapes=[pltpu.VMEM((2 * H, G4), BF16), pltpu.VMEM((G4, 2 * H), BF16), pltpu.VMEM((T, S, R, H), F32),
                        pltpu.VMEM((T, S, R, H), F32), pltpu.VMEM((CH * Q, G4), BF16), pltpu.VMEM((2 * H, CH * Q), BF16), pltpu.VMEM((2 * H, G4), F32)]
        + [pltpu.VMEM((NR, Q, G4), F32), pltpu.VMEM((NR, Q, H), F32), pltpu.VMEM((NR, Q, H), BF16), pltpu.VMEM((NR, S, R, H), BF16)]
        + [DMA((1,)), DMA, DMA((T,)), DMA, DMA, DMA((NR, 4)), DMA((4,))],
        compiler_params=pltpu.CompilerParams(vmem_limit_bytes=56 * MIB, collective_id=1, has_side_effects=True),
        cost_estimate=pl.CostEstimate(flops=110_000_000_000, bytes_accessed=80_000_000, transcendentals=0),
        name="lstm_bwd",
    )(d_top, gates, cprev, hprev, xs, w)


VB = 1280
NVB = V // VB
N = T * R
NW = 4
RB = 64


def head_kernel(x_ref, t_ref, w_hbm, dx_ref, lse_ref, lg, g0, g1, wv, mx, sm, tb, wsem):
    def wcopy(b):
        buf = lax.rem(b, NW)
        return pltpu.make_async_copy(w_hbm.at[:, pl.ds(pl.multiple_of(lax.rem(b, NVB) * VB, VB), VB)], wv.at[buf], wsem.at[buf])

    for b in range(NW - 1):
        wcopy(b).start()

    def ready(b):
        for i in range(2):
            wcopy(b + i).wait()
            wcopy(b + i + 2).start()

    mx[...] = jnp.full(mx.shape, -jnp.inf, F32)
    sm[...] = jnp.zeros(sm.shape, F32)
    dx_ref[...] = jnp.zeros(dx_ref.shape, F32)

    def logits(b):
        for c in range(0, VB, HB):
            lg[b, :, c:c + HB] = dot(x_ref[...], wv[lax.rem(b, NW), :, c:c + HB])

    def sums(b):
        for r in range(0, N, RB):
            rows = slice(r, r + RB)
            m_old = mx[rows, :]
            m_new = m_old
            for c in range(0, VB, LANE):
                m_new = jnp.maximum(m_new, lg[b, rows, c:c + LANE])
            acc = sm[rows, :] * jnp.exp(m_old - m_new)
            for c in range(0, VB, LANE):
                acc = acc + jnp.exp(lg[b, rows, c:c + LANE] - m_new)
            mx[rows, :] = m_new
            sm[rows, :] = acc

    wcopy(0).wait()
    logits(0)

    def first(h, _):
        b = 2 * h + 1
        ready(b)
        for i in range(2):
            logits(b + i)
            sums(b + i - 1)
        return 0

    lax.fori_loop(0, NVB // 2, first, 0)
    sums(NVB - 1)
    for r in range(0, N, LANE):
        rows = slice(r, r + LANE)
        top = jnp.max(mx[rows, :], axis=1, keepdims=True)
        tot = jnp.sum(sm[rows, :] * jnp.exp(mx[rows, :] - top), axis=1, keepdims=True)
        lse = top + jnp.log(tot)
        lse_ref[rows, :] = lse
        mx[rows, :] = jnp.broadcast_to(lse, (LANE, LANE))
        tb[rows, :] = jnp.broadcast_to(t_ref[rows, :], (LANE, LANE))

    def grads(b, gb, c):
        ids = b * VB + c + lax.broadcasted_iota(jnp.int32, (RB, LANE), 1)
        for r in range(0, N, RB):
            rows = slice(r, r + RB)
            lse = mx[rows, :]
            tgt = tb[rows, :] - ids
            for h in (0, LANE):
                p = jnp.exp(lg[b, rows, c + h:c + h + LANE] - lse)
                gb[rows, c + h:c + h + LANE] = jnp.where(tgt == h, p - 1.0, p).astype(BF16)

    def apply(b, gb, c):
        return dot_tt(gb[:, c:c + HB], wv[lax.rem(b + NVB, NW), :, c:c + HB])

    for c in range(0, VB, HB):
        grads(0, g0, c)

    def second(h, _):
        for i in range(2):
            b = 2 * h + NVB + i
            wcopy(b).wait()

            @pl.when(b + 2 < 2 * NVB)
            def _():
                wcopy(b + 2).start()

        for b, gb, gn in ((2 * h, g0, g1), (2 * h + 1, g1, g0)):
            total = jnp.zeros((N, H), F32)
            for c in range(0, VB, HB):
                total = total + apply(b, gb, c)
                grads(b + 1, gn, c)
            dx_ref[...] += total
        return 0

    lax.fori_loop(0, NVB // 2, second, 0)
    wcopy(2 * NVB - 1).wait()
    for c in range(0, VB, HB):
        dx_ref[...] += apply(NVB - 1, g0, c)


def head(x, tgt, w_vocab):
    return pl.pallas_call(
        head_kernel,
        out_shape=(jax.ShapeDtypeStruct((N, H), F32), jax.ShapeDtypeStruct((N, 1), F32)),
        in_specs=[VMEM, VMEM, ANY],
        out_specs=(VMEM, VMEM),
        scratch_shapes=[pltpu.VMEM((NVB, N, VB), F32), pltpu.VMEM((N, VB), BF16), pltpu.VMEM((N, VB), BF16), pltpu.VMEM((NW, H, VB), BF16),
                        pltpu.VMEM((N, LANE), F32), pltpu.VMEM((N, LANE), F32), pltpu.VMEM((N, LANE), jnp.int32), DMA((NW,))],
        compiler_params=pltpu.CompilerParams(vmem_limit_bytes=60 * MIB),
        cost_estimate=pl.CostEstimate(flops=40_000_000_000, bytes_accessed=70_000_000, transcendentals=0),
        name="head",
    )(x, tgt, w_vocab)


TB = 768
NTOK = NDEV * N
NK = NTOK // TB
UN = 2
NOWN = (NVB + 1) // 2


def dwv_kernel(lo, hi, x_hbm, st_ref, w_hbm, *rest):
    dw_hbm, xv, xtv, wv, g0, g1, acc, lse, tgt, wsem, xsem, osem, ssem, rsem = rest[-14:]
    core = lax.rem(lax.axis_index("data"), 2)
    peer = lax.axis_index("data") + 1 - 2 * core

    barrier = pltpu.get_barrier_semaphore()
    pl.semaphore_signal(barrier, inc=1, device_id=(peer,), device_id_type=MESH)

    def block(i, side):
        return lo + i + side * (NVB - 1 - 2 * (lo + i))

    def cols(b):
        return pl.ds(pl.multiple_of(b * VB, VB), VB)

    def wcopy(i):
        buf = lax.rem(i, 2)
        return pltpu.make_async_copy(w_hbm.at[:, cols(block(i, core))], wv.at[buf], wsem.at[buf])

    def keep(i):
        buf = lax.rem(i, 2)
        return pltpu.make_async_copy(acc.at[buf], dw_hbm.at[:, cols(block(i, core))], osem.at[buf])

    def send(i, side):
        buf = lax.rem(i, 2)
        return pltpu.make_async_remote_copy(acc.at[buf], dw_hbm.at[:, cols(block(i, side))], ssem.at[buf], rsem.at[i],
                                            device_id=(peer,), device_id_type=MESH)

    def shared(i):
        return lo + i < NOWN - 1

    def done(i):
        keep(i).start()

        @pl.when(shared(i))
        def _():
            send(i, core).start()

    def drained(i):
        keep(i).wait()

        @pl.when(shared(i))
        def _():
            send(i, core).wait_send()

    n = hi - lo
    wcopy(0).start()
    cx = pltpu.make_async_copy(x_hbm, xv, xsem.at[0])
    cx.start()
    cx.wait()

    def turn(k, _):
        for c in range(0, TB, HB):
            rows = pl.ds(pl.multiple_of(k * TB + c, HB), HB)
            xtv[k, :, c:c + HB] = xv[rows, :].T
            lse[rows, :] = jnp.broadcast_to(st_ref[rows, 0:1], (HB, LANE))
            tgt[rows, :] = jnp.broadcast_to(st_ref[rows, LANE - 1:LANE], (HB, LANE))
        return 0

    lax.fori_loop(0, NK, turn, 0)
    pl.semaphore_wait(barrier, 1)

    def weight(it, gold, cols, reset=False):
        k, i = lax.rem(it + NK, NK), jnp.maximum(it, 0) // NK
        acc_c = acc.at[lax.rem(i, 2), :, cols]
        old = acc_c[...]
        acc_c[...] = (jnp.where(k == 0, 0.0, old) if reset else old) + dot(xtv[k], gold[:, cols])

    def step(it, u):
        gnew, gold = ((g0, g1), (g1, g0))[u % 2]
        k, i = lax.rem(it, NK) + u, it // NK
        base = pl.multiple_of(k * TB, TB)
        lane = lax.broadcasted_iota(jnp.int32, (R, LANE), 1) + block(i, core) * VB
        for c in range(0, VB, HB):
            lgt = dot(xv[pl.ds(base, TB), :], wv[lax.rem(i, 2), :, c:c + HB])
            weight(it + u - 1, gold, slice(c, c + HB), u == 1)
            ids = [jnp.tile((lane + (c + h)).astype(F32), (RB // R, 1)) for h in (0, LANE)]
            for r in range(0, TB, RB):
                here = pl.ds(pl.multiple_of(base + r, RB), RB)
                for h in (0, LANE):
                    p = jnp.exp(lgt[r:r + RB, h:h + LANE] - lse[here, :])
                    gnew[r:r + RB, c + h:c + h + LANE] = jnp.where(tgt[here, :] == ids[h // LANE], p - 1.0, p).astype(BF16)

    def body(h, _):
        it = UN * h
        i0, k0 = it // NK, lax.rem(it, NK)

        @pl.when(k0 == 0)
        def _():
            wcopy(i0).wait()

            @pl.when(i0 < n - 1)
            def _():
                wcopy(i0 + 1).start()

        @pl.when((k0 == 0) & (i0 >= 2))
        def _():
            drained(i0 - 2)

        for u in range(UN):
            step(it, u)

        @pl.when((k0 == UN) & (i0 >= 1))
        def _():
            done(i0 - 1)

        return 0

    lax.fori_loop(0, n * NK // UN, body, 0)

    def last(c, _):
        weight(jnp.int32(n * NK - 1), g1, pl.ds(pl.multiple_of(c * HB, HB), HB))
        return 0

    lax.fori_loop(0, VB // HB, last, 0)
    drained(n - 2)
    done(n - 1)
    drained(n - 1)
    for i in range(min(n, NOWN - 1 - lo)):
        send(i, 1 - core).wait_recv()


def grad_vocab(lo, hi, x_all, stats, w_vocab, before=()):
    return pl.pallas_call(
        functools.partial(dwv_kernel, lo, hi),
        out_shape=jax.ShapeDtypeStruct((H, V), F32),
        in_specs=[ANY, VMEM, ANY] + [ANY] * len(before),
        out_specs=ANY,
        input_output_aliases={3: 0} if before else {},
        scratch_shapes=[pltpu.VMEM((NTOK, H), BF16), pltpu.VMEM((NK, H, TB), BF16), pltpu.VMEM((2, H, VB), BF16)]
        + [pltpu.VMEM((TB, VB), BF16)] * 2
        + [pltpu.VMEM((2, H, VB), F32)] + [pltpu.VMEM((NTOK, LANE), F32)] * 2
        + [DMA((2,)), DMA((1,)), DMA((2,)), DMA((2,)), DMA((hi - lo,))],
        compiler_params=pltpu.CompilerParams(vmem_limit_bytes=48 * MIB, collective_id=2 + lo, has_side_effects=True),
        cost_estimate=pl.CostEstimate(flops=(hi - lo) * 20_000_000_000, bytes_accessed=100_000_000, transcendentals=0),
        name="dwv",
    )(x_all, stats, w_vocab, *before)


NC = 8


def copy_ring(n, src, dst, buf, isem, osem):
    def fetch(i):
        k = lax.rem(i, NC)
        return pltpu.make_async_copy(src(i), buf.at[k], isem.at[k])

    def put(i):
        k = lax.rem(i, NC)
        return pltpu.make_async_copy(buf.at[k], dst(i), osem.at[k])

    for i in range(NC // 2):
        fetch(i).start()

    def body(i, _):
        fetch(i).wait()
        put(i).start()

        @pl.when(i >= NC // 2)
        def _():
            put(i - NC // 2).wait()

        @pl.when(i + NC // 2 < n)
        def _():
            fetch(i + NC // 2).start()

        return 0

    lax.fori_loop(0, n, body, 0)
    for i in range(n - NC // 2, n):
        put(i).wait()


def copy_call(kernel, out, block, args, name):
    return pl.pallas_call(
        kernel,
        out_shape=jax.ShapeDtypeStruct(out, F32),
        in_specs=[ANY] * len(args),
        out_specs=ANY,
        input_output_aliases={1: 0} if len(args) > 1 else {},
        scratch_shapes=[pltpu.VMEM((NC,) + block, F32), DMA((NC,)), DMA((NC,))],
        compiler_params=pltpu.CompilerParams(vmem_limit_bytes=24 * MIB),
        cost_estimate=pl.CostEstimate(flops=20_000_000_000, bytes_accessed=130_000_000, transcendentals=0),
        name=name,
    )(*args)


def copy_dwv(v):
    rows = 2 * R

    def kernel(src, dst, *scratch):
        def at(ref):
            return lambda i: ref.at[pl.ds(pl.multiple_of(i * rows, rows), rows)]

        copy_ring(H // rows, at(src), at(dst), *scratch)

    return copy_call(kernel, (H, V), (rows, V), (v,), "copy_dwv")


def place_dw(quarter, parts, *before):
    def kernel(src, *rest):
        dst, scratch = rest[-4], rest[-3:]

        def target(i):
            return dst.at[gray(lax.rem(i, S)), pl.ds(pl.multiple_of(i // S * H + quarter * HB, HB), HB)]

        copy_ring(NDEV, lambda i: src.at[i], target, *scratch)

    return copy_call(kernel, (L, 2 * H, G4), (HB, G4), (parts,) + before, "place_dw")


SPLITS = (0, 2, 7, NOWN)


def solution(mesh):
    def local_grads(x_rows, tgt_rows, w_lstm, b_lstm, w_vocab):
        tgt = jnp.swapaxes(tgt_rows, 0, 1).reshape(N, 1)
        gates, cprev, hprev, xs, top = forward(jnp.swapaxes(x_rows, 0, 1), w_lstm, b_lstm)
        top = top.reshape(N, H)
        d_top, lse = head(top, tgt, w_vocab)
        half = (N, LANE // 2)
        stats = jnp.concatenate([jnp.broadcast_to(lse, half), jnp.broadcast_to(tgt.astype(F32), half)], axis=1)
        x_all = lax.all_gather(top, 'data', axis=0, tiled=True)
        stats = lax.all_gather(stats, 'data', axis=0, tiled=True)
        d_top, x_all = lax.optimization_barrier((d_top, x_all))
        *halves, db, dx = backward(d_top.reshape(T, R, H), gates, cprev, hprev, xs, w_lstm)
        db = lax.all_gather(db, 'data', axis=0).reshape(NDEV // S, S, R, G4)
        swap = [(i, (i + S) % NDEV) for i in range(NDEV)]
        dwv, gathered = (), []
        for i in range(2):
            own, give = halves[i], halves[2 + i]
            if i:
                give, part = lax.optimization_barrier((give, part))
            got = lax.ppermute(give, 'data', swap)
            dwv = grad_vocab(SPLITS[i], SPLITS[i + 1], x_all, stats, w_vocab, dwv)
            own, dwv = lax.optimization_barrier((own, dwv))
            part, dwv = lax.optimization_barrier((own + got, dwv))
            gathered.append(lax.all_gather(part, 'data', axis=0))
            dwv = (dwv,)
        dwv = copy_dwv(grad_vocab(SPLITS[2], SPLITS[3], x_all, stats, w_vocab, dwv))
        dw = place_dw(1, gathered[1], place_dw(0, gathered[0]))
        db = jnp.sum(db, axis=(0, 2))
        db = jnp.stack([db[gray(i)] for i in range(L)])
        return dw, db, dwv, jnp.swapaxes(dx, 0, 1)

    return jax.shard_map(local_grads, mesh=mesh, in_specs=(P('data'), P('data'), P(), P(), P()), out_specs=(P(), P(), P(), P('data')), check_vma=False)
```

```python
import functools

import jax
import jax.numpy as jnp
from jax import lax
from jax.experimental import pallas as pl
from jax.experimental.pallas import tpu as pltpu
from jax.sharding import PartitionSpec as P

T = 48
R = 8
S = 8
Q = S * R
H = 512
HB = 256
G4 = 4 * H
L = 8
V = 32000
LANE = 128
NDEV = 16
CH = 4
NR = 6
PIECES = ((0, 128), (128, 256), (384, 128))
F32 = jnp.float32
BF16 = jnp.bfloat16
MESH = pl.DeviceIdType.MESH
MIB = 1024 * 1024
ANY = pl.BlockSpec(memory_space=pl.ANY)
VMEM = pl.BlockSpec(memory_space=pltpu.VMEM)
HBM = pl.BlockSpec(memory_space=pltpu.HBM)
DMA = pltpu.SemaphoreType.DMA


def dot(a, b):
    return jnp.dot(a, b, preferred_element_type=F32)


def dot_tt(a, b):
    return lax.dot_general(a, b, (((1,), (1,)), ((), ())), preferred_element_type=F32)


def gray(k):
    chip, core = k // 2, k % 2
    hi, lo = chip // 2, chip % 2
    return 2 * (chip + hi - 2 * hi * lo) + core


LAST = gray(S - 1)


def place():
    me = lax.axis_index("data")
    index = lax.rem(me, S)
    return me - index, index, gray(index)


def plane_signal(base, index):
    barrier = pltpu.get_barrier_semaphore()
    for i in range(1, S):
        pl.semaphore_signal(barrier, inc=1, device_id=(base + lax.rem(index + i, S),), device_id_type=MESH)


def plane_wait():
    pl.semaphore_wait(pltpu.get_barrier_semaphore(), S - 1)


def rows_of(v):
    return v.reshape(Q, v.shape[-1])


def groups_of(v):
    return v.reshape(S, R, v.shape[-1])


def fwd_kernel(x_hbm, w_hbm, b_ref, gates_hbm, cp_hbm, hp_hbm, xs_hbm, xl_hbm,
               w, xbuf, xout, gates, cprev, hprev, z0, z1, wsem, insem, recv, send, lastsem, osem):
    base, index, stage = place()
    first, last = stage == 0, stage == S - 1
    nxt = base + gray(lax.rem(stage + 1, S))
    plane_signal(base, index)
    wcopy = pltpu.make_async_copy(w_hbm.at[stage], w, wsem.at[0])
    wcopy.start()
    plane_wait()

    def feed(k):
        ts = pl.ds(k * CH, CH)

        @pl.when(first)
        def _():
            pltpu.make_async_copy(x_hbm.at[ts], xbuf.at[ts, 0], recv.at[k * CH]).start()

        @pl.when(jnp.logical_not(first))
        def _():
            pltpu.make_async_remote_copy(x_hbm.at[ts], xbuf.at[ts, index], insem, recv.at[k * CH],
                                         device_id=(base,), device_id_type=MESH).start()

        return 0

    def step_out(t):
        return pltpu.make_async_remote_copy(xout.at[t], xbuf.at[t], send, recv.at[t], device_id=(nxt,), device_id_type=MESH)

    def final_out(t, i):
        ts = pl.ds(t, CH)
        if i == LAST:
            return pltpu.make_async_copy(xout.at[ts, i], xl_hbm.at[ts], lastsem)
        return pltpu.make_async_remote_copy(xout.at[ts, i], xl_hbm.at[ts], send, lastsem, device_id=(base + i,), device_id_type=MESH)

    def arrived(t):
        @pl.when(jnp.logical_not(first))
        def _():
            step_out(t).wait_recv()

        @pl.when(first & (lax.rem(t, CH) == 0))
        def _():
            ts = pl.ds(t, CH)
            pltpu.make_async_remote_copy(xout.at[ts], xbuf.at[ts], send, recv.at[t], device_id=(nxt,), device_id_type=MESH).wait_recv()

    def pass_on(t):
        @pl.when(jnp.logical_not(last))
        def _():
            step_out(t).start()

        @pl.when(last & (lax.rem(t, CH) == CH - 1))
        def _():
            for i in range(S):
                final_out(t - CH + 1, i).start()

    lax.fori_loop(0, T // CH, lambda k, _: feed(k), 0)
    bias = b_ref[pl.ds(stage, 1), :]

    def project(zref, t):
        xt = rows_of(xbuf[t].astype(F32)).astype(BF16)
        for n in range(0, G4, HB):
            zref[:, n:n + HB] = dot(xt, w[0:H, n:n + HB]) + bias[:, n:n + HB]

    wcopy.wait()
    arrived(jnp.int32(0))
    project(z0, 0)

    kept = ((gates, gates_hbm), (cprev, cp_hbm), (hprev, hp_hbm), (xbuf, xs_hbm))

    def save(t):
        for i, (src, dst) in enumerate(kept):
            pltpu.make_async_copy(src.at[t], dst.at[t], osem.at[i]).start()

    def two(p, state):
        for u in range(2):
            t = 2 * p + u
            zc, zn = ((z0, z1), (z1, z0))[u]

            @pl.when(t > 0)
            def _():
                pass_on(t - 1)
                save(t - 1)

            @pl.when(t + 1 < T)
            def _():
                arrived(t + 1)

            ha, hc, ca, cc = state
            hlow = jnp.concatenate([ha, hc], axis=1).astype(BF16)
            hprev[t] = hlow
            cprev[t, :, 0:HB] = ca
            cprev[t, :, HB:H] = cc
            nh, nc = [], []
            for q in range(2):
                zz = []
                for g in range(4):
                    cols = slice(g * H + q * HB, g * H + q * HB + HB)
                    zz.append(zc[:, cols] + dot(hlow, w[H:2 * H, cols]))
                gi, gf, gg, go = jax.nn.sigmoid(zz[0]), jax.nn.sigmoid(zz[1]), jnp.tanh(zz[2]), jax.nn.sigmoid(zz[3])
                cn = gf * (ca, cc)[q] + gi * gg
                nh.append(go * jnp.tanh(cn))
                nc.append(cn)
                for g, val in enumerate((gi, gf, gg, go)):
                    gates[t, :, g * H + q * HB:g * H + q * HB + HB] = val
            project(zn, jnp.minimum(t + 1, T - 1))
            xt = rows_of(xbuf[t].astype(F32))
            xout[t] = groups_of(xt + jnp.concatenate(nh, axis=1)).astype(BF16)
            state = (nh[0], nh[1], nc[0], nc[1])
        return state

    zero = jnp.zeros((Q, HB), F32)
    lax.fori_loop(0, T // 2, two, (zero,) * 4)
    pass_on(jnp.int32(T - 1))
    save(T - 1)
    for i, (src, dst) in enumerate(kept):
        pltpu.make_async_copy(src, dst, osem.at[i]).wait()

    @pl.when(jnp.logical_not(first))
    def _():
        pltpu.make_async_remote_copy(x_hbm, xl_hbm, insem, lastsem, device_id=(base,), device_id_type=MESH).wait_send()

    @pl.when(jnp.logical_not(last))
    def _():
        pltpu.make_async_remote_copy(xout, xbuf, send, recv.at[0], device_id=(nxt,), device_id_type=MESH).wait_send()

    @pl.when(last)
    def _():
        others = (slice(None), slice(0, S - 1))
        pltpu.make_async_remote_copy(xout.at[others], xbuf.at[others], send, recv.at[0], device_id=(nxt,), device_id_type=MESH).wait_send()

    pltpu.make_async_copy(x_hbm, xl_hbm, lastsem).wait()


def forward(x, w, b):
    return pl.pallas_call(
        fwd_kernel,
        out_shape=(jax.ShapeDtypeStruct((T, Q, G4), F32), jax.ShapeDtypeStruct((T, Q, H), F32),
                   jax.ShapeDtypeStruct((T, Q, H), BF16), jax.ShapeDtypeStruct((T, S, R, H), BF16),
                   jax.ShapeDtypeStruct((T, R, H), BF16)),
        in_specs=[ANY, ANY, VMEM],
        out_specs=(HBM,) * 5,
        scratch_shapes=[pltpu.VMEM((2 * H, G4), BF16), pltpu.VMEM((T, S, R, H), BF16), pltpu.VMEM((T, S, R, H), BF16),
                        pltpu.VMEM((T, Q, G4), F32), pltpu.VMEM((T, Q, H), F32), pltpu.VMEM((T, Q, H), BF16)]
        + [pltpu.VMEM((Q, G4), F32)] * 2 + [DMA((1,)), DMA, DMA((T,)), DMA, DMA, DMA((4,))],
        compiler_params=pltpu.CompilerParams(vmem_limit_bytes=52 * MIB, collective_id=0, has_side_effects=True),
        cost_estimate=pl.CostEstimate(flops=60_000_000_000, bytes_accessed=80_000_000, transcendentals=0),
        name="lstm_fwd",
    )(x, w, b)


def bwd_kernel(d_hbm, gates_hbm, cp_hbm, hp_hbm, xs_hbm, w_hbm, own0, own1, own2, give0, give1, give2, db_ref, dx_hbm,
               w, wt, dbuf, dout, dall, ut, acc, gin, cin, hin, xin,
               wsem, insem, recv, send, lastsem, isem, osem):
    base, index, stage = place()
    plane = base // S
    first, last = stage == 0, stage == S - 1
    prv = base + gray(lax.rem(stage + S - 1, S))
    top = base + LAST
    plane_signal(base, index)
    wcopy = pltpu.make_async_copy(w_hbm.at[stage], w, wsem.at[0])
    wcopy.start()

    def feed(k):
        t = T - CH - k * CH
        ts = pl.ds(t, CH)

        @pl.when(last)
        def _():
            pltpu.make_async_copy(d_hbm.at[ts], dbuf.at[ts, LAST], recv.at[t]).start()

        @pl.when(jnp.logical_not(last))
        def _():
            pltpu.make_async_remote_copy(d_hbm.at[ts], dbuf.at[ts, index], insem, recv.at[t],
                                         device_id=(top,), device_id_type=MESH).start()

        return 0

    def step_out(t):
        return pltpu.make_async_remote_copy(dout.at[t], dbuf.at[t], send, recv.at[t], device_id=(prv,), device_id_type=MESH)

    def final_out(t, i):
        ts = pl.ds(t, CH)
        if i == 0:
            return pltpu.make_async_copy(dout.at[ts, i], dx_hbm.at[ts], lastsem)
        return pltpu.make_async_remote_copy(dout.at[ts, i], dx_hbm.at[ts], send, lastsem, device_id=(base + i,), device_id_type=MESH)

    def arrived(t):
        @pl.when(jnp.logical_not(last))
        def _():
            step_out(t).wait_recv()

        @pl.when(last & (lax.rem(t, CH) == CH - 1))
        def _():
            ts = pl.ds(t - CH + 1, CH)
            pltpu.make_async_remote_copy(dout.at[ts], dbuf.at[ts], send, recv.at[t - CH + 1], device_id=(prv,), device_id_type=MESH).wait_recv()

    def pass_on(t):
        @pl.when(jnp.logical_not(first))
        def _():
            step_out(t).start()

        @pl.when(first & (lax.rem(t, CH) == 0))
        def _():
            for i in range(S):
                final_out(t, i).start()

    def loads(t):
        k = lax.rem(t, NR)
        return [pltpu.make_async_copy(src.at[t], dst.at[k], isem.at[k, i])
                for i, (src, dst) in enumerate(((gates_hbm, gin), (cp_hbm, cin), (hp_hbm, hin), (xs_hbm, xin)))]

    for t in range(T - NR, T):
        for cp in loads(t):
            cp.start()
    plane_wait()
    lax.fori_loop(0, T // CH, lambda k, _: feed(k), 0)
    db_ref[...] = jnp.zeros(db_ref.shape, F32)
    acc[...] = jnp.zeros(acc.shape, F32)
    wcopy.wait()

    def turn(n, _):
        cols = pl.ds(pl.multiple_of(n * HB, HB), HB)
        wt[cols, :] = w[:, cols].T
        return 0

    lax.fori_loop(0, G4 // HB, turn, 0)

    def weight():
        for n in range(0, G4, HB):
            acc[:, n:n + HB] += dot(ut[...], dall[:, n:n + HB])

    def two(n, state):
        p = T // 2 - 1 - n
        us = []
        for u in (1, 0):
            t = 2 * p + u
            k = lax.rem(t, NR)
            for cp in loads(t):
                cp.wait()

            @pl.when(t < T - 1)
            def _():
                pass_on(t + 1)

            if u == 1:
                @pl.when((p < T // 2 - 1) & (lax.rem(p, CH // 2) == CH // 2 - 1))
                def _():
                    weight()

            arrived(t)
            ea, ec, da, dc_ = state
            dext = rows_of(dbuf[t])
            parts = [[None, None] for _ in range(4)]
            nd = []
            for q in range(2):
                gi, gf, gg, go = (gin[k, :, g * H + q * HB:g * H + q * HB + HB] for g in range(4))
                hq = slice(q * HB, q * HB + HB)
                cprev = cin[k, :, hq]
                th = jnp.tanh(gf * cprev + gi * gg)
                e = dext[:, hq] + (ea, ec)[q]
                dc = (da, dc_)[q] + e * (go * (1.0 - th * th))
                parts[0][q] = dc * (gg * gi * (1.0 - gi))
                parts[1][q] = dc * (cprev * gf * (1.0 - gf))
                parts[2][q] = dc * (gi * (1.0 - gg * gg))
                parts[3][q] = e * (th * go * (1.0 - go))
                nd.append(dc * gf)
            trows = pl.ds(pl.multiple_of(lax.rem(t, CH) * Q, Q), Q)
            lows = []
            for i, v in enumerate(v for ps in parts for v in ps):
                cols = slice(i * HB, i * HB + HB)
                low = v.astype(BF16)
                dall[trows, cols] = low
                lows.append(low)
                db_ref[:, cols] += jnp.sum(v.reshape(Q // R, R, HB), axis=0)
            lowz = jnp.concatenate(lows, axis=1)
            ne = [dot(lowz, wt[:, H + q * HB:H + q * HB + HB]) for q in range(2)]
            for q in range(2):
                hq = slice(q * HB, q * HB + HB)
                dout[t, :, :, hq] = groups_of(dext[:, hq] + dot(lowz, wt[:, hq]))
            state = (ne[0], ne[1], nd[0], nd[1])
            us.append((rows_of(xin[k].astype(F32)), hin[k].astype(F32)))

            @pl.when(t >= NR)
            def _():
                for cp in loads(t - NR):
                    cp.start()

        tcols = pl.ds(pl.multiple_of(lax.rem(p, CH // 2) * 2 * Q, 2 * Q), 2 * Q)
        for j in range(2):
            ut[j * H:j * H + H, tcols] = jnp.concatenate([us[1][j], us[0][j]], axis=0).T.astype(BF16)

        return state

    zero = jnp.zeros((Q, HB), F32)
    lax.fori_loop(0, T // 2, two, (zero,) * 4)
    pass_on(jnp.int32(0))

    weight()
    outs = []
    for i, dst in enumerate((give0, give1, give2, own0, own1, own2)):
        at, (m, rows) = plane if i >= len(PIECES) else 1 - plane, PIECES[i % len(PIECES)]
        outs.append(pltpu.make_async_copy(acc.at[pl.ds(pl.multiple_of(at * H + m, LANE), rows)], dst, osem.at[i]))
        outs[i].start()
    for out in outs:
        out.wait()

    @pl.when(jnp.logical_not(last))
    def _():
        pltpu.make_async_remote_copy(d_hbm, dx_hbm, insem, lastsem, device_id=(top,), device_id_type=MESH).wait_send()

    @pl.when(jnp.logical_not(first))
    def _():
        pltpu.make_async_remote_copy(dout, dbuf, send, recv.at[0], device_id=(prv,), device_id_type=MESH).wait_send()

    @pl.when(first)
    def _():
        others = (slice(None), slice(1, S))
        pltpu.make_async_remote_copy(dout.at[others], dbuf.at[others], send, recv.at[0], device_id=(prv,), device_id_type=MESH).wait_send()

    pltpu.make_async_copy(d_hbm, dx_hbm, lastsem).wait()


def backward(d_top, gates, cprev, hprev, xs, w):
    return pl.pallas_call(
        bwd_kernel,
        out_shape=tuple(jax.ShapeDtypeStruct((rows, G4), F32) for _, rows in PIECES * 2) + (jax.ShapeDtypeStruct((R, G4), F32), jax.ShapeDtypeStruct((T, R, H), F32)),
        in_specs=[ANY] * 6,
        out_specs=(HBM,) * (2 * len(PIECES)) + (VMEM, HBM),
        scratch_shapes=[pltpu.VMEM((2 * H, G4), BF16), pltpu.VMEM((G4, 2 * H), BF16), pltpu.VMEM((T, S, R, H), F32),
                        pltpu.VMEM((T, S, R, H), F32), pltpu.VMEM((CH * Q, G4), BF16), pltpu.VMEM((2 * H, CH * Q), BF16), pltpu.VMEM((2 * H, G4), F32)]
        + [pltpu.VMEM((NR, Q, G4), F32), pltpu.VMEM((NR, Q, H), F32), pltpu.VMEM((NR, Q, H), BF16), pltpu.VMEM((NR, S, R, H), BF16)]
        + [DMA((1,)), DMA, DMA((T,)), DMA, DMA, DMA((NR, 4)), DMA((2 * len(PIECES),))],
        compiler_params=pltpu.CompilerParams(vmem_limit_bytes=56 * MIB, collective_id=1, has_side_effects=True),
        cost_estimate=pl.CostEstimate(flops=110_000_000_000, bytes_accessed=80_000_000, transcendentals=0),
        name="lstm_bwd",
    )(d_top, gates, cprev, hprev, xs, w)


VB = 1280
NVB = V // VB
N = T * R
NW = 4
RB = 64


def head_kernel(x_ref, t_ref, w_hbm, dx_ref, lse_ref, lg, g0, g1, wv, mx, sm, tb, wsem):
    def wcopy(b):
        buf = lax.rem(b, NW)
        return pltpu.make_async_copy(w_hbm.at[:, pl.ds(pl.multiple_of(lax.rem(b, NVB) * VB, VB), VB)], wv.at[buf], wsem.at[buf])

    for b in range(NW - 1):
        wcopy(b).start()

    def ready(b):
        for i in range(2):
            wcopy(b + i).wait()
            wcopy(b + i + 2).start()

    mx[...] = jnp.full(mx.shape, -jnp.inf, F32)
    sm[...] = jnp.zeros(sm.shape, F32)
    dx_ref[...] = jnp.zeros(dx_ref.shape, F32)

    def logits(b):
        for c in range(0, VB, HB):
            lg[b, :, c:c + HB] = dot(x_ref[...], wv[lax.rem(b, NW), :, c:c + HB])

    def sums(b):
        for r in range(0, N, RB):
            rows = slice(r, r + RB)
            m_old = mx[rows, :]
            m_new = m_old
            for c in range(0, VB, LANE):
                m_new = jnp.maximum(m_new, lg[b, rows, c:c + LANE])
            acc = sm[rows, :] * jnp.exp(m_old - m_new)
            for c in range(0, VB, LANE):
                acc = acc + jnp.exp(lg[b, rows, c:c + LANE] - m_new)
            mx[rows, :] = m_new
            sm[rows, :] = acc

    wcopy(0).wait()
    logits(0)

    def first(h, _):
        b = 2 * h + 1
        ready(b)
        for i in range(2):
            logits(b + i)
            sums(b + i - 1)
        return 0

    lax.fori_loop(0, NVB // 2, first, 0)
    sums(NVB - 1)
    for r in range(0, N, LANE):
        rows = slice(r, r + LANE)
        top = jnp.max(mx[rows, :], axis=1, keepdims=True)
        tot = jnp.sum(sm[rows, :] * jnp.exp(mx[rows, :] - top), axis=1, keepdims=True)
        lse = top + jnp.log(tot)
        lse_ref[rows, :] = lse
        mx[rows, :] = jnp.broadcast_to(lse, (LANE, LANE))
        tb[rows, :] = jnp.broadcast_to(t_ref[rows, :], (LANE, LANE))

    def grads(b, gb, c):
        ids = b * VB + c + lax.broadcasted_iota(jnp.int32, (RB, LANE), 1)
        for r in range(0, N, RB):
            rows = slice(r, r + RB)
            lse = mx[rows, :]
            tgt = tb[rows, :] - ids
            for h in (0, LANE):
                p = jnp.exp(lg[b, rows, c + h:c + h + LANE] - lse)
                gb[rows, c + h:c + h + LANE] = jnp.where(tgt == h, p - 1.0, p).astype(BF16)

    def apply(b, gb, c):
        return dot_tt(gb[:, c:c + HB], wv[lax.rem(b + NVB, NW), :, c:c + HB])

    for c in range(0, VB, HB):
        grads(0, g0, c)

    def second(h, _):
        for i in range(2):
            b = 2 * h + NVB + i
            wcopy(b).wait()

            @pl.when(b + 2 < 2 * NVB)
            def _():
                wcopy(b + 2).start()

        for b, gb, gn in ((2 * h, g0, g1), (2 * h + 1, g1, g0)):
            total = jnp.zeros((N, H), F32)
            for c in range(0, VB, HB):
                total = total + apply(b, gb, c)
                grads(b + 1, gn, c)
            dx_ref[...] += total
        return 0

    lax.fori_loop(0, NVB // 2, second, 0)
    wcopy(2 * NVB - 1).wait()
    for c in range(0, VB, HB):
        dx_ref[...] += apply(NVB - 1, g0, c)


def head(x, tgt, w_vocab):
    return pl.pallas_call(
        head_kernel,
        out_shape=(jax.ShapeDtypeStruct((N, H), F32), jax.ShapeDtypeStruct((N, 1), F32)),
        in_specs=[VMEM, VMEM, ANY],
        out_specs=(VMEM, VMEM),
        scratch_shapes=[pltpu.VMEM((NVB, N, VB), F32), pltpu.VMEM((N, VB), BF16), pltpu.VMEM((N, VB), BF16), pltpu.VMEM((NW, H, VB), BF16),
                        pltpu.VMEM((N, LANE), F32), pltpu.VMEM((N, LANE), F32), pltpu.VMEM((N, LANE), jnp.int32), DMA((NW,))],
        compiler_params=pltpu.CompilerParams(vmem_limit_bytes=60 * MIB),
        cost_estimate=pl.CostEstimate(flops=40_000_000_000, bytes_accessed=70_000_000, transcendentals=0),
        name="head",
    )(x, tgt, w_vocab)


TB = 768
NTOK = NDEV * N
NK = NTOK // TB
UN = 2
NOWN = (NVB + 1) // 2


def dwv_kernel(lo, hi, x_hbm, st_ref, w_hbm, *rest):
    dw_hbm, xv, xtv, wv, g0, g1, acc, lse, tgt, wsem, xsem, osem, ssem, rsem = rest[-14:]
    core = lax.rem(lax.axis_index("data"), 2)
    peer = lax.axis_index("data") + 1 - 2 * core

    barrier = pltpu.get_barrier_semaphore()
    pl.semaphore_signal(barrier, inc=1, device_id=(peer,), device_id_type=MESH)

    def block(i, side):
        return lo + i + side * (NVB - 1 - 2 * (lo + i))

    def cols(b):
        return pl.ds(pl.multiple_of(b * VB, VB), VB)

    def wcopy(i):
        buf = lax.rem(i, 2)
        return pltpu.make_async_copy(w_hbm.at[:, cols(block(i, core))], wv.at[buf], wsem.at[buf])

    def keep(i):
        buf = lax.rem(i, 2)
        return pltpu.make_async_copy(acc.at[buf], dw_hbm.at[:, cols(block(i, core))], osem.at[buf])

    def send(i, side):
        buf = lax.rem(i, 2)
        return pltpu.make_async_remote_copy(acc.at[buf], dw_hbm.at[:, cols(block(i, side))], ssem.at[buf], rsem.at[i],
                                            device_id=(peer,), device_id_type=MESH)

    def shared(i):
        return lo + i < NOWN - 1

    def done(i):
        keep(i).start()

        @pl.when(shared(i))
        def _():
            send(i, core).start()

    def drained(i):
        keep(i).wait()

        @pl.when(shared(i))
        def _():
            send(i, core).wait_send()

    n = hi - lo
    wcopy(0).start()
    cx = pltpu.make_async_copy(x_hbm, xv, xsem.at[0])
    cx.start()
    cx.wait()

    def turn(k, _):
        for c in range(0, TB, HB):
            rows = pl.ds(pl.multiple_of(k * TB + c, HB), HB)
            xtv[k, :, c:c + HB] = xv[rows, :].T
            lse[rows, :] = jnp.broadcast_to(st_ref[rows, 0:1], (HB, LANE))
            tgt[rows, :] = jnp.broadcast_to(st_ref[rows, LANE - 1:LANE], (HB, LANE))
        return 0

    lax.fori_loop(0, NK, turn, 0)
    pl.semaphore_wait(barrier, 1)

    def weight(it, gold, cols, reset=False):
        k, i = lax.rem(it + NK, NK), jnp.maximum(it, 0) // NK
        acc_c = acc.at[lax.rem(i, 2), :, cols]
        old = acc_c[...]
        acc_c[...] = (jnp.where(k == 0, 0.0, old) if reset else old) + dot(xtv[k], gold[:, cols])

    def step(it, u):
        gnew, gold = ((g0, g1), (g1, g0))[u % 2]
        k, i = lax.rem(it, NK) + u, it // NK
        base = pl.multiple_of(k * TB, TB)
        lane = lax.broadcasted_iota(jnp.int32, (R, LANE), 1) + block(i, core) * VB
        for c in range(0, VB, HB):
            lgt = dot(xv[pl.ds(base, TB), :], wv[lax.rem(i, 2), :, c:c + HB])
            weight(it + u - 1, gold, slice(c, c + HB), u == 1)
            ids = [jnp.tile((lane + (c + h)).astype(F32), (RB // R, 1)) for h in (0, LANE)]
            for r in range(0, TB, RB):
                here = pl.ds(pl.multiple_of(base + r, RB), RB)
                for h in (0, LANE):
                    p = jnp.exp(lgt[r:r + RB, h:h + LANE] - lse[here, :])
                    gnew[r:r + RB, c + h:c + h + LANE] = jnp.where(tgt[here, :] == ids[h // LANE], p - 1.0, p).astype(BF16)

    def body(h, _):
        it = UN * h
        i0, k0 = it // NK, lax.rem(it, NK)

        @pl.when(k0 == 0)
        def _():
            wcopy(i0).wait()

            @pl.when(i0 < n - 1)
            def _():
                wcopy(i0 + 1).start()

        @pl.when((k0 == 0) & (i0 >= 2))
        def _():
            drained(i0 - 2)

        for u in range(UN):
            step(it, u)

        @pl.when((k0 == UN) & (i0 >= 1))
        def _():
            done(i0 - 1)

        return 0

    lax.fori_loop(0, n * NK // UN, body, 0)

    def last(c, _):
        weight(jnp.int32(n * NK - 1), g1, pl.ds(pl.multiple_of(c * HB, HB), HB))
        return 0

    lax.fori_loop(0, VB // HB, last, 0)
    if n > 1:
        drained(n - 2)
    done(n - 1)
    drained(n - 1)
    for i in range(min(n, NOWN - 1 - lo)):
        send(i, 1 - core).wait_recv()


def grad_vocab(lo, hi, x_all, stats, w_vocab, before=()):
    return pl.pallas_call(
        functools.partial(dwv_kernel, lo, hi),
        out_shape=jax.ShapeDtypeStruct((H, V), F32),
        in_specs=[ANY, VMEM, ANY] + [ANY] * len(before),
        out_specs=ANY,
        input_output_aliases={3: 0} if before else {},
        scratch_shapes=[pltpu.VMEM((NTOK, H), BF16), pltpu.VMEM((NK, H, TB), BF16), pltpu.VMEM((2, H, VB), BF16)]
        + [pltpu.VMEM((TB, VB), BF16)] * 2
        + [pltpu.VMEM((2, H, VB), F32)] + [pltpu.VMEM((NTOK, LANE), F32)] * 2
        + [DMA((2,)), DMA((1,)), DMA((2,)), DMA((2,)), DMA((hi - lo,))],
        compiler_params=pltpu.CompilerParams(vmem_limit_bytes=48 * MIB, collective_id=2 + lo, has_side_effects=True),
        cost_estimate=pl.CostEstimate(flops=(hi - lo) * 20_000_000_000, bytes_accessed=100_000_000, transcendentals=0),
        name="dwv",
    )(x_all, stats, w_vocab, *before)


NC = 8


def copy_ring(n, src, dst, buf, isem, osem):
    def fetch(i):
        k = lax.rem(i, NC)
        return pltpu.make_async_copy(src(i), buf.at[k], isem.at[k])

    def put(i):
        k = lax.rem(i, NC)
        return pltpu.make_async_copy(buf.at[k], dst(i), osem.at[k])

    for i in range(NC // 2):
        fetch(i).start()

    def body(i, _):
        fetch(i).wait()
        put(i).start()

        @pl.when(i >= NC // 2)
        def _():
            put(i - NC // 2).wait()

        @pl.when(i + NC // 2 < n)
        def _():
            fetch(i + NC // 2).start()

        return 0

    lax.fori_loop(0, n, body, 0)
    for i in range(n - NC // 2, n):
        put(i).wait()


def copy_call(kernel, out, block, args, name):
    return pl.pallas_call(
        kernel,
        out_shape=jax.ShapeDtypeStruct(out, F32),
        in_specs=[ANY] * len(args),
        out_specs=ANY,
        input_output_aliases={1: 0} if len(args) > 1 else {},
        scratch_shapes=[pltpu.VMEM((NC,) + block, F32), DMA((NC,)), DMA((NC,))],
        compiler_params=pltpu.CompilerParams(vmem_limit_bytes=24 * MIB),
        cost_estimate=pl.CostEstimate(flops=20_000_000_000, bytes_accessed=130_000_000, transcendentals=0),
        name=name,
    )(*args)


def copy_dwv(v):
    rows = 2 * R

    def kernel(src, dst, *scratch):
        def at(ref):
            return lambda i: ref.at[pl.ds(pl.multiple_of(i * rows, rows), rows)]

        copy_ring(H // rows, at(src), at(dst), *scratch)

    return copy_call(kernel, (H, V), (rows, V), (v,), "copy_dwv")


def place_dw(piece, parts, *before):
    first, rows = PIECES[piece]

    def kernel(src, *rest):
        dst, scratch = rest[-4], rest[-3:]

        def target(i):
            return dst.at[gray(lax.rem(i, S)), pl.ds(pl.multiple_of(i // S * H + first, LANE), rows)]

        copy_ring(NDEV, lambda i: src.at[i, 0:rows], target, *scratch)

    return copy_call(kernel, (L, 2 * H, G4), (rows, G4), (parts,) + before, "place_dw")


SPLITS = (0, 1, 5, NOWN)


def solution(mesh):
    def local_grads(x_rows, tgt_rows, w_lstm, b_lstm, w_vocab):
        tgt = jnp.swapaxes(tgt_rows, 0, 1).reshape(N, 1)
        gates, cprev, hprev, xs, top = forward(jnp.swapaxes(x_rows, 0, 1), w_lstm, b_lstm)
        top = top.reshape(N, H)
        d_top, lse = head(top, tgt, w_vocab)
        half = (N, LANE // 2)
        stats = jnp.concatenate([jnp.broadcast_to(lse, half), jnp.broadcast_to(tgt.astype(F32), half)], axis=1)
        x_all = lax.all_gather(top, 'data', axis=0, tiled=True)
        stats = lax.all_gather(stats, 'data', axis=0, tiled=True)
        d_top, x_all = lax.optimization_barrier((d_top, x_all))
        *pieces, db, dx = backward(d_top.reshape(T, R, H), gates, cprev, hprev, xs, w_lstm)
        swap = [(i, (i + S) % NDEV) for i in range(NDEV)]
        dwv, gathered = (), []
        for i in range(len(PIECES)):
            own, give = pieces[i], pieces[len(PIECES) + i]
            if i:
                give, part = lax.optimization_barrier((give, part))
            got = lax.ppermute(give, 'data', swap)
            dwv = grad_vocab(SPLITS[i], SPLITS[i + 1], x_all, stats, w_vocab, dwv)
            own, dwv = lax.optimization_barrier((own, dwv))
            part = own + got if i != 1 else jnp.concatenate([own + got, db], axis=0)
            part, dwv = lax.optimization_barrier((part, dwv))
            gathered.append(lax.all_gather(part, 'data', axis=0))
            dwv = (dwv,)
        dwv = copy_dwv(*dwv)
        dw = place_dw(2, gathered[2], place_dw(1, gathered[1], place_dw(0, gathered[0])))
        db = gathered[1][:, PIECES[1][1]:].reshape(NDEV // S, S, R, G4).sum(axis=(0, 2))
        db = jnp.stack([db[gray(i)] for i in range(L)])
        return dw, db, dwv, jnp.swapaxes(dx, 0, 1)

    return jax.shard_map(local_grads, mesh=mesh, in_specs=(P('data'), P('data'), P(), P(), P()), out_specs=(P(), P(), P(), P('data')), check_vma=False)
```

```python
import functools

import jax
import jax.numpy as jnp
from jax import lax
from jax.experimental import pallas as pl
from jax.experimental.pallas import tpu as pltpu
from jax.sharding import PartitionSpec as P

T = 48
R = 8
S = 8
Q = S * R
H = 512
HB = 256
G4 = 4 * H
L = 8
V = 32000
LANE = 128
NDEV = 16
CH = 4
NR = 6
PIECES = ((0, 0, 256), (256, 384, 256), (512, 384, 128))
F32 = jnp.float32
BF16 = jnp.bfloat16
MESH = pl.DeviceIdType.MESH
MIB = 1024 * 1024
ANY = pl.BlockSpec(memory_space=pl.ANY)
VMEM = pl.BlockSpec(memory_space=pltpu.VMEM)
HBM = pl.BlockSpec(memory_space=pltpu.HBM)
DMA = pltpu.SemaphoreType.DMA


def dot(a, b):
    return jnp.dot(a, b, preferred_element_type=F32)


def dot_tt(a, b):
    return lax.dot_general(a, b, (((1,), (1,)), ((), ())), preferred_element_type=F32)


def gray(k):
    chip, core = k // 2, k % 2
    hi, lo = chip // 2, chip % 2
    return 2 * (chip + hi - 2 * hi * lo) + core


LAST = gray(S - 1)


def place():
    me = lax.axis_index("data")
    index = lax.rem(me, S)
    return me - index, index, gray(index)


def plane_signal(base, index):
    barrier = pltpu.get_barrier_semaphore()
    for i in range(1, S):
        pl.semaphore_signal(barrier, inc=1, device_id=(base + lax.rem(index + i, S),), device_id_type=MESH)


def plane_wait():
    pl.semaphore_wait(pltpu.get_barrier_semaphore(), S - 1)


def rows_of(v):
    return v.reshape(Q, v.shape[-1])


def groups_of(v):
    return v.reshape(S, R, v.shape[-1])


def fwd_kernel(x_hbm, w_hbm, b_ref, gates_hbm, cp_hbm, hp_hbm, xs_hbm, xl_hbm,
               w, xbuf, xout, gates, cprev, hprev, z0, z1, wsem, insem, recv, send, lastsem, osem):
    base, index, stage = place()
    first, last = stage == 0, stage == S - 1
    nxt = base + gray(lax.rem(stage + 1, S))
    plane_signal(base, index)
    wcopy = pltpu.make_async_copy(w_hbm.at[stage], w, wsem.at[0])
    wcopy.start()
    plane_wait()

    def feed(k):
        ts = pl.ds(k * CH, CH)

        @pl.when(first)
        def _():
            pltpu.make_async_copy(x_hbm.at[ts], xbuf.at[ts, 0], recv.at[k * CH]).start()

        @pl.when(jnp.logical_not(first))
        def _():
            pltpu.make_async_remote_copy(x_hbm.at[ts], xbuf.at[ts, index], insem, recv.at[k * CH],
                                         device_id=(base,), device_id_type=MESH).start()

        return 0

    def step_out(t):
        return pltpu.make_async_remote_copy(xout.at[t], xbuf.at[t], send, recv.at[t], device_id=(nxt,), device_id_type=MESH)

    def final_out(t, i):
        ts = pl.ds(t, CH)
        if i == LAST:
            return pltpu.make_async_copy(xout.at[ts, i], xl_hbm.at[ts], lastsem)
        return pltpu.make_async_remote_copy(xout.at[ts, i], xl_hbm.at[ts], send, lastsem, device_id=(base + i,), device_id_type=MESH)

    def arrived(t):
        @pl.when(jnp.logical_not(first))
        def _():
            step_out(t).wait_recv()

        @pl.when(first & (lax.rem(t, CH) == 0))
        def _():
            ts = pl.ds(t, CH)
            pltpu.make_async_remote_copy(xout.at[ts], xbuf.at[ts], send, recv.at[t], device_id=(nxt,), device_id_type=MESH).wait_recv()

    def pass_on(t):
        @pl.when(jnp.logical_not(last))
        def _():
            step_out(t).start()

        @pl.when(last & (lax.rem(t, CH) == CH - 1))
        def _():
            for i in range(S):
                final_out(t - CH + 1, i).start()

    lax.fori_loop(0, T // CH, lambda k, _: feed(k), 0)
    bias = b_ref[pl.ds(stage, 1), :]

    def project(zref, t):
        xt = rows_of(xbuf[t].astype(F32)).astype(BF16)
        for n in range(0, G4, HB):
            zref[:, n:n + HB] = dot(xt, w[0:H, n:n + HB]) + bias[:, n:n + HB]

    wcopy.wait()
    arrived(jnp.int32(0))
    project(z0, 0)

    kept = ((gates, gates_hbm), (cprev, cp_hbm), (hprev, hp_hbm), (xbuf, xs_hbm))

    def save(t):
        for i, (src, dst) in enumerate(kept):
            pltpu.make_async_copy(src.at[t], dst.at[t], osem.at[i]).start()

    def two(p, state):
        for u in range(2):
            t = 2 * p + u
            zc, zn = ((z0, z1), (z1, z0))[u]

            @pl.when(t > 0)
            def _():
                pass_on(t - 1)
                save(t - 1)

            @pl.when(t + 1 < T)
            def _():
                arrived(t + 1)

            ha, hc, ca, cc = state
            hlow = jnp.concatenate([ha, hc], axis=1).astype(BF16)
            hprev[t] = hlow
            cprev[t, :, 0:HB] = ca
            cprev[t, :, HB:H] = cc
            nh, nc = [], []
            for q in range(2):
                zz = []
                for g in range(4):
                    cols = slice(g * H + q * HB, g * H + q * HB + HB)
                    zz.append(zc[:, cols] + dot(hlow, w[H:2 * H, cols]))
                gi, gf, gg, go = jax.nn.sigmoid(zz[0]), jax.nn.sigmoid(zz[1]), jnp.tanh(zz[2]), jax.nn.sigmoid(zz[3])
                cn = gf * (ca, cc)[q] + gi * gg
                nh.append(go * jnp.tanh(cn))
                nc.append(cn)
                for g, val in enumerate((gi, gf, gg, go)):
                    gates[t, :, g * H + q * HB:g * H + q * HB + HB] = val
            project(zn, jnp.minimum(t + 1, T - 1))
            xt = rows_of(xbuf[t].astype(F32))
            xout[t] = groups_of(xt + jnp.concatenate(nh, axis=1)).astype(BF16)
            state = (nh[0], nh[1], nc[0], nc[1])
        return state

    zero = jnp.zeros((Q, HB), F32)
    lax.fori_loop(0, T // 2, two, (zero,) * 4)
    pass_on(jnp.int32(T - 1))
    save(T - 1)
    for i, (src, dst) in enumerate(kept):
        pltpu.make_async_copy(src, dst, osem.at[i]).wait()

    @pl.when(jnp.logical_not(first))
    def _():
        pltpu.make_async_remote_copy(x_hbm, xl_hbm, insem, lastsem, device_id=(base,), device_id_type=MESH).wait_send()

    @pl.when(jnp.logical_not(last))
    def _():
        pltpu.make_async_remote_copy(xout, xbuf, send, recv.at[0], device_id=(nxt,), device_id_type=MESH).wait_send()

    @pl.when(last)
    def _():
        others = (slice(None), slice(0, S - 1))
        pltpu.make_async_remote_copy(xout.at[others], xbuf.at[others], send, recv.at[0], device_id=(nxt,), device_id_type=MESH).wait_send()

    pltpu.make_async_copy(x_hbm, xl_hbm, lastsem).wait()


def forward(x, w, b):
    return pl.pallas_call(
        fwd_kernel,
        out_shape=(jax.ShapeDtypeStruct((T, Q, G4), F32), jax.ShapeDtypeStruct((T, Q, H), F32),
                   jax.ShapeDtypeStruct((T, Q, H), BF16), jax.ShapeDtypeStruct((T, S, R, H), BF16),
                   jax.ShapeDtypeStruct((T, R, H), BF16)),
        in_specs=[ANY, ANY, VMEM],
        out_specs=(HBM,) * 5,
        scratch_shapes=[pltpu.VMEM((2 * H, G4), BF16), pltpu.VMEM((T, S, R, H), BF16), pltpu.VMEM((T, S, R, H), BF16),
                        pltpu.VMEM((T, Q, G4), F32), pltpu.VMEM((T, Q, H), F32), pltpu.VMEM((T, Q, H), BF16)]
        + [pltpu.VMEM((Q, G4), F32)] * 2 + [DMA((1,)), DMA, DMA((T,)), DMA, DMA, DMA((4,))],
        compiler_params=pltpu.CompilerParams(vmem_limit_bytes=52 * MIB, collective_id=0, has_side_effects=True),
        cost_estimate=pl.CostEstimate(flops=60_000_000_000, bytes_accessed=80_000_000, transcendentals=0),
        name="lstm_fwd",
    )(x, w, b)


def bwd_kernel(d_hbm, gates_hbm, cp_hbm, hp_hbm, xs_hbm, w_hbm, both, own1, own2, give1, give2, db_ref, dx_hbm,
               w, wt, dbuf, dout, dall, ut, acc, gin, cin, hin, xin,
               wsem, insem, recv, send, lastsem, isem, osem):
    base, index, stage = place()
    plane = base // S
    first, last = stage == 0, stage == S - 1
    prv = base + gray(lax.rem(stage + S - 1, S))
    top = base + LAST
    plane_signal(base, index)
    wcopy = pltpu.make_async_copy(w_hbm.at[stage], w, wsem.at[0])
    wcopy.start()

    def feed(k):
        t = T - CH - k * CH
        ts = pl.ds(t, CH)

        @pl.when(last)
        def _():
            pltpu.make_async_copy(d_hbm.at[ts], dbuf.at[ts, LAST], recv.at[t]).start()

        @pl.when(jnp.logical_not(last))
        def _():
            pltpu.make_async_remote_copy(d_hbm.at[ts], dbuf.at[ts, index], insem, recv.at[t],
                                         device_id=(top,), device_id_type=MESH).start()

        return 0

    def step_out(t):
        return pltpu.make_async_remote_copy(dout.at[t], dbuf.at[t], send, recv.at[t], device_id=(prv,), device_id_type=MESH)

    def final_out(t, i):
        ts = pl.ds(t, CH)
        if i == 0:
            return pltpu.make_async_copy(dout.at[ts, i], dx_hbm.at[ts], lastsem)
        return pltpu.make_async_remote_copy(dout.at[ts, i], dx_hbm.at[ts], send, lastsem, device_id=(base + i,), device_id_type=MESH)

    def arrived(t):
        @pl.when(jnp.logical_not(last))
        def _():
            step_out(t).wait_recv()

        @pl.when(last & (lax.rem(t, CH) == CH - 1))
        def _():
            ts = pl.ds(t - CH + 1, CH)
            pltpu.make_async_remote_copy(dout.at[ts], dbuf.at[ts], send, recv.at[t - CH + 1], device_id=(prv,), device_id_type=MESH).wait_recv()

    def pass_on(t):
        @pl.when(jnp.logical_not(first))
        def _():
            step_out(t).start()

        @pl.when(first & (lax.rem(t, CH) == 0))
        def _():
            for i in range(S):
                final_out(t, i).start()

    def loads(t):
        k = lax.rem(t, NR)
        return [pltpu.make_async_copy(src.at[t], dst.at[k], isem.at[k, i])
                for i, (src, dst) in enumerate(((gates_hbm, gin), (cp_hbm, cin), (hp_hbm, hin), (xs_hbm, xin)))]

    for t in range(T - NR, T):
        for cp in loads(t):
            cp.start()
    plane_wait()
    lax.fori_loop(0, T // CH, lambda k, _: feed(k), 0)
    db_ref[...] = jnp.zeros(db_ref.shape, F32)
    acc[...] = jnp.zeros(acc.shape, F32)
    wcopy.wait()

    def turn(n, _):
        cols = pl.ds(pl.multiple_of(n * HB, HB), HB)
        wt[cols, :] = w[:, cols].T
        return 0

    lax.fori_loop(0, G4 // HB, turn, 0)

    def weight():
        def part(k, _):
            for n in range(0, 2 * H, HB):
                cols = pl.ds(pl.multiple_of(k * 2 * H + n, HB), HB)
                acc[:, cols] += dot(ut[...], dall[:, cols])
            return 0

        lax.fori_loop(0, G4 // (2 * H), part, 0)

    def two(n, state):
        p = T // 2 - 1 - n
        us = []
        for u in (1, 0):
            t = 2 * p + u
            k = lax.rem(t, NR)
            for cp in loads(t):
                cp.wait()

            @pl.when(t < T - 1)
            def _():
                pass_on(t + 1)

            if u == 1:
                @pl.when((p < T // 2 - 1) & (lax.rem(p, CH // 2) == CH // 2 - 1))
                def _():
                    weight()

            arrived(t)
            ea, ec, da, dc_ = state
            dext = rows_of(dbuf[t])
            parts = [[None, None] for _ in range(4)]
            nd = []
            for q in range(2):
                gi, gf, gg, go = (gin[k, :, g * H + q * HB:g * H + q * HB + HB] for g in range(4))
                hq = slice(q * HB, q * HB + HB)
                cprev = cin[k, :, hq]
                th = jnp.tanh(gf * cprev + gi * gg)
                e = dext[:, hq] + (ea, ec)[q]
                dc = (da, dc_)[q] + e * (go * (1.0 - th * th))
                parts[0][q] = dc * (gg * gi * (1.0 - gi))
                parts[1][q] = dc * (cprev * gf * (1.0 - gf))
                parts[2][q] = dc * (gi * (1.0 - gg * gg))
                parts[3][q] = e * (th * go * (1.0 - go))
                nd.append(dc * gf)
            trows = pl.ds(pl.multiple_of(lax.rem(t, CH) * Q, Q), Q)
            lows = []
            for i, v in enumerate(v for ps in parts for v in ps):
                cols = slice(i * HB, i * HB + HB)
                low = v.astype(BF16)
                dall[trows, cols] = low
                lows.append(low)
                db_ref[:, cols] += jnp.sum(v.reshape(Q // R, R, HB), axis=0)
            lowz = jnp.concatenate(lows, axis=1)
            ne = [dot(lowz, wt[:, H + q * HB:H + q * HB + HB]) for q in range(2)]
            for q in range(2):
                hq = slice(q * HB, q * HB + HB)
                dout[t, :, :, hq] = groups_of(dext[:, hq] + dot(lowz, wt[:, hq]))
            state = (ne[0], ne[1], nd[0], nd[1])
            us.append((rows_of(xin[k].astype(F32)), hin[k].astype(F32)))

            @pl.when(t >= NR)
            def _():
                for cp in loads(t - NR):
                    cp.start()

        tcols = pl.ds(pl.multiple_of(lax.rem(p, CH // 2) * 2 * Q, 2 * Q), 2 * Q)
        for j in range(2):
            ut[j * H:j * H + H, tcols] = jnp.concatenate([us[1][j], us[0][j]], axis=0).T.astype(BF16)

        return state

    zero = jnp.zeros((Q, HB), F32)
    lax.fori_loop(0, T // 2, two, (zero,) * 4)
    pass_on(jnp.int32(0))

    weight()
    outs = []
    for i, (dst, (row, step, rows), at) in enumerate(((both, PIECES[0], 0), (give1, PIECES[1], 1 - plane), (give2, PIECES[2], 1 - plane),
                                                      (own1, PIECES[1], plane), (own2, PIECES[2], plane))):
        outs.append(pltpu.make_async_copy(acc.at[pl.ds(pl.multiple_of(row + at * step, LANE), rows)], dst, osem.at[i]))
        outs[i].start()
    for out in outs:
        out.wait()

    @pl.when(jnp.logical_not(last))
    def _():
        pltpu.make_async_remote_copy(d_hbm, dx_hbm, insem, lastsem, device_id=(top,), device_id_type=MESH).wait_send()

    @pl.when(jnp.logical_not(first))
    def _():
        pltpu.make_async_remote_copy(dout, dbuf, send, recv.at[0], device_id=(prv,), device_id_type=MESH).wait_send()

    @pl.when(first)
    def _():
        others = (slice(None), slice(1, S))
        pltpu.make_async_remote_copy(dout.at[others], dbuf.at[others], send, recv.at[0], device_id=(prv,), device_id_type=MESH).wait_send()

    pltpu.make_async_copy(d_hbm, dx_hbm, lastsem).wait()


def backward(d_top, gates, cprev, hprev, xs, w):
    return pl.pallas_call(
        bwd_kernel,
        out_shape=tuple(jax.ShapeDtypeStruct((rows, G4), F32) for _, _, rows in PIECES + PIECES[1:]) + (jax.ShapeDtypeStruct((R, G4), F32), jax.ShapeDtypeStruct((T, R, H), F32)),
        in_specs=[ANY] * 6,
        out_specs=(HBM,) * 5 + (VMEM, HBM),
        scratch_shapes=[pltpu.VMEM((2 * H, G4), BF16), pltpu.VMEM((G4, 2 * H), BF16), pltpu.VMEM((T, S, R, H), F32),
                        pltpu.VMEM((T, S, R, H), F32), pltpu.VMEM((CH * Q, G4), BF16), pltpu.VMEM((2 * H, CH * Q), BF16), pltpu.VMEM((2 * H, G4), F32)]
        + [pltpu.VMEM((NR, Q, G4), F32), pltpu.VMEM((NR, Q, H), F32), pltpu.VMEM((NR, Q, H), BF16), pltpu.VMEM((NR, S, R, H), BF16)]
        + [DMA((1,)), DMA, DMA((T,)), DMA, DMA, DMA((NR, 4)), DMA((5,))],
        compiler_params=pltpu.CompilerParams(vmem_limit_bytes=56 * MIB, collective_id=1, has_side_effects=True),
        cost_estimate=pl.CostEstimate(flops=110_000_000_000, bytes_accessed=80_000_000, transcendentals=0),
        name="lstm_bwd",
    )(d_top, gates, cprev, hprev, xs, w)


VB = 1280
NVB = V // VB
N = T * R
NW = 4
RB = 64


def head_kernel(x_ref, t_ref, w_hbm, dx_ref, lse_ref, lg, g0, g1, wv, mx, sm, tb, wsem):
    def wcopy(b):
        buf = lax.rem(b, NW)
        return pltpu.make_async_copy(w_hbm.at[:, pl.ds(pl.multiple_of(lax.rem(b, NVB) * VB, VB), VB)], wv.at[buf], wsem.at[buf])

    for b in range(NW - 1):
        wcopy(b).start()

    def ready(b):
        for i in range(2):
            wcopy(b + i).wait()
            wcopy(b + i + 2).start()

    mx[...] = jnp.full(mx.shape, -jnp.inf, F32)
    sm[...] = jnp.zeros(sm.shape, F32)
    dx_ref[...] = jnp.zeros(dx_ref.shape, F32)

    def each(n, act):
        lax.fori_loop(0, n, lambda i, _: (act(i), 0)[1], 0)

    def at(i, size):
        return pl.ds(pl.multiple_of(i * size, size), size)

    def logits(b, cols):
        lg[b, :, cols] = dot(x_ref[...], wv[lax.rem(b, NW), :, cols])

    def sums(b, rows):
        m_old = mx[rows, :]
        m_new = m_old
        for c in range(0, VB, LANE):
            m_new = jnp.maximum(m_new, lg[b, rows, c:c + LANE])
        acc = sm[rows, :] * jnp.exp(m_old - m_new)
        for c in range(0, VB, LANE):
            acc = acc + jnp.exp(lg[b, rows, c:c + LANE] - m_new)
        mx[rows, :] = m_new
        sm[rows, :] = acc

    wcopy(0).wait()
    each(VB // HB, lambda c: logits(0, at(c, HB)))

    def first(h, _):
        b = 2 * h + 1
        ready(b)
        for i in range(2):
            for c in range(0, VB, HB):
                logits(b + i, slice(c, c + HB))
            for r in range(0, N, RB):
                sums(b + i - 1, slice(r, r + RB))
        return 0

    lax.fori_loop(0, NVB // 2, first, 0)
    each(N // RB, lambda r: sums(NVB - 1, at(r, RB)))

    def finish(r):
        rows = at(r, LANE)
        top = jnp.max(mx[rows, :], axis=1, keepdims=True)
        tot = jnp.sum(sm[rows, :] * jnp.exp(mx[rows, :] - top), axis=1, keepdims=True)
        lse = top + jnp.log(tot)
        lse_ref[rows, :] = lse
        mx[rows, :] = jnp.broadcast_to(lse, (LANE, LANE))
        tb[rows, :] = jnp.broadcast_to(t_ref[rows, :], (LANE, LANE))

    each(N // LANE, finish)

    def grads(b, gb, c):
        ids = [b * VB + c + h + lax.broadcasted_iota(jnp.int32, (RB, LANE), 1) for h in (0, LANE)]
        for r in range(0, N, RB):
            rows = slice(r, r + RB)
            lse = mx[rows, :]
            for h in (0, LANE):
                cols = pl.ds(c + h, LANE)
                p = jnp.exp(lg[b, rows, cols] - lse)
                gb[rows, cols] = jnp.where(tb[rows, :] == ids[h // LANE], p - 1.0, p).astype(BF16)

    def apply(b, gb, cols):
        return dot_tt(gb[:, cols], wv[lax.rem(b + NVB, NW), :, cols])

    each(VB // HB, lambda c: grads(0, g0, pl.multiple_of(c * HB, HB)))

    def second(h, _):
        for i in range(2):
            b = 2 * h + NVB + i
            wcopy(b).wait()

            @pl.when(b + 2 < 2 * NVB)
            def _():
                wcopy(b + 2).start()

        for b, gb, gn in ((2 * h, g0, g1), (2 * h + 1, g1, g0)):
            total = jnp.zeros((N, H), F32)
            for c in range(0, VB, HB):
                total = total + apply(b, gb, slice(c, c + HB))
                grads(b + 1, gn, c)
            dx_ref[...] += total
        return 0

    lax.fori_loop(0, NVB // 2, second, 0)
    wcopy(2 * NVB - 1).wait()

    def last(c):
        dx_ref[...] += apply(NVB - 1, g0, at(c, HB))

    each(VB // HB, last)


def head(x, tgt, w_vocab):
    return pl.pallas_call(
        head_kernel,
        out_shape=(jax.ShapeDtypeStruct((N, H), F32), jax.ShapeDtypeStruct((N, 1), F32)),
        in_specs=[VMEM, VMEM, ANY],
        out_specs=(VMEM, VMEM),
        scratch_shapes=[pltpu.VMEM((NVB, N, VB), F32), pltpu.VMEM((N, VB), BF16), pltpu.VMEM((N, VB), BF16), pltpu.VMEM((NW, H, VB), BF16),
                        pltpu.VMEM((N, LANE), F32), pltpu.VMEM((N, LANE), F32), pltpu.VMEM((N, LANE), jnp.int32), DMA((NW,))],
        compiler_params=pltpu.CompilerParams(vmem_limit_bytes=60 * MIB),
        cost_estimate=pl.CostEstimate(flops=40_000_000_000, bytes_accessed=70_000_000, transcendentals=0),
        name="head",
    )(x, tgt, w_vocab)


TB = 768
NTOK = NDEV * N
NK = NTOK // TB
UN = 2
NOWN = (NVB + 1) // 2


def dwv_kernel(lo, hi, came, x_hbm, st_ref, w_hbm, *rest):
    nshared = min(hi, NOWN - 1) - lo
    arrived = rest[len(rest) - 15 - 1 - (nshared > 0) - len(came):]
    dw_hbm = arrived[len(came)]
    give_hbm = arrived[len(came) + 1]
    xv, xtv, wv, g0, g1, acc, lse, tgt, box, wsem, xsem, osem, gsem, isem, psem = rest[-15:]
    core = lax.rem(lax.axis_index("data"), 2)

    def block(j, side):
        return j + side * (NVB - 1 - 2 * j)

    def cols(b):
        return pl.ds(pl.multiple_of(b * VB, VB), VB)

    def wcopy(i):
        buf = lax.rem(i, 2)
        return pltpu.make_async_copy(w_hbm.at[:, cols(block(lo + i, core))], wv.at[buf], wsem.at[buf])

    def keep(i):
        buf = lax.rem(i, 2)
        return pltpu.make_async_copy(acc.at[buf], dw_hbm.at[:, cols(block(lo + i, core))], osem.at[buf])

    def give(i):
        buf = lax.rem(i, 2)
        return pltpu.make_async_copy(acc.at[buf], give_hbm.at[i], gsem.at[buf])

    def done(i):
        keep(i).start()
        if nshared > 0:
            give(i).start()

    def drained(i):
        keep(i).wait()
        if nshared > 0:
            give(i).wait()

    pieces = [(src, first, i, r) for src, (first, count) in zip(arrived, came) for i in range(count) for r in range(0, H, LANE)]
    per = -(-len(pieces) // ((hi - lo) * NK // UN))

    def fetch(src, i, r, k, slot):
        return pltpu.make_async_copy(src.at[i, pl.ds(r, LANE)], box.at[k, slot], isem.at[k, slot])

    def put(first, i, r, k, slot):
        return pltpu.make_async_copy(box.at[k, slot], dw_hbm.at[pl.ds(r, LANE), cols(block(first + i, 1 - core))], psem.at[k, slot])

    def pieces_of(h, act):
        at = 0
        for src, (first, count) in zip(arrived, came):
            total = count * H // LANE
            for slot in range(per):
                c = h * per + slot - at
                i, r = c // (H // LANE), pl.multiple_of(lax.rem(c, H // LANE) * LANE, LANE)

                @pl.when((c >= 0) & (c < total))
                def _():
                    act(src, first, i, r, lax.rem(h, 2), slot)

            at += total

    def land(src, first, i, r, k, slot):
        fetch(src, i, r, k, slot).wait()
        put(first, i, r, k, slot).start()

    def move(h):
        if came:
            pieces_of(h, land)
            pieces_of(h - 1 + 2 * (h == 0) * len(pieces), lambda src, first, i, r, k, slot: put(first, i, r, k, slot).wait())
            pieces_of(h + 1, lambda src, first, i, r, k, slot: fetch(src, i, r, k, slot).start())

    n = hi - lo
    wcopy(0).start()
    cx = pltpu.make_async_copy(x_hbm, xv, xsem.at[0])
    cx.start()
    cx.wait()

    def turn(k, _):
        for c in range(0, TB, HB):
            rows = pl.ds(pl.multiple_of(k * TB + c, HB), HB)
            xtv[k, :, c:c + HB] = xv[rows, :].T
            lse[rows, :] = jnp.broadcast_to(st_ref[rows, 0:1], (HB, LANE))
            tgt[rows, :] = jnp.broadcast_to(st_ref[rows, LANE - 1:LANE], (HB, LANE))
        return 0

    lax.fori_loop(0, NK, turn, 0)
    if came:
        pieces_of(jnp.int32(0), lambda src, first, i, r, k, slot: fetch(src, i, r, k, slot).start())

    def weight(it, gold, cols, reset=False):
        k, i = lax.rem(it + NK, NK), jnp.maximum(it, 0) // NK
        acc_c = acc.at[lax.rem(i, 2), :, cols]
        old = acc_c[...]
        acc_c[...] = (jnp.where(k == 0, 0.0, old) if reset else old) + dot(xtv[k], gold[:, cols])

    def step(it, u):
        gnew, gold = ((g0, g1), (g1, g0))[u % 2]
        k, i = lax.rem(it, NK) + u, it // NK
        base = pl.multiple_of(k * TB, TB)
        lane = lax.broadcasted_iota(jnp.int32, (R, LANE), 1) + block(lo + i, core) * VB
        for c in range(0, VB, HB):
            lgt = dot(xv[pl.ds(base, TB), :], wv[lax.rem(i, 2), :, c:c + HB])
            weight(it + u - 1, gold, slice(c, c + HB), u == 1)
            ids = [jnp.tile((lane + (c + h)).astype(F32), (RB // R, 1)) for h in (0, LANE)]
            for r in range(0, TB, RB):
                here = pl.ds(pl.multiple_of(base + r, RB), RB)
                for h in (0, LANE):
                    p = jnp.exp(lgt[r:r + RB, h:h + LANE] - lse[here, :])
                    gnew[r:r + RB, c + h:c + h + LANE] = jnp.where(tgt[here, :] == ids[h // LANE], p - 1.0, p).astype(BF16)

    def body(h, _):
        it = UN * h
        i0, k0 = it // NK, lax.rem(it, NK)
        move(h)

        @pl.when(k0 == 0)
        def _():
            wcopy(i0).wait()

            @pl.when(i0 < n - 1)
            def _():
                wcopy(i0 + 1).start()

        @pl.when((k0 == 0) & (i0 >= 2))
        def _():
            drained(i0 - 2)

        for u in range(UN):
            step(it, u)

        @pl.when((k0 == UN) & (i0 >= 1))
        def _():
            done(i0 - 1)

        return 0

    lax.fori_loop(0, n * NK // UN, body, 0)

    def last(c, _):
        weight(jnp.int32(n * NK - 1), g1, pl.ds(pl.multiple_of(c * HB, HB), HB))
        return 0

    lax.fori_loop(0, VB // HB, last, 0)
    if n > 1:
        drained(n - 2)
    done(n - 1)
    if came:
        pieces_of(jnp.int32(n * NK // UN - 1), lambda src, first, i, r, k, slot: put(first, i, r, k, slot).wait())
    drained(n - 1)


def grad_vocab(lo, hi, x_all, stats, w_vocab, before=(), came=()):
    counts = tuple((first, v.shape[0]) for first, v in came)
    nshared = min(hi, NOWN - 1) - lo
    out = (jax.ShapeDtypeStruct((H, V), F32), jax.ShapeDtypeStruct((nshared, H, VB), F32))[:1 + (nshared > 0)]
    per = max(1, -(-sum(c for _, c in counts) * (H // LANE) // ((hi - lo) * NK // UN)))
    return pl.pallas_call(
        functools.partial(dwv_kernel, lo, hi, counts),
        out_shape=out,
        in_specs=[ANY, VMEM, ANY] + [HBM] * (len(before) + len(came)),
        out_specs=(HBM,) * len(out),
        input_output_aliases={3: 0} if before else {},
        scratch_shapes=[pltpu.VMEM((NTOK, H), BF16), pltpu.VMEM((NK, H, TB), BF16), pltpu.VMEM((2, H, VB), BF16)]
        + [pltpu.VMEM((TB, VB), BF16)] * 2
        + [pltpu.VMEM((2, H, VB), F32)] + [pltpu.VMEM((NTOK, LANE), F32)] * 2 + [pltpu.VMEM((2, per, LANE, VB), F32)]
        + [DMA((2,)), DMA((1,)), DMA((2,)), DMA((2,)), DMA((2, per)), DMA((2, per))],
        compiler_params=pltpu.CompilerParams(vmem_limit_bytes=62 * MIB),
        cost_estimate=pl.CostEstimate(flops=(hi - lo) * 20_000_000_000, bytes_accessed=100_000_000, transcendentals=0),
        name="dwv",
    )(x_all, stats, w_vocab, *before, *(v for _, v in came))


NC = 8


def copy_ring(n, src, dst, buf, isem, osem):
    def fetch(i):
        k = lax.rem(i, NC)
        return pltpu.make_async_copy(src(i), buf.at[k], isem.at[k])

    def put(i):
        k = lax.rem(i, NC)
        return pltpu.make_async_copy(buf.at[k], dst(i), osem.at[k])

    for i in range(NC // 2):
        fetch(i).start()

    def body(i, _):
        fetch(i).wait()
        put(i).start()

        @pl.when(i >= NC // 2)
        def _():
            put(i - NC // 2).wait()

        @pl.when(i + NC // 2 < n)
        def _():
            fetch(i + NC // 2).start()

        return 0

    lax.fori_loop(0, n, body, 0)
    for i in range(n - NC // 2, n):
        put(i).wait()


def copy_call(kernel, out, block, args):
    return pl.pallas_call(
        kernel,
        out_shape=jax.ShapeDtypeStruct(out, F32),
        in_specs=[HBM] * len(args),
        out_specs=HBM,
        input_output_aliases={1: 0} if len(args) > 1 else {},
        scratch_shapes=[pltpu.VMEM((NC,) + block, F32), DMA((NC,)), DMA((NC,))],
        compiler_params=pltpu.CompilerParams(vmem_limit_bytes=24 * MIB),
        cost_estimate=pl.CostEstimate(flops=20_000_000_000, bytes_accessed=130_000_000, transcendentals=0),
    )(*args)


def place_dw(piece, parts, *before):
    row, step, rows = PIECES[piece]

    def kernel(src, *rest):
        dst, scratch = rest[-4], rest[-3:]

        def target(i):
            return dst.at[gray(lax.rem(i, S)), pl.ds(pl.multiple_of(row + i // S * step, LANE), rows)]

        copy_ring(parts.shape[0], lambda i: src.at[i, 0:rows], target, *scratch)

    return copy_call(kernel, (L, 2 * H, G4), (rows, G4), (parts,) + before)


SPLITS = (0, 2, 5, 12, NOWN)


def solution(mesh):
    def local_grads(x_rows, tgt_rows, w_lstm, b_lstm, w_vocab):
        tgt = jnp.swapaxes(tgt_rows, 0, 1).reshape(N, 1)
        gates, cprev, hprev, xs, top = forward(jnp.swapaxes(x_rows, 0, 1), w_lstm, b_lstm)
        top = top.reshape(N, H)
        d_top, lse = head(top, tgt, w_vocab)
        half = (N, LANE // 2)
        stats = jnp.concatenate([jnp.broadcast_to(lse, half), jnp.broadcast_to(tgt.astype(F32), half)], axis=1)
        x_all = lax.all_gather(top, 'data', axis=0, tiled=True)
        stats = lax.all_gather(stats, 'data', axis=0, tiled=True)
        d_top, x_all = lax.optimization_barrier((d_top, x_all))
        both, *owns, give1, give2, db, dx = backward(d_top.reshape(T, R, H), gates, cprev, hprev, xs, w_lstm)
        other_plane = [(i, (i + S) % NDEV) for i in range(NDEV)]
        other_core = [(i, i + 1 - 2 * (i % 2)) for i in range(NDEV)]
        planes = [list(range(S)), list(range(S, NDEV))]
        dwv, part, gathered, swapped = (), both, [], []
        for i, (own, give) in enumerate(((both, both), (owns[0], give1), (owns[1], give2))):
            if i:
                give, part = lax.optimization_barrier((give, part))
            got = lax.ppermute(give, 'data', other_plane)
            dwv, sent = grad_vocab(SPLITS[i], SPLITS[i + 1], x_all, stats, w_vocab, dwv, swapped[:1] if i == 2 else ())
            own, dwv = lax.optimization_barrier((own, dwv))
            part = own + got if i != 1 else jnp.concatenate([own + got, db], axis=0)
            part, dwv = lax.optimization_barrier((part, dwv))
            gathered.append(lax.all_gather(part, 'data', axis=0, axis_index_groups=None if i else planes))
            swapped.append((SPLITS[i], lax.ppermute(sent, 'data', other_core)))
            dwv = (dwv,)
        dwv, = grad_vocab(SPLITS[3], SPLITS[4], x_all, stats, w_vocab, dwv, swapped[1:])
        dw = place_dw(0, gathered[0])
        dw = place_dw(2, gathered[2], place_dw(1, gathered[1], dw))
        db = gathered[1][:, PIECES[1][2]:].reshape(NDEV // S, S, R, G4).sum(axis=(0, 2))
        db = jnp.stack([db[gray(i)] for i in range(L)])
        return dw, db, dwv, jnp.swapaxes(dx, 0, 1)

    return jax.shard_map(local_grads, mesh=mesh, in_specs=(P('data'), P('data'), P(), P(), P()), out_specs=(P(), P(), P(), P('data')), check_vma=False)
```

```python
import functools

import jax
import jax.numpy as jnp
from jax import lax
from jax.experimental import pallas as pl
from jax.experimental.pallas import tpu as pltpu
from jax.sharding import PartitionSpec as P

T = 48
R = 8
S = 8
Q = S * R
H = 512
HB = 256
G4 = 4 * H
L = 8
V = 32000
LANE = 128
NDEV = 16
CH = 4
NR = 6
PIECES = ((0, 0, 256), (256, 384, 352), (608, 384, 32))
F32 = jnp.float32
BF16 = jnp.bfloat16
MESH = pl.DeviceIdType.MESH
MIB = 1024 * 1024
ANY = pl.BlockSpec(memory_space=pl.ANY)
VMEM = pl.BlockSpec(memory_space=pltpu.VMEM)
HBM = pl.BlockSpec(memory_space=pltpu.HBM)
DMA = pltpu.SemaphoreType.DMA


def dot(a, b):
    return jnp.dot(a, b, preferred_element_type=F32)


def dot_tt(a, b):
    return lax.dot_general(a, b, (((1,), (1,)), ((), ())), preferred_element_type=F32)


def gray(k):
    chip, core = k // 2, k % 2
    hi, lo = chip // 2, chip % 2
    return 2 * (chip + hi - 2 * hi * lo) + core


LAST = gray(S - 1)


def place():
    me = lax.axis_index("data")
    index = lax.rem(me, S)
    return me - index, index, gray(index)


def plane_signal(base, index):
    barrier = pltpu.get_barrier_semaphore()
    for i in range(1, S):
        pl.semaphore_signal(barrier, inc=1, device_id=(base + lax.rem(index + i, S),), device_id_type=MESH)


def plane_wait():
    pl.semaphore_wait(pltpu.get_barrier_semaphore(), S - 1)


def rows_of(v):
    return v.reshape(Q, v.shape[-1])


def groups_of(v):
    return v.reshape(S, R, v.shape[-1])


def fwd_kernel(x_hbm, w_hbm, b_ref, gates_hbm, cp_hbm, hp_hbm, xs_hbm, xl_hbm,
               w, xbuf, xout, gates, cprev, hprev, z0, z1, wsem, insem, recv, send, lastsem, osem):
    base, index, stage = place()
    first, last = stage == 0, stage == S - 1
    nxt = base + gray(lax.rem(stage + 1, S))
    plane_signal(base, index)
    wcopy = pltpu.make_async_copy(w_hbm.at[stage], w, wsem.at[0])
    wcopy.start()
    plane_wait()

    def feed(k):
        ts = pl.ds(k * CH, CH)

        @pl.when(first)
        def _():
            pltpu.make_async_copy(x_hbm.at[ts], xbuf.at[ts, 0], recv.at[k * CH]).start()

        @pl.when(jnp.logical_not(first))
        def _():
            pltpu.make_async_remote_copy(x_hbm.at[ts], xbuf.at[ts, index], insem, recv.at[k * CH],
                                         device_id=(base,), device_id_type=MESH).start()

        return 0

    def step_out(t):
        return pltpu.make_async_remote_copy(xout.at[t], xbuf.at[t], send, recv.at[t], device_id=(nxt,), device_id_type=MESH)

    def final_out(t, i):
        ts = pl.ds(t, CH)
        if i == LAST:
            return pltpu.make_async_copy(xout.at[ts, i], xl_hbm.at[ts], lastsem)
        return pltpu.make_async_remote_copy(xout.at[ts, i], xl_hbm.at[ts], send, lastsem, device_id=(base + i,), device_id_type=MESH)

    def arrived(t):
        @pl.when(jnp.logical_not(first))
        def _():
            step_out(t).wait_recv()

        @pl.when(first & (lax.rem(t, CH) == 0))
        def _():
            ts = pl.ds(t, CH)
            pltpu.make_async_remote_copy(xout.at[ts], xbuf.at[ts], send, recv.at[t], device_id=(nxt,), device_id_type=MESH).wait_recv()

    def pass_on(t):
        @pl.when(jnp.logical_not(last))
        def _():
            step_out(t).start()

        @pl.when(last & (lax.rem(t, CH) == CH - 1))
        def _():
            for i in range(S):
                final_out(t - CH + 1, i).start()

    lax.fori_loop(0, T // CH, lambda k, _: feed(k), 0)
    bias = b_ref[pl.ds(stage, 1), :]

    def project(zref, t):
        xt = rows_of(xbuf[t].astype(F32)).astype(BF16)
        for n in range(0, G4, HB):
            zref[:, n:n + HB] = dot(xt, w[0:H, n:n + HB]) + bias[:, n:n + HB]

    wcopy.wait()
    arrived(jnp.int32(0))
    project(z0, 0)

    kept = ((gates, gates_hbm), (cprev, cp_hbm), (hprev, hp_hbm), (xbuf, xs_hbm))

    def save(t):
        for i, (src, dst) in enumerate(kept):
            pltpu.make_async_copy(src.at[t], dst.at[t], osem.at[i]).start()

    def two(p, state):
        for u in range(2):
            t = 2 * p + u
            zc, zn = ((z0, z1), (z1, z0))[u]

            @pl.when(t > 0)
            def _():
                pass_on(t - 1)
                save(t - 1)

            @pl.when(t + 1 < T)
            def _():
                arrived(t + 1)

            ha, hc, ca, cc = state
            hlow = jnp.concatenate([ha, hc], axis=1).astype(BF16)
            hprev[t] = hlow
            cprev[t, :, 0:HB] = ca
            cprev[t, :, HB:H] = cc
            nh, nc = [], []
            for q in range(2):
                zz = []
                for g in range(4):
                    cols = slice(g * H + q * HB, g * H + q * HB + HB)
                    zz.append(zc[:, cols] + dot(hlow, w[H:2 * H, cols]))
                gi, gf, gg, go = jax.nn.sigmoid(zz[0]), jax.nn.sigmoid(zz[1]), jnp.tanh(zz[2]), jax.nn.sigmoid(zz[3])
                cn = gf * (ca, cc)[q] + gi * gg
                nh.append(go * jnp.tanh(cn))
                nc.append(cn)
                for g, val in enumerate((gi, gf, gg, go)):
                    gates[t, :, g * H + q * HB:g * H + q * HB + HB] = val
            project(zn, jnp.minimum(t + 1, T - 1))
            xt = rows_of(xbuf[t].astype(F32))
            xout[t] = groups_of(xt + jnp.concatenate(nh, axis=1)).astype(BF16)
            state = (nh[0], nh[1], nc[0], nc[1])
        return state

    zero = jnp.zeros((Q, HB), F32)
    lax.fori_loop(0, T // 2, two, (zero,) * 4)
    pass_on(jnp.int32(T - 1))
    save(T - 1)
    for i, (src, dst) in enumerate(kept):
        pltpu.make_async_copy(src, dst, osem.at[i]).wait()

    @pl.when(jnp.logical_not(first))
    def _():
        pltpu.make_async_remote_copy(x_hbm, xl_hbm, insem, lastsem, device_id=(base,), device_id_type=MESH).wait_send()

    @pl.when(jnp.logical_not(last))
    def _():
        pltpu.make_async_remote_copy(xout, xbuf, send, recv.at[0], device_id=(nxt,), device_id_type=MESH).wait_send()

    @pl.when(last)
    def _():
        others = (slice(None), slice(0, S - 1))
        pltpu.make_async_remote_copy(xout.at[others], xbuf.at[others], send, recv.at[0], device_id=(nxt,), device_id_type=MESH).wait_send()

    pltpu.make_async_copy(x_hbm, xl_hbm, lastsem).wait()


def forward(x, w, b):
    return pl.pallas_call(
        fwd_kernel,
        out_shape=(jax.ShapeDtypeStruct((T, Q, G4), F32), jax.ShapeDtypeStruct((T, Q, H), F32),
                   jax.ShapeDtypeStruct((T, Q, H), BF16), jax.ShapeDtypeStruct((T, S, R, H), BF16),
                   jax.ShapeDtypeStruct((T, R, H), BF16)),
        in_specs=[ANY, ANY, VMEM],
        out_specs=(HBM,) * 5,
        scratch_shapes=[pltpu.VMEM((2 * H, G4), BF16), pltpu.VMEM((T, S, R, H), BF16), pltpu.VMEM((T, S, R, H), BF16),
                        pltpu.VMEM((T, Q, G4), F32), pltpu.VMEM((T, Q, H), F32), pltpu.VMEM((T, Q, H), BF16)]
        + [pltpu.VMEM((Q, G4), F32)] * 2 + [DMA((1,)), DMA, DMA((T,)), DMA, DMA, DMA((4,))],
        compiler_params=pltpu.CompilerParams(vmem_limit_bytes=52 * MIB, collective_id=0, has_side_effects=True),
        cost_estimate=pl.CostEstimate(flops=60_000_000_000, bytes_accessed=80_000_000, transcendentals=0),
        name="lstm_fwd",
    )(x, w, b)


def bwd_kernel(d_hbm, gates_hbm, cp_hbm, hp_hbm, xs_hbm, w_hbm, both, own1, own2, give1, give2, db_ref, dx_hbm,
               w, wt, dbuf, dout, dall, ut, acc, gin, cin, hin, xin,
               wsem, insem, recv, send, lastsem, isem, osem):
    base, index, stage = place()
    plane = base // S
    first, last = stage == 0, stage == S - 1
    prv = base + gray(lax.rem(stage + S - 1, S))
    top = base + LAST
    plane_signal(base, index)
    wcopy = pltpu.make_async_copy(w_hbm.at[stage], w, wsem.at[0])
    wcopy.start()

    def feed(k):
        t = T - CH - k * CH
        ts = pl.ds(t, CH)

        @pl.when(last)
        def _():
            pltpu.make_async_copy(d_hbm.at[ts], dbuf.at[ts, LAST], recv.at[t]).start()

        @pl.when(jnp.logical_not(last))
        def _():
            pltpu.make_async_remote_copy(d_hbm.at[ts], dbuf.at[ts, index], insem, recv.at[t],
                                         device_id=(top,), device_id_type=MESH).start()

        return 0

    def step_out(t):
        return pltpu.make_async_remote_copy(dout.at[t], dbuf.at[t], send, recv.at[t], device_id=(prv,), device_id_type=MESH)

    def final_out(t, i):
        ts = pl.ds(t, CH)
        if i == 0:
            return pltpu.make_async_copy(dout.at[ts, i], dx_hbm.at[ts], lastsem)
        return pltpu.make_async_remote_copy(dout.at[ts, i], dx_hbm.at[ts], send, lastsem, device_id=(base + i,), device_id_type=MESH)

    def arrived(t):
        @pl.when(jnp.logical_not(last))
        def _():
            step_out(t).wait_recv()

        @pl.when(last & (lax.rem(t, CH) == CH - 1))
        def _():
            ts = pl.ds(t - CH + 1, CH)
            pltpu.make_async_remote_copy(dout.at[ts], dbuf.at[ts], send, recv.at[t - CH + 1], device_id=(prv,), device_id_type=MESH).wait_recv()

    def pass_on(t):
        @pl.when(jnp.logical_not(first))
        def _():
            step_out(t).start()

        @pl.when(first & (lax.rem(t, CH) == 0))
        def _():
            for i in range(S):
                final_out(t, i).start()

    def loads(t):
        k = lax.rem(t, NR)
        return [pltpu.make_async_copy(src.at[t], dst.at[k], isem.at[k, i])
                for i, (src, dst) in enumerate(((gates_hbm, gin), (cp_hbm, cin), (hp_hbm, hin), (xs_hbm, xin)))]

    for t in range(T - NR, T):
        for cp in loads(t):
            cp.start()
    plane_wait()
    lax.fori_loop(0, T // CH, lambda k, _: feed(k), 0)
    db_ref[...] = jnp.zeros(db_ref.shape, F32)
    acc[...] = jnp.zeros(acc.shape, F32)
    wcopy.wait()

    def turn(n, _):
        cols = pl.ds(pl.multiple_of(n * HB, HB), HB)
        wt[cols, :] = w[:, cols].T
        return 0

    lax.fori_loop(0, G4 // HB, turn, 0)

    def weight():
        def part(k, _):
            for n in range(0, 2 * H, HB):
                cols = pl.ds(pl.multiple_of(k * 2 * H + n, HB), HB)
                acc[:, cols] += dot(ut[...], dall[:, cols])
            return 0

        lax.fori_loop(0, G4 // (2 * H), part, 0)

    def two(n, state):
        p = T // 2 - 1 - n
        us = []
        for u in (1, 0):
            t = 2 * p + u
            k = lax.rem(t, NR)
            for cp in loads(t):
                cp.wait()

            @pl.when(t < T - 1)
            def _():
                pass_on(t + 1)

            if u == 1:
                @pl.when((p < T // 2 - 1) & (lax.rem(p, CH // 2) == CH // 2 - 1))
                def _():
                    weight()

            arrived(t)
            ea, ec, da, dc_ = state
            dext = rows_of(dbuf[t])
            parts = [[None, None] for _ in range(4)]
            nd = []
            for q in range(2):
                gi, gf, gg, go = (gin[k, :, g * H + q * HB:g * H + q * HB + HB] for g in range(4))
                hq = slice(q * HB, q * HB + HB)
                cprev = cin[k, :, hq]
                th = jnp.tanh(gf * cprev + gi * gg)
                e = dext[:, hq] + (ea, ec)[q]
                dc = (da, dc_)[q] + e * (go * (1.0 - th * th))
                parts[0][q] = dc * (gg * gi * (1.0 - gi))
                parts[1][q] = dc * (cprev * gf * (1.0 - gf))
                parts[2][q] = dc * (gi * (1.0 - gg * gg))
                parts[3][q] = e * (th * go * (1.0 - go))
                nd.append(dc * gf)
            trows = pl.ds(pl.multiple_of(lax.rem(t, CH) * Q, Q), Q)
            lows = []
            for i, v in enumerate(v for ps in parts for v in ps):
                cols = slice(i * HB, i * HB + HB)
                low = v.astype(BF16)
                dall[trows, cols] = low
                lows.append(low)
                db_ref[:, cols] += jnp.sum(v.reshape(Q // R, R, HB), axis=0)
            lowz = jnp.concatenate(lows, axis=1)
            ne = [dot(lowz, wt[:, H + q * HB:H + q * HB + HB]) for q in range(2)]
            for q in range(2):
                hq = slice(q * HB, q * HB + HB)
                dout[t, :, :, hq] = groups_of(dext[:, hq] + dot(lowz, wt[:, hq]))
            state = (ne[0], ne[1], nd[0], nd[1])
            us.append((rows_of(xin[k].astype(F32)), hin[k].astype(F32)))

            @pl.when(t >= NR)
            def _():
                for cp in loads(t - NR):
                    cp.start()

        tcols = pl.ds(pl.multiple_of(lax.rem(p, CH // 2) * 2 * Q, 2 * Q), 2 * Q)
        for j in range(2):
            ut[j * H:j * H + H, tcols] = jnp.concatenate([us[1][j], us[0][j]], axis=0).T.astype(BF16)

        return state

    zero = jnp.zeros((Q, HB), F32)
    lax.fori_loop(0, T // 2, two, (zero,) * 4)
    pass_on(jnp.int32(0))

    weight()
    outs = []
    for i, (dst, (row, step, rows), at) in enumerate(((both, PIECES[0], 0), (give1, PIECES[1], 1 - plane), (give2, PIECES[2], 1 - plane),
                                                      (own1, PIECES[1], plane), (own2, PIECES[2], plane))):
        outs.append(pltpu.make_async_copy(acc.at[pl.ds(pl.multiple_of(row + at * step, R), rows)], dst, osem.at[i]))
        outs[i].start()
    for out in outs:
        out.wait()

    @pl.when(jnp.logical_not(last))
    def _():
        pltpu.make_async_remote_copy(d_hbm, dx_hbm, insem, lastsem, device_id=(top,), device_id_type=MESH).wait_send()

    @pl.when(jnp.logical_not(first))
    def _():
        pltpu.make_async_remote_copy(dout, dbuf, send, recv.at[0], device_id=(prv,), device_id_type=MESH).wait_send()

    @pl.when(first)
    def _():
        others = (slice(None), slice(1, S))
        pltpu.make_async_remote_copy(dout.at[others], dbuf.at[others], send, recv.at[0], device_id=(prv,), device_id_type=MESH).wait_send()

    pltpu.make_async_copy(d_hbm, dx_hbm, lastsem).wait()


def backward(d_top, gates, cprev, hprev, xs, w):
    return pl.pallas_call(
        bwd_kernel,
        out_shape=tuple(jax.ShapeDtypeStruct((rows, G4), F32) for _, _, rows in PIECES + PIECES[1:]) + (jax.ShapeDtypeStruct((R, G4), F32), jax.ShapeDtypeStruct((T, R, H), F32)),
        in_specs=[ANY] * 6,
        out_specs=(HBM,) * 5 + (VMEM, HBM),
        scratch_shapes=[pltpu.VMEM((2 * H, G4), BF16), pltpu.VMEM((G4, 2 * H), BF16), pltpu.VMEM((T, S, R, H), F32),
                        pltpu.VMEM((T, S, R, H), F32), pltpu.VMEM((CH * Q, G4), BF16), pltpu.VMEM((2 * H, CH * Q), BF16), pltpu.VMEM((2 * H, G4), F32)]
        + [pltpu.VMEM((NR, Q, G4), F32), pltpu.VMEM((NR, Q, H), F32), pltpu.VMEM((NR, Q, H), BF16), pltpu.VMEM((NR, S, R, H), BF16)]
        + [DMA((1,)), DMA, DMA((T,)), DMA, DMA, DMA((NR, 4)), DMA((5,))],
        compiler_params=pltpu.CompilerParams(vmem_limit_bytes=56 * MIB, collective_id=1, has_side_effects=True),
        cost_estimate=pl.CostEstimate(flops=110_000_000_000, bytes_accessed=80_000_000, transcendentals=0),
        name="lstm_bwd",
    )(d_top, gates, cprev, hprev, xs, w)


VB = 1280
NVB = V // VB
N = T * R
NW = 4
RB = 64


def head_kernel(x_ref, t_ref, w_hbm, dx_ref, lse_ref, lg, g0, g1, wv, mx, sm, tb, wsem):
    def wcopy(b):
        buf = lax.rem(b, NW)
        return pltpu.make_async_copy(w_hbm.at[:, pl.ds(pl.multiple_of(lax.rem(b, NVB) * VB, VB), VB)], wv.at[buf], wsem.at[buf])

    for b in range(NW - 1):
        wcopy(b).start()

    def ready(b):
        for i in range(2):
            wcopy(b + i).wait()
            wcopy(b + i + 2).start()

    mx[...] = jnp.full(mx.shape, -jnp.inf, F32)
    sm[...] = jnp.zeros(sm.shape, F32)
    dx_ref[...] = jnp.zeros(dx_ref.shape, F32)

    def each(n, act):
        lax.fori_loop(0, n, lambda i, _: (act(i), 0)[1], 0)

    def at(i, size):
        return pl.ds(pl.multiple_of(i * size, size), size)

    def logits(b, cols):
        lg[b, :, cols] = dot(x_ref[...], wv[lax.rem(b, NW), :, cols])

    def sums(b, rows):
        m_old = mx[rows, :]
        m_new = m_old
        for c in range(0, VB, LANE):
            m_new = jnp.maximum(m_new, lg[b, rows, c:c + LANE])
        acc = sm[rows, :] * jnp.exp(m_old - m_new)
        for c in range(0, VB, LANE):
            acc = acc + jnp.exp(lg[b, rows, c:c + LANE] - m_new)
        mx[rows, :] = m_new
        sm[rows, :] = acc

    wcopy(0).wait()
    each(VB // HB, lambda c: logits(0, at(c, HB)))

    def first(h, _):
        b = 2 * h + 1
        ready(b)
        for i in range(2):
            for c in range(0, VB, HB):
                logits(b + i, slice(c, c + HB))
            for r in range(0, N, RB):
                sums(b + i - 1, slice(r, r + RB))
        return 0

    lax.fori_loop(0, NVB // 2, first, 0)
    each(N // RB, lambda r: sums(NVB - 1, at(r, RB)))

    def finish(r):
        rows = at(r, LANE)
        top = jnp.max(mx[rows, :], axis=1, keepdims=True)
        tot = jnp.sum(sm[rows, :] * jnp.exp(mx[rows, :] - top), axis=1, keepdims=True)
        lse = top + jnp.log(tot)
        lse_ref[rows, :] = lse
        mx[rows, :] = jnp.broadcast_to(lse, (LANE, LANE))
        tb[rows, :] = jnp.broadcast_to(t_ref[rows, :], (LANE, LANE))

    each(N // LANE, finish)

    def grads(b, gb, c):
        ids = [b * VB + c + h + lax.broadcasted_iota(jnp.int32, (RB, LANE), 1) for h in (0, LANE)]
        for r in range(0, N, RB):
            rows = slice(r, r + RB)
            lse = mx[rows, :]
            for h in (0, LANE):
                cols = pl.ds(c + h, LANE)
                p = jnp.exp(lg[b, rows, cols] - lse)
                gb[rows, cols] = jnp.where(tb[rows, :] == ids[h // LANE], p - 1.0, p).astype(BF16)

    def apply(b, gb, cols):
        return dot_tt(gb[:, cols], wv[lax.rem(b + NVB, NW), :, cols])

    each(VB // HB, lambda c: grads(0, g0, pl.multiple_of(c * HB, HB)))

    def second(h, _):
        for i in range(2):
            b = 2 * h + NVB + i
            wcopy(b).wait()

            @pl.when(b + 2 < 2 * NVB)
            def _():
                wcopy(b + 2).start()

        for b, gb, gn in ((2 * h, g0, g1), (2 * h + 1, g1, g0)):
            total = jnp.zeros((N, H), F32)
            for c in range(0, VB, HB):
                total = total + apply(b, gb, slice(c, c + HB))
                grads(b + 1, gn, c)
            dx_ref[...] += total
        return 0

    lax.fori_loop(0, NVB // 2, second, 0)
    wcopy(2 * NVB - 1).wait()

    def last(c):
        dx_ref[...] += apply(NVB - 1, g0, at(c, HB))

    each(VB // HB, last)


def head(x, tgt, w_vocab):
    return pl.pallas_call(
        head_kernel,
        out_shape=(jax.ShapeDtypeStruct((N, H), F32), jax.ShapeDtypeStruct((N, 1), F32)),
        in_specs=[VMEM, VMEM, ANY],
        out_specs=(VMEM, VMEM),
        scratch_shapes=[pltpu.VMEM((NVB, N, VB), F32), pltpu.VMEM((N, VB), BF16), pltpu.VMEM((N, VB), BF16), pltpu.VMEM((NW, H, VB), BF16),
                        pltpu.VMEM((N, LANE), F32), pltpu.VMEM((N, LANE), F32), pltpu.VMEM((N, LANE), jnp.int32), DMA((NW,))],
        compiler_params=pltpu.CompilerParams(vmem_limit_bytes=60 * MIB),
        cost_estimate=pl.CostEstimate(flops=40_000_000_000, bytes_accessed=70_000_000, transcendentals=0),
        name="head",
    )(x, tgt, w_vocab)


TB = 768
NTOK = NDEV * N
NK = NTOK // TB
UN = 2
NOWN = (NVB + 1) // 2


def block_of(j, side):
    return j + side * (NVB - 1 - 2 * j)


def dwv_kernel(lo, hi, came, x_hbm, st_ref, w_hbm, *rest):
    nshared = min(hi, NOWN - 1) - lo
    arrived = rest[len(rest) - 15 - 1 - (nshared > 0) - len(came):]
    dw_hbm = arrived[len(came)]
    give_hbm = arrived[len(came) + 1]
    xv, xtv, wv, g0, g1, acc, lse, tgt, box, wsem, xsem, osem, gsem, isem, psem = rest[-15:]
    core = lax.rem(lax.axis_index("data"), 2)

    def cols(b):
        return pl.ds(pl.multiple_of(b * VB, VB), VB)

    def wcopy(i):
        buf = lax.rem(i, 2)
        return pltpu.make_async_copy(w_hbm.at[:, cols(block_of(lo + i, core))], wv.at[buf], wsem.at[buf])

    def keep(i):
        buf = lax.rem(i, 2)
        return pltpu.make_async_copy(acc.at[buf], dw_hbm.at[:, cols(block_of(lo + i, core))], osem.at[buf])

    def give(i):
        buf = lax.rem(i, 2)
        return pltpu.make_async_copy(acc.at[buf], give_hbm.at[i], gsem.at[buf])

    def done(i):
        keep(i).start()

        @pl.when(i < nshared)
        def _():
            give(i).start()

    def drained(i):
        keep(i).wait()

        @pl.when(i < nshared)
        def _():
            give(i).wait()

    pieces = [(src, first, i, r) for src, (first, count) in zip(arrived, came) for i in range(count) for r in range(0, H, LANE)]
    per = -(-len(pieces) // ((hi - lo) * NK // UN))

    def fetch(src, i, r, k, slot):
        return pltpu.make_async_copy(src.at[i, pl.ds(r, LANE)], box.at[k, slot], isem.at[k, slot])

    def put(first, i, r, k, slot):
        return pltpu.make_async_copy(box.at[k, slot], dw_hbm.at[pl.ds(r, LANE), cols(block_of(first + i, 1 - core))], psem.at[k, slot])

    def pieces_of(h, act):
        at = 0
        for src, (first, count) in zip(arrived, came):
            total = count * H // LANE
            for slot in range(per):
                c = h * per + slot - at
                i, r = c // (H // LANE), pl.multiple_of(lax.rem(c, H // LANE) * LANE, LANE)

                @pl.when((c >= 0) & (c < total))
                def _():
                    act(src, first, i, r, lax.rem(h, 2), slot)

            at += total

    def land(src, first, i, r, k, slot):
        fetch(src, i, r, k, slot).wait()
        put(first, i, r, k, slot).start()

    def move(h):
        if came:
            pieces_of(h, land)
            pieces_of(h - 1 + 2 * (h == 0) * len(pieces), lambda src, first, i, r, k, slot: put(first, i, r, k, slot).wait())
            pieces_of(h + 1, lambda src, first, i, r, k, slot: fetch(src, i, r, k, slot).start())

    n = hi - lo
    wcopy(0).start()
    cx = pltpu.make_async_copy(x_hbm, xv, xsem.at[0])
    cx.start()
    cx.wait()

    def turn(k, _):
        for c in range(0, TB, HB):
            rows = pl.ds(pl.multiple_of(k * TB + c, HB), HB)
            xtv[k, :, c:c + HB] = xv[rows, :].T
            lse[rows, :] = jnp.broadcast_to(st_ref[rows, 0:1], (HB, LANE))
            tgt[rows, :] = jnp.broadcast_to(st_ref[rows, LANE - 1:LANE], (HB, LANE))
        return 0

    lax.fori_loop(0, NK, turn, 0)
    if came:
        pieces_of(jnp.int32(0), lambda src, first, i, r, k, slot: fetch(src, i, r, k, slot).start())

    def weight(it, gold, cols, reset=False):
        k, i = lax.rem(it + NK, NK), jnp.maximum(it, 0) // NK
        acc_c = acc.at[lax.rem(i, 2), :, cols]
        old = acc_c[...]
        acc_c[...] = (jnp.where(k == 0, 0.0, old) if reset else old) + dot(xtv[k], gold[:, cols])

    def step(it, u):
        gnew, gold = ((g0, g1), (g1, g0))[u % 2]
        k, i = lax.rem(it, NK) + u, it // NK
        base = pl.multiple_of(k * TB, TB)
        lane = lax.broadcasted_iota(jnp.int32, (R, LANE), 1) + block_of(lo + i, core) * VB
        for c in range(0, VB, HB):
            lgt = dot(xv[pl.ds(base, TB), :], wv[lax.rem(i, 2), :, c:c + HB])
            weight(it + u - 1, gold, slice(c, c + HB), u == 1)
            ids = [jnp.tile((lane + (c + h)).astype(F32), (RB // R, 1)) for h in (0, LANE)]
            for r in range(0, TB, RB):
                here = pl.ds(pl.multiple_of(base + r, RB), RB)
                for h in (0, LANE):
                    p = jnp.exp(lgt[r:r + RB, h:h + LANE] - lse[here, :])
                    gnew[r:r + RB, c + h:c + h + LANE] = jnp.where(tgt[here, :] == ids[h // LANE], p - 1.0, p).astype(BF16)

    def body(h, _):
        it = UN * h
        i0, k0 = it // NK, lax.rem(it, NK)
        move(h)

        @pl.when(k0 == 0)
        def _():
            wcopy(i0).wait()

            @pl.when(i0 < n - 1)
            def _():
                wcopy(i0 + 1).start()

        @pl.when((k0 == 0) & (i0 >= 2))
        def _():
            drained(i0 - 2)

        for u in range(UN):
            step(it, u)

        @pl.when((k0 == UN) & (i0 >= 1))
        def _():
            done(i0 - 1)

        return 0

    lax.fori_loop(0, n * NK // UN, body, 0)

    def last(c, _):
        weight(jnp.int32(n * NK - 1), g1, pl.ds(pl.multiple_of(c * HB, HB), HB))
        return 0

    lax.fori_loop(0, VB // HB, last, 0)
    if n > 1:
        drained(n - 2)
    done(n - 1)
    if came:
        pieces_of(jnp.int32(n * NK // UN - 1), lambda src, first, i, r, k, slot: put(first, i, r, k, slot).wait())
    drained(n - 1)


def grad_vocab(lo, hi, x_all, stats, w_vocab, before=(), came=()):
    counts = tuple((first, v.shape[0]) for first, v in came)
    nshared = min(hi, NOWN - 1) - lo
    out = (jax.ShapeDtypeStruct((H, V), F32), jax.ShapeDtypeStruct((nshared, H, VB), F32))[:1 + (nshared > 0)]
    per = max(1, -(-sum(c for _, c in counts) * (H // LANE) // ((hi - lo) * NK // UN)))
    return pl.pallas_call(
        functools.partial(dwv_kernel, lo, hi, counts),
        out_shape=out,
        in_specs=[ANY, VMEM, ANY] + [HBM] * (len(before) + len(came)),
        out_specs=(HBM,) * len(out),
        input_output_aliases={3: 0} if before else {},
        scratch_shapes=[pltpu.VMEM((NTOK, H), BF16), pltpu.VMEM((NK, H, TB), BF16), pltpu.VMEM((2, H, VB), BF16)]
        + [pltpu.VMEM((TB, VB), BF16)] * 2
        + [pltpu.VMEM((2, H, VB), F32)] + [pltpu.VMEM((NTOK, LANE), F32)] * 2 + [pltpu.VMEM((2, per, LANE, VB), F32)]
        + [DMA((2,)), DMA((1,)), DMA((2,)), DMA((2,)), DMA((2, per)), DMA((2, per))],
        compiler_params=pltpu.CompilerParams(vmem_limit_bytes=62 * MIB),
        cost_estimate=pl.CostEstimate(flops=(hi - lo) * 20_000_000_000, bytes_accessed=100_000_000, transcendentals=0),
        name="dwv",
    )(x_all, stats, w_vocab, *before, *(v for _, v in came))


NC = 8


def copy_ring(n, src, dst, buf, isem, osem):
    def fetch(i):
        k = lax.rem(i, NC)
        return pltpu.make_async_copy(src(i), buf.at[k], isem.at[k])

    def put(i):
        k = lax.rem(i, NC)
        return pltpu.make_async_copy(buf.at[k], dst(i), osem.at[k])

    for i in range(NC // 2):
        fetch(i).start()

    def body(i, _):
        fetch(i).wait()
        put(i).start()

        @pl.when(i >= NC // 2)
        def _():
            put(i - NC // 2).wait()

        @pl.when(i + NC // 2 < n)
        def _():
            fetch(i + NC // 2).start()

        return 0

    lax.fori_loop(0, n, body, 0)
    for i in range(n - NC // 2, n):
        put(i).wait()


def copy_call(kernel, out, block, args):
    return pl.pallas_call(
        kernel,
        out_shape=jax.ShapeDtypeStruct(out, F32),
        in_specs=[HBM] * len(args),
        out_specs=HBM,
        input_output_aliases={1: 0} if len(args) > 1 else {},
        scratch_shapes=[pltpu.VMEM((NC,) + block, F32), DMA((NC,)), DMA((NC,))],
        compiler_params=pltpu.CompilerParams(vmem_limit_bytes=24 * MIB),
        cost_estimate=pl.CostEstimate(flops=20_000_000_000, bytes_accessed=130_000_000, transcendentals=0),
    )(*args)


def land_blocks(first, sent, dwv):
    per = H // LANE

    def kernel(src, _, dst, *scratch):
        other = 1 - lax.rem(lax.axis_index("data"), 2)

        def rows(i):
            return pl.ds(pl.multiple_of(lax.rem(i, per) * LANE, LANE), LANE)

        def target(i):
            return dst.at[rows(i), pl.ds(pl.multiple_of(block_of(first + i // per, other) * VB, VB), VB)]

        copy_ring(sent.shape[0] * per, lambda i: src.at[i // per, rows(i)], target, *scratch)

    return copy_call(kernel, (H, V), (LANE, VB), (sent, dwv))


def place_dw(piece, parts, *before):
    row, step, rows = PIECES[piece]

    def kernel(src, *rest):
        dst, scratch = rest[-4], rest[-3:]

        def target(i):
            return dst.at[gray(lax.rem(i, S)), pl.ds(pl.multiple_of(row + i // S * step, R), rows)]

        copy_ring(parts.shape[0], lambda i: src.at[i, 0:rows], target, *scratch)

    return copy_call(kernel, (L, 2 * H, G4), (rows, G4), (parts,) + before)


SPLITS = (0, 2, 6, NOWN)


def solution(mesh):
    def local_grads(x_rows, tgt_rows, w_lstm, b_lstm, w_vocab):
        tgt = jnp.swapaxes(tgt_rows, 0, 1).reshape(N, 1)
        gates, cprev, hprev, xs, top = forward(jnp.swapaxes(x_rows, 0, 1), w_lstm, b_lstm)
        top = top.reshape(N, H)
        d_top, lse = head(top, tgt, w_vocab)
        half = (N, LANE // 2)
        stats = jnp.concatenate([jnp.broadcast_to(lse, half), jnp.broadcast_to(tgt.astype(F32), half)], axis=1)
        x_all = lax.all_gather(top, 'data', axis=0, tiled=True)
        stats = lax.all_gather(stats, 'data', axis=0, tiled=True)
        d_top, x_all = lax.optimization_barrier((d_top, x_all))
        both, *owns, give1, give2, db, dx = backward(d_top.reshape(T, R, H), gates, cprev, hprev, xs, w_lstm)
        other_plane = [(i, (i + S) % NDEV) for i in range(NDEV)]
        other_core = [(i, i + 1 - 2 * (i % 2)) for i in range(NDEV)]
        planes = [list(range(S)), list(range(S, NDEV))]
        dwv, part, gathered, swapped = (), both, [], []
        for i, (own, give) in enumerate(((both, both), (owns[0], give1), (owns[1], give2))):
            if i:
                give, part = lax.optimization_barrier((give, part))
            got = lax.ppermute(give, 'data', other_plane)
            dwv, sent = grad_vocab(SPLITS[i], SPLITS[i + 1], x_all, stats, w_vocab, dwv, swapped[:1] if i == 2 else ())
            own, dwv = lax.optimization_barrier((own, dwv))
            part = own + got if i != 1 else jnp.concatenate([own + got, db], axis=0)
            part, dwv = lax.optimization_barrier((part, dwv))
            gathered.append(lax.all_gather(part, 'data', axis=0, axis_index_groups=None if i else planes))
            swapped.append((SPLITS[i], lax.ppermute(sent, 'data', other_core)))
            dwv = (dwv,)
        dw = place_dw(0, gathered[0])
        for first, sent in swapped[1:]:
            dwv = (land_blocks(first, sent, *dwv),)
        dw = place_dw(2, gathered[2], place_dw(1, gathered[1], dw))
        db = gathered[1][:, PIECES[1][2]:].reshape(NDEV // S, S, R, G4).sum(axis=(0, 2))
        db = jnp.stack([db[gray(i)] for i in range(L)])
        return dw, db, dwv[0], jnp.swapaxes(dx, 0, 1)

    return jax.shard_map(local_grads, mesh=mesh, in_specs=(P('data'), P('data'), P(), P(), P()), out_specs=(P(), P(), P(), P('data')), check_vma=False)
```

```python
import functools

import jax
import jax.numpy as jnp
from jax import lax
from jax.experimental import pallas as pl
from jax.experimental.pallas import tpu as pltpu
from jax.sharding import PartitionSpec as P

T = 48
R = 8
S = 8
Q = S * R
H = 512
HB = 256
G4 = 4 * H
L = 8
V = 32000
LANE = 128
NDEV = 16
CH = 4
NR = 6
PIECES = ((0, 0, 256), (256, 384, 352), (608, 384, 32))
F32 = jnp.float32
BF16 = jnp.bfloat16
MESH = pl.DeviceIdType.MESH
MIB = 1024 * 1024
ANY = pl.BlockSpec(memory_space=pl.ANY)
VMEM = pl.BlockSpec(memory_space=pltpu.VMEM)
HBM = pl.BlockSpec(memory_space=pltpu.HBM)
DMA = pltpu.SemaphoreType.DMA


def dot(a, b):
    return jnp.dot(a, b, preferred_element_type=F32)


def dot_tt(a, b):
    return lax.dot_general(a, b, (((1,), (1,)), ((), ())), preferred_element_type=F32)


def gray(k):
    chip, core = k // 2, k % 2
    hi, lo = chip // 2, chip % 2
    return 2 * (chip + hi - 2 * hi * lo) + core


LAST = gray(S - 1)


def place():
    me = lax.axis_index("data")
    index = lax.rem(me, S)
    return me - index, index, gray(index)


def plane_signal(base, index):
    barrier = pltpu.get_barrier_semaphore()
    for i in range(1, S):
        pl.semaphore_signal(barrier, inc=1, device_id=(base + lax.rem(index + i, S),), device_id_type=MESH)


def plane_wait():
    pl.semaphore_wait(pltpu.get_barrier_semaphore(), S - 1)


def rows_of(v):
    return v.reshape(Q, v.shape[-1])


def groups_of(v):
    return v.reshape(S, R, v.shape[-1])


def fwd_kernel(x_hbm, w_hbm, b_ref, gates_hbm, cp_hbm, hp_hbm, xs_hbm, xl_hbm,
               w, xbuf, xout, gates, cprev, hprev, z0, z1, wsem, insem, recv, send, lastsem, osem):
    base, index, stage = place()
    first, last = stage == 0, stage == S - 1
    nxt = base + gray(lax.rem(stage + 1, S))
    plane_signal(base, index)
    wcopy = pltpu.make_async_copy(w_hbm.at[stage], w, wsem.at[0])
    wcopy.start()
    plane_wait()

    def feed(k):
        ts = pl.ds(k * CH, CH)

        @pl.when(first)
        def _():
            pltpu.make_async_copy(x_hbm.at[ts], xbuf.at[ts, 0], recv.at[k * CH]).start()

        @pl.when(jnp.logical_not(first))
        def _():
            pltpu.make_async_remote_copy(x_hbm.at[ts], xbuf.at[ts, index], insem, recv.at[k * CH],
                                         device_id=(base,), device_id_type=MESH).start()

        return 0

    def step_out(t):
        return pltpu.make_async_remote_copy(xout.at[t], xbuf.at[t], send, recv.at[t], device_id=(nxt,), device_id_type=MESH)

    def final_out(t, i):
        ts = pl.ds(t, CH)
        if i == LAST:
            return pltpu.make_async_copy(xout.at[ts, i], xl_hbm.at[ts], lastsem)
        return pltpu.make_async_remote_copy(xout.at[ts, i], xl_hbm.at[ts], send, lastsem, device_id=(base + i,), device_id_type=MESH)

    def arrived(t):
        @pl.when(jnp.logical_not(first))
        def _():
            step_out(t).wait_recv()

        @pl.when(first & (lax.rem(t, CH) == 0))
        def _():
            ts = pl.ds(t, CH)
            pltpu.make_async_remote_copy(xout.at[ts], xbuf.at[ts], send, recv.at[t], device_id=(nxt,), device_id_type=MESH).wait_recv()

    def pass_on(t):
        @pl.when(jnp.logical_not(last))
        def _():
            step_out(t).start()

        @pl.when(last & (lax.rem(t, CH) == CH - 1))
        def _():
            for i in range(S):
                final_out(t - CH + 1, i).start()

    lax.fori_loop(0, T // CH, lambda k, _: feed(k), 0)
    bias = b_ref[pl.ds(stage, 1), :]

    def project(zref, t):
        xt = rows_of(xbuf[t].astype(F32)).astype(BF16)
        for n in range(0, G4, HB):
            zref[:, n:n + HB] = dot(xt, w[0:H, n:n + HB]) + bias[:, n:n + HB]

    wcopy.wait()
    arrived(jnp.int32(0))
    project(z0, 0)

    kept = ((gates, gates_hbm), (cprev, cp_hbm), (hprev, hp_hbm), (xbuf, xs_hbm))

    def save(t):
        for i, (src, dst) in enumerate(kept):
            pltpu.make_async_copy(src.at[t], dst.at[t], osem.at[i]).start()

    def two(p, state):
        for u in range(2):
            t = 2 * p + u
            zc, zn = ((z0, z1), (z1, z0))[u]

            @pl.when(t > 0)
            def _():
                pass_on(t - 1)
                save(t - 1)

            @pl.when(t + 1 < T)
            def _():
                arrived(t + 1)

            ha, hc, ca, cc = state
            hlow = jnp.concatenate([ha, hc], axis=1).astype(BF16)
            hprev[t] = hlow
            cprev[t, :, 0:HB] = ca
            cprev[t, :, HB:H] = cc
            nh, nc = [], []
            for q in range(2):
                zz = []
                for g in range(4):
                    cols = slice(g * H + q * HB, g * H + q * HB + HB)
                    zz.append(zc[:, cols] + dot(hlow, w[H:2 * H, cols]))
                gi, gf, gg, go = jax.nn.sigmoid(zz[0]), jax.nn.sigmoid(zz[1]), jnp.tanh(zz[2]), jax.nn.sigmoid(zz[3])
                cn = gf * (ca, cc)[q] + gi * gg
                nh.append(go * jnp.tanh(cn))
                nc.append(cn)
                for g, val in enumerate((gi, gf, gg, go)):
                    gates[t, :, g * H + q * HB:g * H + q * HB + HB] = val
            project(zn, jnp.minimum(t + 1, T - 1))
            xt = rows_of(xbuf[t].astype(F32))
            xout[t] = groups_of(xt + jnp.concatenate(nh, axis=1)).astype(BF16)
            state = (nh[0], nh[1], nc[0], nc[1])
        return state

    zero = jnp.zeros((Q, HB), F32)
    lax.fori_loop(0, T // 2, two, (zero,) * 4)
    pass_on(jnp.int32(T - 1))
    save(T - 1)
    for i, (src, dst) in enumerate(kept):
        pltpu.make_async_copy(src, dst, osem.at[i]).wait()

    @pl.when(jnp.logical_not(first))
    def _():
        pltpu.make_async_remote_copy(x_hbm, xl_hbm, insem, lastsem, device_id=(base,), device_id_type=MESH).wait_send()

    @pl.when(jnp.logical_not(last))
    def _():
        pltpu.make_async_remote_copy(xout, xbuf, send, recv.at[0], device_id=(nxt,), device_id_type=MESH).wait_send()

    @pl.when(last)
    def _():
        others = (slice(None), slice(0, S - 1))
        pltpu.make_async_remote_copy(xout.at[others], xbuf.at[others], send, recv.at[0], device_id=(nxt,), device_id_type=MESH).wait_send()

    pltpu.make_async_copy(x_hbm, xl_hbm, lastsem).wait()


def forward(x, w, b):
    return pl.pallas_call(
        fwd_kernel,
        out_shape=(jax.ShapeDtypeStruct((T, Q, G4), F32), jax.ShapeDtypeStruct((T, Q, H), F32),
                   jax.ShapeDtypeStruct((T, Q, H), BF16), jax.ShapeDtypeStruct((T, S, R, H), BF16),
                   jax.ShapeDtypeStruct((T, R, H), BF16)),
        in_specs=[ANY, ANY, VMEM],
        out_specs=(HBM,) * 5,
        scratch_shapes=[pltpu.VMEM((2 * H, G4), BF16), pltpu.VMEM((T, S, R, H), BF16), pltpu.VMEM((T, S, R, H), BF16),
                        pltpu.VMEM((T, Q, G4), F32), pltpu.VMEM((T, Q, H), F32), pltpu.VMEM((T, Q, H), BF16)]
        + [pltpu.VMEM((Q, G4), F32)] * 2 + [DMA((1,)), DMA, DMA((T,)), DMA, DMA, DMA((4,))],
        compiler_params=pltpu.CompilerParams(vmem_limit_bytes=52 * MIB, collective_id=0, has_side_effects=True),
        cost_estimate=pl.CostEstimate(flops=60_000_000_000, bytes_accessed=80_000_000, transcendentals=0),
        name="lstm_fwd",
    )(x, w, b)


def bwd_kernel(d_hbm, gates_hbm, cp_hbm, hp_hbm, xs_hbm, w_hbm, both, own1, own2, give1, give2, db_ref, dx_hbm,
               w, wt, dbuf, dout, dall, ut, acc, gin, cin, hin, xin,
               wsem, insem, recv, send, lastsem, isem, osem):
    base, index, stage = place()
    plane = base // S
    first, last = stage == 0, stage == S - 1
    prv = base + gray(lax.rem(stage + S - 1, S))
    top = base + LAST
    plane_signal(base, index)
    wcopy = pltpu.make_async_copy(w_hbm.at[stage], w, wsem.at[0])
    wcopy.start()

    def feed(k):
        t = T - CH - k * CH
        ts = pl.ds(t, CH)

        @pl.when(last)
        def _():
            pltpu.make_async_copy(d_hbm.at[ts], dbuf.at[ts, LAST], recv.at[t]).start()

        @pl.when(jnp.logical_not(last))
        def _():
            pltpu.make_async_remote_copy(d_hbm.at[ts], dbuf.at[ts, index], insem, recv.at[t],
                                         device_id=(top,), device_id_type=MESH).start()

        return 0

    def step_out(t):
        return pltpu.make_async_remote_copy(dout.at[t], dbuf.at[t], send, recv.at[t], device_id=(prv,), device_id_type=MESH)

    def final_out(t, i):
        ts = pl.ds(t, CH)
        if i == 0:
            return pltpu.make_async_copy(dout.at[ts, i], dx_hbm.at[ts], lastsem)
        return pltpu.make_async_remote_copy(dout.at[ts, i], dx_hbm.at[ts], send, lastsem, device_id=(base + i,), device_id_type=MESH)

    def arrived(t):
        @pl.when(jnp.logical_not(last))
        def _():
            step_out(t).wait_recv()

        @pl.when(last & (lax.rem(t, CH) == CH - 1))
        def _():
            ts = pl.ds(t - CH + 1, CH)
            pltpu.make_async_remote_copy(dout.at[ts], dbuf.at[ts], send, recv.at[t - CH + 1], device_id=(prv,), device_id_type=MESH).wait_recv()

    def pass_on(t):
        @pl.when(jnp.logical_not(first))
        def _():
            step_out(t).start()

        @pl.when(first & (lax.rem(t, CH) == 0))
        def _():
            for i in range(S):
                final_out(t, i).start()

    def loads(t):
        k = lax.rem(t, NR)
        return [pltpu.make_async_copy(src.at[t], dst.at[k], isem.at[k, i])
                for i, (src, dst) in enumerate(((gates_hbm, gin), (cp_hbm, cin), (hp_hbm, hin), (xs_hbm, xin)))]

    for t in range(T - NR, T):
        for cp in loads(t):
            cp.start()
    plane_wait()
    lax.fori_loop(0, T // CH, lambda k, _: feed(k), 0)
    db_ref[...] = jnp.zeros(db_ref.shape, F32)
    acc[...] = jnp.zeros(acc.shape, F32)
    wcopy.wait()

    def turn(n, _):
        cols = pl.ds(pl.multiple_of(n * HB, HB), HB)
        wt[cols, :] = w[:, cols].T
        return 0

    lax.fori_loop(0, G4 // HB, turn, 0)

    def weight():
        for n in range(0, G4, HB):
            acc[:, n:n + HB] += dot(ut[...], dall[:, n:n + HB])

    def two(n, state):
        p = T // 2 - 1 - n
        us = []
        for u in (1, 0):
            t = 2 * p + u
            k = lax.rem(t, NR)
            for cp in loads(t):
                cp.wait()

            @pl.when(t < T - 1)
            def _():
                pass_on(t + 1)

            if u == 1:
                @pl.when((p < T // 2 - 1) & (lax.rem(p, CH // 2) == CH // 2 - 1))
                def _():
                    weight()

            arrived(t)
            ea, ec, da, dc_ = state
            dext = rows_of(dbuf[t])
            parts = [[None, None] for _ in range(4)]
            nd = []
            for q in range(2):
                gi, gf, gg, go = (gin[k, :, g * H + q * HB:g * H + q * HB + HB] for g in range(4))
                hq = slice(q * HB, q * HB + HB)
                cprev = cin[k, :, hq]
                th = jnp.tanh(gf * cprev + gi * gg)
                e = dext[:, hq] + (ea, ec)[q]
                dc = (da, dc_)[q] + e * (go * (1.0 - th * th))
                parts[0][q] = dc * (gg * gi * (1.0 - gi))
                parts[1][q] = dc * (cprev * gf * (1.0 - gf))
                parts[2][q] = dc * (gi * (1.0 - gg * gg))
                parts[3][q] = e * (th * go * (1.0 - go))
                nd.append(dc * gf)
            trows = pl.ds(pl.multiple_of(lax.rem(t, CH) * Q, Q), Q)
            lows = []
            for i, v in enumerate(v for ps in parts for v in ps):
                cols = slice(i * HB, i * HB + HB)
                low = v.astype(BF16)
                dall[trows, cols] = low
                lows.append(low)
                db_ref[:, cols] += jnp.sum(v.reshape(Q // R, R, HB), axis=0)
            lowz = jnp.concatenate(lows, axis=1)
            ne = [dot(lowz, wt[:, H + q * HB:H + q * HB + HB]) for q in range(2)]
            for q in range(2):
                hq = slice(q * HB, q * HB + HB)
                dout[t, :, :, hq] = groups_of(dext[:, hq] + dot(lowz, wt[:, hq]))
            state = (ne[0], ne[1], nd[0], nd[1])
            us.append((rows_of(xin[k].astype(F32)), hin[k].astype(F32)))

            @pl.when(t >= NR)
            def _():
                for cp in loads(t - NR):
                    cp.start()

        tcols = pl.ds(pl.multiple_of(lax.rem(p, CH // 2) * 2 * Q, 2 * Q), 2 * Q)
        for j in range(2):
            ut[j * H:j * H + H, tcols] = jnp.concatenate([us[1][j], us[0][j]], axis=0).T.astype(BF16)

        return state

    zero = jnp.zeros((Q, HB), F32)
    lax.fori_loop(0, T // 2, two, (zero,) * 4)
    pass_on(jnp.int32(0))

    weight()
    outs = []
    for i, (dst, (row, step, rows), at) in enumerate(((both, PIECES[0], 0), (give1, PIECES[1], 1 - plane), (give2, PIECES[2], 1 - plane),
                                                      (own1, PIECES[1], plane), (own2, PIECES[2], plane))):
        outs.append(pltpu.make_async_copy(acc.at[pl.ds(pl.multiple_of(row + at * step, R), rows)], dst, osem.at[i]))
        outs[i].start()
    for out in outs:
        out.wait()

    @pl.when(jnp.logical_not(last))
    def _():
        pltpu.make_async_remote_copy(d_hbm, dx_hbm, insem, lastsem, device_id=(top,), device_id_type=MESH).wait_send()

    @pl.when(jnp.logical_not(first))
    def _():
        pltpu.make_async_remote_copy(dout, dbuf, send, recv.at[0], device_id=(prv,), device_id_type=MESH).wait_send()

    @pl.when(first)
    def _():
        others = (slice(None), slice(1, S))
        pltpu.make_async_remote_copy(dout.at[others], dbuf.at[others], send, recv.at[0], device_id=(prv,), device_id_type=MESH).wait_send()

    pltpu.make_async_copy(d_hbm, dx_hbm, lastsem).wait()


def backward(d_top, gates, cprev, hprev, xs, w):
    return pl.pallas_call(
        bwd_kernel,
        out_shape=tuple(jax.ShapeDtypeStruct((rows, G4), F32) for _, _, rows in PIECES + PIECES[1:]) + (jax.ShapeDtypeStruct((R, G4), F32), jax.ShapeDtypeStruct((T, R, H), F32)),
        in_specs=[ANY] * 6,
        out_specs=(HBM,) * 5 + (VMEM, HBM),
        scratch_shapes=[pltpu.VMEM((2 * H, G4), BF16), pltpu.VMEM((G4, 2 * H), BF16), pltpu.VMEM((T, S, R, H), F32),
                        pltpu.VMEM((T, S, R, H), F32), pltpu.VMEM((CH * Q, G4), BF16), pltpu.VMEM((2 * H, CH * Q), BF16), pltpu.VMEM((2 * H, G4), F32)]
        + [pltpu.VMEM((NR, Q, G4), F32), pltpu.VMEM((NR, Q, H), F32), pltpu.VMEM((NR, Q, H), BF16), pltpu.VMEM((NR, S, R, H), BF16)]
        + [DMA((1,)), DMA, DMA((T,)), DMA, DMA, DMA((NR, 4)), DMA((5,))],
        compiler_params=pltpu.CompilerParams(vmem_limit_bytes=56 * MIB, collective_id=1, has_side_effects=True),
        cost_estimate=pl.CostEstimate(flops=110_000_000_000, bytes_accessed=80_000_000, transcendentals=0),
        name="lstm_bwd",
    )(d_top, gates, cprev, hprev, xs, w)


VB = 1280
NVB = V // VB
N = T * R
CHUNKS = ((0, 512), (512, 512), (1024, 256))
NW = 4
RB = 64


def head_kernel(x_ref, t_ref, w_hbm, dx_ref, lse_ref, lg, g0, g1, wv, mx, sm, tb, wsem):
    def wcopy(b):
        buf = lax.rem(b, NW)
        return pltpu.make_async_copy(w_hbm.at[:, pl.ds(pl.multiple_of(lax.rem(b, NVB) * VB, VB), VB)], wv.at[buf], wsem.at[buf])

    for b in range(NW - 1):
        wcopy(b).start()

    def ready(b):
        for i in range(2):
            wcopy(b + i).wait()
            wcopy(b + i + 2).start()

    mx[...] = jnp.full(mx.shape, -jnp.inf, F32)
    sm[...] = jnp.zeros(sm.shape, F32)
    dx_ref[...] = jnp.zeros(dx_ref.shape, F32)

    def logits(b, c, size):
        part = dot(x_ref[...], wv[lax.rem(b, NW), :, c:c + size])
        lg[b, :, c:c + size] = part
        for r in range(0, N, RB):
            rows = slice(r, r + RB)
            vals = [part[rows, h:h + LANE] for h in range(0, size, LANE)]
            m_old = mx[rows, :]
            m_new = functools.reduce(jnp.maximum, vals, m_old)
            mx[rows, :] = m_new
            sm[rows, :] = functools.reduce(jnp.add, [jnp.exp(v - m_new) for v in vals], sm[rows, :] * jnp.exp(m_old - m_new))

    def block(b):
        for c, size in CHUNKS:
            logits(b, c, size)

    wcopy(0).wait()
    block(0)

    def first(h, _):
        b = 2 * h + 1
        ready(b)
        for i in range(2):
            block(b + i)
        return 0

    lax.fori_loop(0, NVB // 2, first, 0)

    def finish(r):
        rows = slice(r, r + LANE)
        top = jnp.max(mx[rows, :], axis=1, keepdims=True)
        tot = jnp.sum(sm[rows, :] * jnp.exp(mx[rows, :] - top), axis=1, keepdims=True)
        lse = top + jnp.log(tot)
        lse_ref[rows, :] = lse
        mx[rows, :] = jnp.broadcast_to(lse, (LANE, LANE))
        tb[rows, :] = jnp.broadcast_to(t_ref[rows, :], (LANE, LANE))

    for r in range(0, N, LANE):
        finish(r)

    def grads(b, gb, c):
        ids = [b * VB + c + h + lax.broadcasted_iota(jnp.int32, (RB, LANE), 1) for h in (0, LANE)]
        for r in range(0, N, RB):
            rows = slice(r, r + RB)
            lse = mx[rows, :]
            for h in (0, LANE):
                cols = pl.ds(c + h, LANE)
                p = jnp.exp(lg[b, rows, cols] - lse)
                gb[rows, cols] = jnp.where(tb[rows, :] == ids[h // LANE], p - 1.0, p).astype(BF16)

    def apply(b, gb, cols):
        return dot_tt(gb[:, cols], wv[lax.rem(b + NVB, NW), :, cols])

    for c in range(0, VB, HB):
        grads(0, g0, c)

    def second(h, _):
        for i in range(2):
            b = 2 * h + NVB + i
            wcopy(b).wait()

            @pl.when(b + 2 < 2 * NVB)
            def _():
                wcopy(b + 2).start()

        for b, gb, gn in ((2 * h, g0, g1), (2 * h + 1, g1, g0)):
            total = jnp.zeros((N, H), F32)
            for c in range(0, VB, HB):
                total = total + apply(b, gb, slice(c, c + HB))
                grads(b + 1, gn, c)
            dx_ref[...] += total
        return 0

    lax.fori_loop(0, NVB // 2, second, 0)
    wcopy(2 * NVB - 1).wait()
    for c in range(0, VB, HB):
        dx_ref[...] += apply(NVB - 1, g0, slice(c, c + HB))


def head(x, tgt, w_vocab):
    return pl.pallas_call(
        head_kernel,
        out_shape=(jax.ShapeDtypeStruct((N, H), F32), jax.ShapeDtypeStruct((N, 1), F32)),
        in_specs=[VMEM, VMEM, ANY],
        out_specs=(VMEM, VMEM),
        scratch_shapes=[pltpu.VMEM((NVB, N, VB), F32), pltpu.VMEM((N, VB), BF16), pltpu.VMEM((N, VB), BF16), pltpu.VMEM((NW, H, VB), BF16),
                        pltpu.VMEM((N, LANE), F32), pltpu.VMEM((N, LANE), F32), pltpu.VMEM((N, LANE), jnp.int32), DMA((NW,))],
        compiler_params=pltpu.CompilerParams(vmem_limit_bytes=60 * MIB),
        cost_estimate=pl.CostEstimate(flops=40_000_000_000, bytes_accessed=70_000_000, transcendentals=0),
        name="head",
    )(x, tgt, w_vocab)


TB = 768
NTOK = NDEV * N
NK = NTOK // TB
UN = 2
NOWN = (NVB + 1) // 2


def block_of(j, side):
    return j + side * (NVB - 1 - 2 * j)


def dwv_kernel(lo, hi, came, x_hbm, st_ref, w_hbm, *rest):
    nshared = min(hi, NOWN - 1) - lo
    arrived = rest[len(rest) - 15 - 1 - (nshared > 0) - len(came):]
    dw_hbm = arrived[len(came)]
    give_hbm = arrived[len(came) + 1]
    xv, xtv, wv, g0, g1, acc, lse, tgt, box, wsem, xsem, osem, gsem, isem, psem = rest[-15:]
    core = lax.rem(lax.axis_index("data"), 2)

    def cols(b):
        return pl.ds(pl.multiple_of(b * VB, VB), VB)

    def wcopy(i):
        buf = lax.rem(i, 2)
        return pltpu.make_async_copy(w_hbm.at[:, cols(block_of(lo + i, core))], wv.at[buf], wsem.at[buf])

    def keep(i):
        buf = lax.rem(i, 2)
        return pltpu.make_async_copy(acc.at[buf], dw_hbm.at[:, cols(block_of(lo + i, core))], osem.at[buf])

    def give(i):
        buf = lax.rem(i, 2)
        return pltpu.make_async_copy(acc.at[buf], give_hbm.at[i], gsem.at[buf])

    def done(i):
        keep(i).start()

        @pl.when(i < nshared)
        def _():
            give(i).start()

    def drained(i):
        keep(i).wait()

        @pl.when(i < nshared)
        def _():
            give(i).wait()

    pieces = [(src, first, i, r) for src, (first, count) in zip(arrived, came) for i in range(count) for r in range(0, H, LANE)]
    per = -(-len(pieces) // ((hi - lo) * NK // UN))

    def fetch(src, i, r, k, slot):
        return pltpu.make_async_copy(src.at[i, pl.ds(r, LANE)], box.at[k, slot], isem.at[k, slot])

    def put(first, i, r, k, slot):
        return pltpu.make_async_copy(box.at[k, slot], dw_hbm.at[pl.ds(r, LANE), cols(block_of(first + i, 1 - core))], psem.at[k, slot])

    def pieces_of(h, act):
        at = 0
        for src, (first, count) in zip(arrived, came):
            total = count * H // LANE
            for slot in range(per):
                c = h * per + slot - at
                i, r = c // (H // LANE), pl.multiple_of(lax.rem(c, H // LANE) * LANE, LANE)

                @pl.when((c >= 0) & (c < total))
                def _():
                    act(src, first, i, r, lax.rem(h, 2), slot)

            at += total

    def land(src, first, i, r, k, slot):
        fetch(src, i, r, k, slot).wait()
        put(first, i, r, k, slot).start()

    def move(h):
        if came:
            pieces_of(h, land)
            pieces_of(h - 1 + 2 * (h == 0) * len(pieces), lambda src, first, i, r, k, slot: put(first, i, r, k, slot).wait())
            pieces_of(h + 1, lambda src, first, i, r, k, slot: fetch(src, i, r, k, slot).start())

    n = hi - lo
    wcopy(0).start()

    def xcopy(k):
        rows = pl.ds(k * TB, TB)
        return pltpu.make_async_copy(x_hbm.at[rows], xv.at[rows], xsem.at[k])

    for k in range(NK):
        xcopy(k).start()

    def turn(k, _):
        xcopy(k).wait()
        for c in range(0, TB, HB):
            rows = pl.ds(pl.multiple_of(k * TB + c, HB), HB)
            xtv[k, :, c:c + HB] = xv[rows, :].T
            lse[rows, :] = jnp.broadcast_to(st_ref[rows, 0:1], (HB, LANE))
            tgt[rows, :] = jnp.broadcast_to(st_ref[rows, LANE - 1:LANE], (HB, LANE))
        return 0

    lax.fori_loop(0, NK, turn, 0)
    if came:
        pieces_of(jnp.int32(0), lambda src, first, i, r, k, slot: fetch(src, i, r, k, slot).start())

    def weight(it, gold, cols, reset=False):
        k, i = lax.rem(it + NK, NK), jnp.maximum(it, 0) // NK
        acc_c = acc.at[lax.rem(i, 2), :, cols]
        old = acc_c[...]
        acc_c[...] = (jnp.where(k == 0, 0.0, old) if reset else old) + dot(xtv[k], gold[:, cols])

    def step(it, u):
        gnew, gold = ((g0, g1), (g1, g0))[u % 2]
        k, i = lax.rem(it, NK) + u, it // NK
        base = pl.multiple_of(k * TB, TB)
        lane = lax.broadcasted_iota(jnp.int32, (R, LANE), 1) + block_of(lo + i, core) * VB
        for c in range(0, VB, HB):
            lgt = dot(xv[pl.ds(base, TB), :], wv[lax.rem(i, 2), :, c:c + HB])
            weight(it + u - 1, gold, slice(c, c + HB), u == 1)
            ids = [jnp.tile((lane + (c + h)).astype(F32), (RB // R, 1)) for h in (0, LANE)]
            for r in range(0, TB, RB):
                here = pl.ds(pl.multiple_of(base + r, RB), RB)
                for h in (0, LANE):
                    p = jnp.exp(lgt[r:r + RB, h:h + LANE] - lse[here, :])
                    gnew[r:r + RB, c + h:c + h + LANE] = jnp.where(tgt[here, :] == ids[h // LANE], p - 1.0, p).astype(BF16)

    def body(h, _):
        it = UN * h
        i0, k0 = it // NK, lax.rem(it, NK)
        move(h)

        @pl.when(k0 == 0)
        def _():
            wcopy(i0).wait()

            @pl.when(i0 < n - 1)
            def _():
                wcopy(i0 + 1).start()

        @pl.when((k0 == 0) & (i0 >= 2))
        def _():
            drained(i0 - 2)

        for u in range(UN):
            step(it, u)

        @pl.when((k0 == UN) & (i0 >= 1))
        def _():
            done(i0 - 1)

        return 0

    lax.fori_loop(0, n * NK // UN, body, 0)

    def last(c, _):
        weight(jnp.int32(n * NK - 1), g1, pl.ds(pl.multiple_of(c * HB, HB), HB))
        return 0

    lax.fori_loop(0, VB // HB, last, 0)
    if n > 1:
        drained(n - 2)
    done(n - 1)
    if came:
        pieces_of(jnp.int32(n * NK // UN - 1), lambda src, first, i, r, k, slot: put(first, i, r, k, slot).wait())
    drained(n - 1)


def grad_vocab(lo, hi, x_all, stats, w_vocab, before=(), came=()):
    counts = tuple((first, v.shape[0]) for first, v in came)
    nshared = min(hi, NOWN - 1) - lo
    out = (jax.ShapeDtypeStruct((H, V), F32), jax.ShapeDtypeStruct((nshared, H, VB), F32))[:1 + (nshared > 0)]
    per = max(1, -(-sum(c for _, c in counts) * (H // LANE) // ((hi - lo) * NK // UN)))
    return pl.pallas_call(
        functools.partial(dwv_kernel, lo, hi, counts),
        out_shape=out,
        in_specs=[ANY, VMEM, ANY] + [HBM] * (len(before) + len(came)),
        out_specs=(HBM,) * len(out),
        input_output_aliases={3: 0} if before else {},
        scratch_shapes=[pltpu.VMEM((NTOK, H), BF16), pltpu.VMEM((NK, H, TB), BF16), pltpu.VMEM((2, H, VB), BF16)]
        + [pltpu.VMEM((TB, VB), BF16)] * 2
        + [pltpu.VMEM((2, H, VB), F32)] + [pltpu.VMEM((NTOK, LANE), F32)] * 2 + [pltpu.VMEM((2, per, LANE, VB), F32)]
        + [DMA((2,)), DMA((NK,)), DMA((2,)), DMA((2,)), DMA((2, per)), DMA((2, per))],
        compiler_params=pltpu.CompilerParams(vmem_limit_bytes=62 * MIB),
        cost_estimate=pl.CostEstimate(flops=(hi - lo) * 20_000_000_000, bytes_accessed=100_000_000, transcendentals=0),
        name="dwv",
    )(x_all, stats, w_vocab, *before, *(v for _, v in came))


NC = 8


def copy_ring(n, src, dst, buf, isem, osem):
    def fetch(i):
        k = lax.rem(i, NC)
        return pltpu.make_async_copy(src(i), buf.at[k], isem.at[k])

    def put(i):
        k = lax.rem(i, NC)
        return pltpu.make_async_copy(buf.at[k], dst(i), osem.at[k])

    for i in range(NC // 2):
        fetch(i).start()

    def body(i, _):
        fetch(i).wait()
        put(i).start()

        @pl.when(i >= NC // 2)
        def _():
            put(i - NC // 2).wait()

        @pl.when(i + NC // 2 < n)
        def _():
            fetch(i + NC // 2).start()

        return 0

    lax.fori_loop(0, n, body, 0)
    for i in range(n - NC // 2, n):
        put(i).wait()


def copy_call(kernel, out, block, args):
    return pl.pallas_call(
        kernel,
        out_shape=jax.ShapeDtypeStruct(out, F32),
        in_specs=[HBM] * len(args),
        out_specs=HBM,
        input_output_aliases={1: 0} if len(args) > 1 else {},
        scratch_shapes=[pltpu.VMEM((NC,) + block, F32), DMA((NC,)), DMA((NC,))],
        compiler_params=pltpu.CompilerParams(vmem_limit_bytes=24 * MIB),
        cost_estimate=pl.CostEstimate(flops=20_000_000_000, bytes_accessed=130_000_000, transcendentals=0),
    )(*args)


def land_blocks(first, sent, dwv):
    per = H // LANE

    def kernel(src, _, dst, *scratch):
        other = 1 - lax.rem(lax.axis_index("data"), 2)

        def rows(i):
            return pl.ds(pl.multiple_of(lax.rem(i, per) * LANE, LANE), LANE)

        def target(i):
            return dst.at[rows(i), pl.ds(pl.multiple_of(block_of(first + i // per, other) * VB, VB), VB)]

        copy_ring(sent.shape[0] * per, lambda i: src.at[i // per, rows(i)], target, *scratch)

    return copy_call(kernel, (H, V), (LANE, VB), (sent, dwv))


def place_dw(piece, parts, *before):
    row, step, rows = PIECES[piece]

    def kernel(src, *rest):
        dst, scratch = rest[-4], rest[-3:]

        def target(i):
            return dst.at[gray(lax.rem(i, S)), pl.ds(pl.multiple_of(row + i // S * step, R), rows)]

        copy_ring(parts.shape[0], lambda i: src.at[i, 0:rows], target, *scratch)

    return copy_call(kernel, (L, 2 * H, G4), (rows, G4), (parts,) + before)


SPLITS = (0, 2, 6, NOWN)


def solution(mesh):
    def local_grads(x_rows, tgt_rows, w_lstm, b_lstm, w_vocab):
        tgt = jnp.swapaxes(tgt_rows, 0, 1).reshape(N, 1)
        gates, cprev, hprev, xs, top = forward(jnp.swapaxes(x_rows, 0, 1), w_lstm, b_lstm)
        top = top.reshape(N, H)
        d_top, lse = head(top, tgt, w_vocab)
        half = (N, LANE // 2)
        stats = jnp.concatenate([jnp.broadcast_to(lse, half), jnp.broadcast_to(tgt.astype(F32), half)], axis=1)
        x_all = lax.all_gather(top, 'data', axis=0, tiled=True)
        stats = lax.all_gather(stats, 'data', axis=0, tiled=True)
        d_top, x_all = lax.optimization_barrier((d_top, x_all))
        both, *owns, give1, give2, db, dx = backward(d_top.reshape(T, R, H), gates, cprev, hprev, xs, w_lstm)
        other_plane = [(i, (i + S) % NDEV) for i in range(NDEV)]
        other_core = [(i, i + 1 - 2 * (i % 2)) for i in range(NDEV)]
        planes = [list(range(S)), list(range(S, NDEV))]
        dwv, part, gathered, swapped = (), both, [], []
        for i, (own, give) in enumerate(((both, both), (owns[0], give1), (owns[1], give2))):
            if i:
                give, part = lax.optimization_barrier((give, part))
            got = lax.ppermute(give, 'data', other_plane)
            dwv, sent = grad_vocab(SPLITS[i], SPLITS[i + 1], x_all, stats, w_vocab, dwv, swapped[:1] if i == 2 else ())
            own, dwv = lax.optimization_barrier((own, dwv))
            part = own + got if i != 1 else jnp.concatenate([own + got, db], axis=0)
            part, dwv = lax.optimization_barrier((part, dwv))
            gathered.append(lax.all_gather(part, 'data', axis=0, axis_index_groups=None if i else planes))
            swapped.append((SPLITS[i], lax.ppermute(sent, 'data', other_core)))
            dwv = (dwv,)
        dw = place_dw(0, gathered[0])
        for first, sent in swapped[1:]:
            dwv = (land_blocks(first, sent, *dwv),)
        dw = place_dw(2, gathered[2], place_dw(1, gathered[1], dw))
        db = gathered[1][:, PIECES[1][2]:].reshape(NDEV // S, S, R, G4).sum(axis=(0, 2))
        db = jnp.stack([db[gray(i)] for i in range(L)])
        return dw, db, dwv[0], jnp.swapaxes(dx, 0, 1)

    return jax.shard_map(local_grads, mesh=mesh, in_specs=(P('data'), P('data'), P(), P(), P()), out_specs=(P(), P(), P(), P('data')), check_vma=False)
```

```python
import functools

import jax
import jax.numpy as jnp
from jax import lax
from jax.experimental import pallas as pl
from jax.experimental.pallas import tpu as pltpu
from jax.sharding import PartitionSpec as P

T = 48
R = 8
S = 8
Q = S * R
H = 512
HB = 256
G4 = 4 * H
L = 8
V = 32000
LANE = 128
NDEV = 16
CH = 4
NR = 6
PIECES = ((0, 0, 256), (256, 384, 352), (608, 384, 32))
F32 = jnp.float32
BF16 = jnp.bfloat16
MESH = pl.DeviceIdType.MESH
MIB = 1024 * 1024
ANY = pl.BlockSpec(memory_space=pl.ANY)
VMEM = pl.BlockSpec(memory_space=pltpu.VMEM)
HBM = pl.BlockSpec(memory_space=pltpu.HBM)
DMA = pltpu.SemaphoreType.DMA


def dot(a, b):
    return jnp.dot(a, b, preferred_element_type=F32)


def dot_tt(a, b):
    return lax.dot_general(a, b, (((1,), (1,)), ((), ())), preferred_element_type=F32)


def gray(k):
    chip, core = k // 2, k % 2
    hi, lo = chip // 2, chip % 2
    return 2 * (chip + hi - 2 * hi * lo) + core


LAST = gray(S - 1)


def place():
    me = lax.axis_index("data")
    index = lax.rem(me, S)
    return me - index, index, gray(index)


def plane_signal(base, index):
    barrier = pltpu.get_barrier_semaphore()
    for i in range(1, S):
        pl.semaphore_signal(barrier, inc=1, device_id=(base + lax.rem(index + i, S),), device_id_type=MESH)


def plane_wait():
    pl.semaphore_wait(pltpu.get_barrier_semaphore(), S - 1)


def rows_of(v):
    return v.reshape(Q, v.shape[-1])


def groups_of(v):
    return v.reshape(S, R, v.shape[-1])


def fwd_kernel(x_hbm, w_hbm, b_ref, gates_hbm, cp_hbm, hp_hbm, xs_hbm, xl_hbm,
               w, xbuf, xout, gates, cprev, hprev, wsem, insem, recv, send, lastsem, osem):
    base, index, stage = place()
    first, last = stage == 0, stage == S - 1
    nxt = base + gray(lax.rem(stage + 1, S))
    plane_signal(base, index)
    wcopy = pltpu.make_async_copy(w_hbm.at[stage], w, wsem.at[0])
    wcopy.start()
    plane_wait()

    def feed(k):
        ts = pl.ds(k * CH, CH)

        @pl.when(first)
        def _():
            pltpu.make_async_copy(x_hbm.at[ts], xbuf.at[ts, 0], recv.at[k * CH]).start()

        @pl.when(jnp.logical_not(first))
        def _():
            pltpu.make_async_remote_copy(x_hbm.at[ts], xbuf.at[ts, index], insem, recv.at[k * CH],
                                         device_id=(base,), device_id_type=MESH).start()

        return 0

    def step_out(t):
        return pltpu.make_async_remote_copy(xout.at[t], xbuf.at[t], send, recv.at[t], device_id=(nxt,), device_id_type=MESH)

    def final_out(t, i):
        ts = pl.ds(t, CH)
        if i == LAST:
            return pltpu.make_async_copy(xout.at[ts, i], xl_hbm.at[ts], lastsem)
        return pltpu.make_async_remote_copy(xout.at[ts, i], xl_hbm.at[ts], send, lastsem, device_id=(base + i,), device_id_type=MESH)

    def arrived(t):
        @pl.when(jnp.logical_not(first))
        def _():
            step_out(t).wait_recv()

        @pl.when(first & (lax.rem(t, CH) == 0))
        def _():
            ts = pl.ds(t, CH)
            pltpu.make_async_remote_copy(xout.at[ts], xbuf.at[ts], send, recv.at[t], device_id=(nxt,), device_id_type=MESH).wait_recv()

    def pass_on(t):
        @pl.when(jnp.logical_not(last))
        def _():
            step_out(t).start()

        @pl.when(last & (lax.rem(t, CH) == CH - 1))
        def _():
            for i in range(S):
                final_out(t - CH + 1, i).start()

    lax.fori_loop(0, T // CH, lambda k, _: feed(k), 0)
    bias = b_ref[pl.ds(stage, 1), :]

    wcopy.wait()

    kept = ((gates, gates_hbm), (cprev, cp_hbm), (hprev, hp_hbm), (xbuf, xs_hbm))

    def save(t):
        for i, (src, dst) in enumerate(kept):
            pltpu.make_async_copy(src.at[t], dst.at[t], osem.at[i]).start()

    def two(p, state):
        for u in range(2):
            t = 2 * p + u

            @pl.when(t > 0)
            def _():
                pass_on(t - 1)
                save(t - 1)

            arrived(t)
            ha, hc, ca, cc = state
            xt = rows_of(xbuf[t].astype(F32))
            xlow = xt.astype(BF16)
            hlow = jnp.concatenate([ha, hc], axis=1).astype(BF16)
            hprev[t] = hlow
            cprev[t, :, 0:HB] = ca
            cprev[t, :, HB:H] = cc
            nh, nc = [], []
            for q in range(2):
                zz = []
                for g in range(4):
                    cols = slice(g * H + q * HB, g * H + q * HB + HB)
                    zz.append(dot(xlow, w[0:H, cols]) + dot(hlow, w[H:2 * H, cols]) + bias[:, cols])
                gi, gf, gg, go = jax.nn.sigmoid(zz[0]), jax.nn.sigmoid(zz[1]), jnp.tanh(zz[2]), jax.nn.sigmoid(zz[3])
                cn = gf * (ca, cc)[q] + gi * gg
                nh.append(go * jnp.tanh(cn))
                nc.append(cn)
                for g, val in enumerate((gi, gf, gg, go)):
                    gates[t, :, g * H + q * HB:g * H + q * HB + HB] = val
            xout[t] = groups_of(xt + jnp.concatenate(nh, axis=1)).astype(BF16)
            state = (nh[0], nh[1], nc[0], nc[1])
        return state

    zero = jnp.zeros((Q, HB), F32)
    lax.fori_loop(0, T // 2, two, (zero,) * 4)
    pass_on(jnp.int32(T - 1))
    save(T - 1)
    for i, (src, dst) in enumerate(kept):
        pltpu.make_async_copy(src, dst, osem.at[i]).wait()

    @pl.when(jnp.logical_not(first))
    def _():
        pltpu.make_async_remote_copy(x_hbm, xl_hbm, insem, lastsem, device_id=(base,), device_id_type=MESH).wait_send()

    @pl.when(jnp.logical_not(last))
    def _():
        pltpu.make_async_remote_copy(xout, xbuf, send, recv.at[0], device_id=(nxt,), device_id_type=MESH).wait_send()

    @pl.when(last)
    def _():
        others = (slice(None), slice(0, S - 1))
        pltpu.make_async_remote_copy(xout.at[others], xbuf.at[others], send, recv.at[0], device_id=(nxt,), device_id_type=MESH).wait_send()

    pltpu.make_async_copy(x_hbm, xl_hbm, lastsem).wait()


def forward(x, w, b):
    return pl.pallas_call(
        fwd_kernel,
        out_shape=(jax.ShapeDtypeStruct((T, Q, G4), F32), jax.ShapeDtypeStruct((T, Q, H), F32),
                   jax.ShapeDtypeStruct((T, Q, H), BF16), jax.ShapeDtypeStruct((T, S, R, H), BF16),
                   jax.ShapeDtypeStruct((T, R, H), BF16)),
        in_specs=[ANY, ANY, VMEM],
        out_specs=(HBM,) * 5,
        scratch_shapes=[pltpu.VMEM((2 * H, G4), BF16), pltpu.VMEM((T, S, R, H), BF16), pltpu.VMEM((T, S, R, H), BF16),
                        pltpu.VMEM((T, Q, G4), F32), pltpu.VMEM((T, Q, H), F32), pltpu.VMEM((T, Q, H), BF16)]
        + [DMA((1,)), DMA, DMA((T,)), DMA, DMA, DMA((4,))],
        compiler_params=pltpu.CompilerParams(vmem_limit_bytes=52 * MIB, collective_id=0, has_side_effects=True),
        cost_estimate=pl.CostEstimate(flops=60_000_000_000, bytes_accessed=80_000_000, transcendentals=0),
        name="lstm_fwd",
    )(x, w, b)


def bwd_kernel(d_hbm, gates_hbm, cp_hbm, hp_hbm, xs_hbm, w_hbm, both, own1, own2, give1, give2, db_ref, dx_hbm,
               w, wt, dbuf, dout, dall, ut, acc, gin, cin, hin, xin,
               wsem, insem, recv, send, lastsem, isem, osem):
    base, index, stage = place()
    plane = base // S
    first, last = stage == 0, stage == S - 1
    prv = base + gray(lax.rem(stage + S - 1, S))
    top = base + LAST
    plane_signal(base, index)
    wcopy = pltpu.make_async_copy(w_hbm.at[stage], w, wsem.at[0])
    wcopy.start()

    def feed(k):
        t = T - CH - k * CH
        ts = pl.ds(t, CH)

        @pl.when(last)
        def _():
            pltpu.make_async_copy(d_hbm.at[ts], dbuf.at[ts, LAST], recv.at[t]).start()

        @pl.when(jnp.logical_not(last))
        def _():
            pltpu.make_async_remote_copy(d_hbm.at[ts], dbuf.at[ts, index], insem, recv.at[t],
                                         device_id=(top,), device_id_type=MESH).start()

        return 0

    def step_out(t):
        return pltpu.make_async_remote_copy(dout.at[t], dbuf.at[t], send, recv.at[t], device_id=(prv,), device_id_type=MESH)

    def final_out(t, i):
        ts = pl.ds(t, CH)
        if i == 0:
            return pltpu.make_async_copy(dout.at[ts, i], dx_hbm.at[ts], lastsem)
        return pltpu.make_async_remote_copy(dout.at[ts, i], dx_hbm.at[ts], send, lastsem, device_id=(base + i,), device_id_type=MESH)

    def arrived(t):
        @pl.when(jnp.logical_not(last))
        def _():
            step_out(t).wait_recv()

        @pl.when(last & (lax.rem(t, CH) == CH - 1))
        def _():
            ts = pl.ds(t - CH + 1, CH)
            pltpu.make_async_remote_copy(dout.at[ts], dbuf.at[ts], send, recv.at[t - CH + 1], device_id=(prv,), device_id_type=MESH).wait_recv()

    def pass_on(t):
        @pl.when(jnp.logical_not(first))
        def _():
            step_out(t).start()

        @pl.when(first & (lax.rem(t, CH) == 0))
        def _():
            for i in range(S):
                final_out(t, i).start()

    def loads(t):
        k = lax.rem(t, NR)
        return [pltpu.make_async_copy(src.at[t], dst.at[k], isem.at[k, i])
                for i, (src, dst) in enumerate(((gates_hbm, gin), (cp_hbm, cin), (hp_hbm, hin), (xs_hbm, xin)))]

    for t in range(T - NR, T):
        for cp in loads(t):
            cp.start()
    plane_wait()
    lax.fori_loop(0, T // CH, lambda k, _: feed(k), 0)
    db_ref[...] = jnp.zeros(db_ref.shape, F32)
    acc[...] = jnp.zeros(acc.shape, F32)
    wcopy.wait()

    def turn(n, _):
        cols = pl.ds(pl.multiple_of(n * HB, HB), HB)
        wt[cols, :] = w[:, cols].T
        return 0

    lax.fori_loop(0, G4 // HB, turn, 0)

    def weight():
        for n in range(0, G4, HB):
            acc[:, n:n + HB] += dot(ut[...], dall[:, n:n + HB])

    def two(n, state):
        p = T // 2 - 1 - n
        us = []
        for u in (1, 0):
            t = 2 * p + u
            k = lax.rem(t, NR)
            for cp in loads(t):
                cp.wait()

            @pl.when(t < T - 1)
            def _():
                pass_on(t + 1)

            if u == 1:
                @pl.when((p < T // 2 - 1) & (lax.rem(p, CH // 2) == CH // 2 - 1))
                def _():
                    weight()

            arrived(t)
            ea, ec, da, dc_ = state
            dext = rows_of(dbuf[t])
            parts = [[None, None] for _ in range(4)]
            nd = []
            for q in range(2):
                gi, gf, gg, go = (gin[k, :, g * H + q * HB:g * H + q * HB + HB] for g in range(4))
                hq = slice(q * HB, q * HB + HB)
                cprev = cin[k, :, hq]
                th = jnp.tanh(gf * cprev + gi * gg)
                e = dext[:, hq] + (ea, ec)[q]
                dc = (da, dc_)[q] + e * (go * (1.0 - th * th))
                parts[0][q] = dc * (gg * gi * (1.0 - gi))
                parts[1][q] = dc * (cprev * gf * (1.0 - gf))
                parts[2][q] = dc * (gi * (1.0 - gg * gg))
                parts[3][q] = e * (th * go * (1.0 - go))
                nd.append(dc * gf)
            trows = pl.ds(pl.multiple_of(lax.rem(t, CH) * Q, Q), Q)
            lows = []
            for i, v in enumerate(v for ps in parts for v in ps):
                cols = slice(i * HB, i * HB + HB)
                low = v.astype(BF16)
                dall[trows, cols] = low
                lows.append(low)
                db_ref[:, cols] += jnp.sum(v.reshape(Q // R, R, HB), axis=0)
            lowz = jnp.concatenate(lows, axis=1)
            ne = [dot(lowz, wt[:, H + q * HB:H + q * HB + HB]) for q in range(2)]
            for q in range(2):
                hq = slice(q * HB, q * HB + HB)
                dout[t, :, :, hq] = groups_of(dext[:, hq] + dot(lowz, wt[:, hq]))
            state = (ne[0], ne[1], nd[0], nd[1])
            us.append((rows_of(xin[k].astype(F32)), hin[k].astype(F32)))

            @pl.when(t >= NR)
            def _():
                for cp in loads(t - NR):
                    cp.start()

        tcols = pl.ds(pl.multiple_of(lax.rem(p, CH // 2) * 2 * Q, 2 * Q), 2 * Q)
        for j in range(2):
            ut[j * H:j * H + H, tcols] = jnp.concatenate([us[1][j], us[0][j]], axis=0).T.astype(BF16)

        return state

    zero = jnp.zeros((Q, HB), F32)
    lax.fori_loop(0, T // 2, two, (zero,) * 4)
    pass_on(jnp.int32(0))

    weight()
    outs = []
    for i, (dst, (row, step, rows), at) in enumerate(((both, PIECES[0], 0), (give1, PIECES[1], 1 - plane), (give2, PIECES[2], 1 - plane),
                                                      (own1, PIECES[1], plane), (own2, PIECES[2], plane))):
        outs.append(pltpu.make_async_copy(acc.at[pl.ds(pl.multiple_of(row + at * step, R), rows)], dst, osem.at[i]))
        outs[i].start()
    for out in outs:
        out.wait()

    @pl.when(jnp.logical_not(last))
    def _():
        pltpu.make_async_remote_copy(d_hbm, dx_hbm, insem, lastsem, device_id=(top,), device_id_type=MESH).wait_send()

    @pl.when(jnp.logical_not(first))
    def _():
        pltpu.make_async_remote_copy(dout, dbuf, send, recv.at[0], device_id=(prv,), device_id_type=MESH).wait_send()

    @pl.when(first)
    def _():
        others = (slice(None), slice(1, S))
        pltpu.make_async_remote_copy(dout.at[others], dbuf.at[others], send, recv.at[0], device_id=(prv,), device_id_type=MESH).wait_send()

    pltpu.make_async_copy(d_hbm, dx_hbm, lastsem).wait()


def backward(d_top, gates, cprev, hprev, xs, w):
    return pl.pallas_call(
        bwd_kernel,
        out_shape=tuple(jax.ShapeDtypeStruct((rows, G4), F32) for _, _, rows in PIECES + PIECES[1:]) + (jax.ShapeDtypeStruct((R, G4), F32), jax.ShapeDtypeStruct((T, R, H), F32)),
        in_specs=[ANY] * 6,
        out_specs=(HBM,) * 5 + (VMEM, HBM),
        scratch_shapes=[pltpu.VMEM((2 * H, G4), BF16), pltpu.VMEM((G4, 2 * H), BF16), pltpu.VMEM((T, S, R, H), F32),
                        pltpu.VMEM((T, S, R, H), F32), pltpu.VMEM((CH * Q, G4), BF16), pltpu.VMEM((2 * H, CH * Q), BF16), pltpu.VMEM((2 * H, G4), F32)]
        + [pltpu.VMEM((NR, Q, G4), F32), pltpu.VMEM((NR, Q, H), F32), pltpu.VMEM((NR, Q, H), BF16), pltpu.VMEM((NR, S, R, H), BF16)]
        + [DMA((1,)), DMA, DMA((T,)), DMA, DMA, DMA((NR, 4)), DMA((5,))],
        compiler_params=pltpu.CompilerParams(vmem_limit_bytes=56 * MIB, collective_id=1, has_side_effects=True),
        cost_estimate=pl.CostEstimate(flops=110_000_000_000, bytes_accessed=80_000_000, transcendentals=0),
        name="lstm_bwd",
    )(d_top, gates, cprev, hprev, xs, w)


VB = 1280
NVB = V // VB
N = T * R
CHUNKS = ((0, 512), (512, 512), (1024, 256))
NW = 4
RB = 64


def head_kernel(x_ref, t_ref, w_hbm, dx_ref, stats_ref, lg, g0, g1, wv, mx, sm, tb, wsem):
    def wcopy(b):
        buf = lax.rem(b, NW)
        return pltpu.make_async_copy(w_hbm.at[:, pl.ds(pl.multiple_of(lax.rem(b, NVB) * VB, VB), VB)], wv.at[buf], wsem.at[buf])

    for b in range(NW - 1):
        wcopy(b).start()

    def ready(b):
        for i in range(2):
            wcopy(b + i).wait()
            wcopy(b + i + 2).start()

    mx[...] = jnp.full(mx.shape, -jnp.inf, F32)
    sm[...] = jnp.zeros(sm.shape, F32)
    dx_ref[...] = jnp.zeros(dx_ref.shape, F32)

    def logits(b, c, size):
        part = dot(x_ref[...], wv[lax.rem(b, NW), :, c:c + size])
        lg[b, :, c:c + size] = part
        for r in range(0, N, RB):
            rows = slice(r, r + RB)
            vals = [part[rows, h:h + LANE] for h in range(0, size, LANE)]
            m_old = mx[rows, :]
            m_new = functools.reduce(jnp.maximum, vals, m_old)
            mx[rows, :] = m_new
            sm[rows, :] = functools.reduce(jnp.add, [jnp.exp(v - m_new) for v in vals], sm[rows, :] * jnp.exp(m_old - m_new))

    def block(b):
        for c, size in CHUNKS:
            logits(b, c, size)

    wcopy(0).wait()
    block(0)

    def first(h, _):
        b = 2 * h + 1
        ready(b)
        for i in range(2):
            block(b + i)
        return 0

    lax.fori_loop(0, NVB // 2, first, 0)

    def finish(r):
        rows = slice(r, r + LANE)
        top = jnp.max(mx[rows, :], axis=1, keepdims=True)
        tot = jnp.sum(sm[rows, :] * jnp.exp(mx[rows, :] - top), axis=1, keepdims=True)
        lse = top + jnp.log(tot)
        mx[rows, :] = jnp.broadcast_to(lse, (LANE, LANE))
        tb[rows, :] = jnp.broadcast_to(t_ref[rows, :], (LANE, LANE))
        lane = lax.broadcasted_iota(jnp.int32, (LANE, LANE), 1)
        stats_ref[rows, :] = jnp.where(lane < LANE // 2, mx[rows, :], tb[rows, :].astype(F32))

    for r in range(0, N, LANE):
        finish(r)

    def grads(b, gb, c):
        ids = [b * VB + c + h + lax.broadcasted_iota(jnp.int32, (RB, LANE), 1) for h in (0, LANE)]
        for r in range(0, N, RB):
            rows = slice(r, r + RB)
            lse = mx[rows, :]
            for h in (0, LANE):
                cols = pl.ds(c + h, LANE)
                p = jnp.exp(lg[b, rows, cols] - lse)
                gb[rows, cols] = jnp.where(tb[rows, :] == ids[h // LANE], p - 1.0, p).astype(BF16)

    def apply(b, gb, cols):
        return dot_tt(gb[:, cols], wv[lax.rem(b + NVB, NW), :, cols])

    for c in range(0, VB, HB):
        grads(0, g0, c)

    def second(h, _):
        for i in range(2):
            b = 2 * h + NVB + i
            wcopy(b).wait()

            @pl.when(b + 2 < 2 * NVB)
            def _():
                wcopy(b + 2).start()

        for b, gb, gn in ((2 * h, g0, g1), (2 * h + 1, g1, g0)):
            total = jnp.zeros((N, H), F32)
            for c in range(0, VB, HB):
                total = total + apply(b, gb, slice(c, c + HB))
                grads(b + 1, gn, c)
            dx_ref[...] += total
        return 0

    lax.fori_loop(0, NVB // 2, second, 0)
    wcopy(2 * NVB - 1).wait()
    for c in range(0, VB, HB):
        dx_ref[...] += apply(NVB - 1, g0, slice(c, c + HB))


def head(x, tgt, w_vocab):
    return pl.pallas_call(
        head_kernel,
        out_shape=(jax.ShapeDtypeStruct((N, H), F32), jax.ShapeDtypeStruct((N, LANE), F32)),
        in_specs=[VMEM, VMEM, ANY],
        out_specs=(VMEM, VMEM),
        scratch_shapes=[pltpu.VMEM((NVB, N, VB), F32), pltpu.VMEM((N, VB), BF16), pltpu.VMEM((N, VB), BF16), pltpu.VMEM((NW, H, VB), BF16),
                        pltpu.VMEM((N, LANE), F32), pltpu.VMEM((N, LANE), F32), pltpu.VMEM((N, LANE), jnp.int32), DMA((NW,))],
        compiler_params=pltpu.CompilerParams(vmem_limit_bytes=60 * MIB),
        cost_estimate=pl.CostEstimate(flops=40_000_000_000, bytes_accessed=70_000_000, transcendentals=0),
        name="head",
    )(x, tgt, w_vocab)


TB = 768
NTOK = NDEV * N
NK = NTOK // TB
UN = 2
NOWN = (NVB + 1) // 2


def block_of(j, side):
    return j + side * (NVB - 1 - 2 * j)


def dwv_kernel(lo, hi, came, x_hbm, st_ref, w_hbm, *rest):
    nshared = min(hi, NOWN - 1) - lo
    arrived = rest[len(rest) - 15 - 1 - (nshared > 0) - len(came):]
    dw_hbm = arrived[len(came)]
    give_hbm = arrived[len(came) + 1]
    xv, xtv, wv, g0, g1, acc, lse, tgt, box, wsem, xsem, osem, gsem, isem, psem = rest[-15:]
    core = lax.rem(lax.axis_index("data"), 2)

    def cols(b):
        return pl.ds(pl.multiple_of(b * VB, VB), VB)

    def wcopy(i):
        buf = lax.rem(i, 2)
        return pltpu.make_async_copy(w_hbm.at[:, cols(block_of(lo + i, core))], wv.at[buf], wsem.at[buf])

    def keep(i):
        buf = lax.rem(i, 2)
        return pltpu.make_async_copy(acc.at[buf], dw_hbm.at[:, cols(block_of(lo + i, core))], osem.at[buf])

    def give(i):
        buf = lax.rem(i, 2)
        return pltpu.make_async_copy(acc.at[buf], give_hbm.at[i], gsem.at[buf])

    def done(i):
        keep(i).start()

        @pl.when(i < nshared)
        def _():
            give(i).start()

    def drained(i):
        keep(i).wait()

        @pl.when(i < nshared)
        def _():
            give(i).wait()

    pieces = [(src, first, i, r) for src, (first, count) in zip(arrived, came) for i in range(count) for r in range(0, H, LANE)]
    per = -(-len(pieces) // ((hi - lo) * NK // UN))

    def fetch(src, i, r, k, slot):
        return pltpu.make_async_copy(src.at[i, pl.ds(r, LANE)], box.at[k, slot], isem.at[k, slot])

    def put(first, i, r, k, slot):
        return pltpu.make_async_copy(box.at[k, slot], dw_hbm.at[pl.ds(r, LANE), cols(block_of(first + i, 1 - core))], psem.at[k, slot])

    def pieces_of(h, act):
        at = 0
        for src, (first, count) in zip(arrived, came):
            total = count * H // LANE
            for slot in range(per):
                c = h * per + slot - at
                i, r = c // (H // LANE), pl.multiple_of(lax.rem(c, H // LANE) * LANE, LANE)

                @pl.when((c >= 0) & (c < total))
                def _():
                    act(src, first, i, r, lax.rem(h, 2), slot)

            at += total

    def land(src, first, i, r, k, slot):
        fetch(src, i, r, k, slot).wait()
        put(first, i, r, k, slot).start()

    def move(h):
        if came:
            pieces_of(h, land)
            pieces_of(h - 1 + 2 * (h == 0) * len(pieces), lambda src, first, i, r, k, slot: put(first, i, r, k, slot).wait())
            pieces_of(h + 1, lambda src, first, i, r, k, slot: fetch(src, i, r, k, slot).start())

    n = hi - lo
    wcopy(0).start()

    def xcopy(k):
        rows = pl.ds(k * TB, TB)
        return pltpu.make_async_copy(x_hbm.at[rows], xv.at[rows], xsem.at[k])

    for k in range(NK):
        xcopy(k).start()

    def turn(k, _):
        xcopy(k).wait()
        for c in range(0, TB, HB):
            rows = pl.ds(pl.multiple_of(k * TB + c, HB), HB)
            xtv[k, :, c:c + HB] = xv[rows, :].T
            lse[rows, :] = jnp.broadcast_to(st_ref[rows, 0:1], (HB, LANE))
            tgt[rows, :] = jnp.broadcast_to(st_ref[rows, LANE - 1:LANE], (HB, LANE))
        return 0

    lax.fori_loop(0, NK, turn, 0)
    if came:
        pieces_of(jnp.int32(0), lambda src, first, i, r, k, slot: fetch(src, i, r, k, slot).start())

    def weight(it, gold, cols, reset=False):
        k, i = lax.rem(it + NK, NK), jnp.maximum(it, 0) // NK
        acc_c = acc.at[lax.rem(i, 2), :, cols]
        old = acc_c[...]
        acc_c[...] = (jnp.where(k == 0, 0.0, old) if reset else old) + dot(xtv[k], gold[:, cols])

    def step(it, u):
        gnew, gold = ((g0, g1), (g1, g0))[u % 2]
        k, i = lax.rem(it, NK) + u, it // NK
        base = pl.multiple_of(k * TB, TB)
        lane = lax.broadcasted_iota(jnp.int32, (R, LANE), 1) + block_of(lo + i, core) * VB
        for c in range(0, VB, HB):
            lgt = dot(xv[pl.ds(base, TB), :], wv[lax.rem(i, 2), :, c:c + HB])
            weight(it + u - 1, gold, slice(c, c + HB), u == 1)
            ids = [jnp.tile((lane + (c + h)).astype(F32), (RB // R, 1)) for h in (0, LANE)]
            for r in range(0, TB, RB):
                here = pl.ds(pl.multiple_of(base + r, RB), RB)
                for h in (0, LANE):
                    p = jnp.exp(lgt[r:r + RB, h:h + LANE] - lse[here, :])
                    gnew[r:r + RB, c + h:c + h + LANE] = jnp.where(tgt[here, :] == ids[h // LANE], p - 1.0, p).astype(BF16)

    def body(h, _):
        it = UN * h
        i0, k0 = it // NK, lax.rem(it, NK)
        move(h)

        @pl.when(k0 == 0)
        def _():
            wcopy(i0).wait()

            @pl.when(i0 < n - 1)
            def _():
                wcopy(i0 + 1).start()

        @pl.when((k0 == 0) & (i0 >= 2))
        def _():
            drained(i0 - 2)

        for u in range(UN):
            step(it, u)

        @pl.when((k0 == UN) & (i0 >= 1))
        def _():
            done(i0 - 1)

        return 0

    lax.fori_loop(0, n * NK // UN, body, 0)

    def last(c, _):
        weight(jnp.int32(n * NK - 1), g1, pl.ds(pl.multiple_of(c * HB, HB), HB))
        return 0

    lax.fori_loop(0, VB // HB, last, 0)
    if n > 1:
        drained(n - 2)
    done(n - 1)
    if came:
        pieces_of(jnp.int32(n * NK // UN - 1), lambda src, first, i, r, k, slot: put(first, i, r, k, slot).wait())
    drained(n - 1)


def grad_vocab(lo, hi, x_all, stats, w_vocab, before=(), came=()):
    counts = tuple((first, v.shape[0]) for first, v in came)
    nshared = min(hi, NOWN - 1) - lo
    out = (jax.ShapeDtypeStruct((H, V), F32), jax.ShapeDtypeStruct((nshared, H, VB), F32))[:1 + (nshared > 0)]
    per = max(1, -(-sum(c for _, c in counts) * (H // LANE) // ((hi - lo) * NK // UN)))
    return pl.pallas_call(
        functools.partial(dwv_kernel, lo, hi, counts),
        out_shape=out,
        in_specs=[ANY, VMEM, ANY] + [HBM] * (len(before) + len(came)),
        out_specs=(HBM,) * len(out),
        input_output_aliases={3: 0} if before else {},
        scratch_shapes=[pltpu.VMEM((NTOK, H), BF16), pltpu.VMEM((NK, H, TB), BF16), pltpu.VMEM((2, H, VB), BF16)]
        + [pltpu.VMEM((TB, VB), BF16)] * 2
        + [pltpu.VMEM((2, H, VB), F32)] + [pltpu.VMEM((NTOK, LANE), F32)] * 2 + [pltpu.VMEM((2, per, LANE, VB), F32)]
        + [DMA((2,)), DMA((NK,)), DMA((2,)), DMA((2,)), DMA((2, per)), DMA((2, per))],
        compiler_params=pltpu.CompilerParams(vmem_limit_bytes=62 * MIB),
        cost_estimate=pl.CostEstimate(flops=(hi - lo) * 20_000_000_000, bytes_accessed=100_000_000, transcendentals=0),
        name="dwv",
    )(x_all, stats, w_vocab, *before, *(v for _, v in came))


NC = 8


def copy_ring(n, src, dst, buf, isem, osem):
    def fetch(i):
        k = lax.rem(i, NC)
        return pltpu.make_async_copy(src(i), buf.at[k], isem.at[k])

    def put(i):
        k = lax.rem(i, NC)
        return pltpu.make_async_copy(buf.at[k], dst(i), osem.at[k])

    for i in range(NC // 2):
        fetch(i).start()

    def body(i, _):
        fetch(i).wait()
        put(i).start()

        @pl.when(i >= NC // 2)
        def _():
            put(i - NC // 2).wait()

        @pl.when(i + NC // 2 < n)
        def _():
            fetch(i + NC // 2).start()

        return 0

    lax.fori_loop(0, n, body, 0)
    for i in range(n - NC // 2, n):
        put(i).wait()


def copy_call(kernel, out, block, args):
    return pl.pallas_call(
        kernel,
        out_shape=jax.ShapeDtypeStruct(out, F32),
        in_specs=[HBM] * len(args),
        out_specs=HBM,
        input_output_aliases={1: 0} if len(args) > 1 else {},
        scratch_shapes=[pltpu.VMEM((NC,) + block, F32), DMA((NC,)), DMA((NC,))],
        compiler_params=pltpu.CompilerParams(vmem_limit_bytes=24 * MIB),
        cost_estimate=pl.CostEstimate(flops=20_000_000_000, bytes_accessed=130_000_000, transcendentals=0),
    )(*args)


def land_blocks(first, sent, dwv):
    per = H // LANE

    def kernel(src, _, dst, *scratch):
        other = 1 - lax.rem(lax.axis_index("data"), 2)

        def rows(i):
            return pl.ds(pl.multiple_of(lax.rem(i, per) * LANE, LANE), LANE)

        def target(i):
            return dst.at[rows(i), pl.ds(pl.multiple_of(block_of(first + i // per, other) * VB, VB), VB)]

        copy_ring(sent.shape[0] * per, lambda i: src.at[i // per, rows(i)], target, *scratch)

    return copy_call(kernel, (H, V), (LANE, VB), (sent, dwv))


def place_dw(piece, parts, *before):
    row, step, rows = PIECES[piece]

    def kernel(src, *rest):
        dst, scratch = rest[-4], rest[-3:]

        def target(i):
            return dst.at[gray(lax.rem(i, S)), pl.ds(pl.multiple_of(row + i // S * step, R), rows)]

        copy_ring(parts.shape[0], lambda i: src.at[i, 0:rows], target, *scratch)

    return copy_call(kernel, (L, 2 * H, G4), (rows, G4), (parts,) + before)


SPLITS = (0, 2, 6, NOWN)


def solution(mesh):
    def local_grads(x_rows, tgt_rows, w_lstm, b_lstm, w_vocab):
        tgt = jnp.swapaxes(tgt_rows, 0, 1).reshape(N, 1)
        gates, cprev, hprev, xs, top = forward(jnp.swapaxes(x_rows, 0, 1), w_lstm, b_lstm)
        top = top.reshape(N, H)
        d_top, stats = head(top, tgt, w_vocab)
        x_all = lax.all_gather(top, 'data', axis=0, tiled=True)
        stats = lax.all_gather(stats, 'data', axis=0, tiled=True)
        d_top, x_all = lax.optimization_barrier((d_top, x_all))
        both, *owns, give1, give2, db, dx = backward(d_top.reshape(T, R, H), gates, cprev, hprev, xs, w_lstm)
        other_plane = [(i, (i + S) % NDEV) for i in range(NDEV)]
        other_core = [(i, i + 1 - 2 * (i % 2)) for i in range(NDEV)]
        planes = [list(range(S)), list(range(S, NDEV))]
        dwv, part, gathered, swapped = (), both, [], []
        for i, (own, give) in enumerate(((both, both), (owns[0], give1), (owns[1], give2))):
            if i:
                give, part = lax.optimization_barrier((give, part))
            got = lax.ppermute(give, 'data', other_plane)
            dwv, sent = grad_vocab(SPLITS[i], SPLITS[i + 1], x_all, stats, w_vocab, dwv, swapped[:1] if i == 2 else ())
            own, dwv = lax.optimization_barrier((own, dwv))
            part = own + got if i != 1 else jnp.concatenate([own + got, db], axis=0)
            part, dwv = lax.optimization_barrier((part, dwv))
            gathered.append(lax.all_gather(part, 'data', axis=0, axis_index_groups=None if i else planes))
            swapped.append((SPLITS[i], lax.ppermute(sent, 'data', other_core)))
            dwv = (dwv,)
        dw = place_dw(0, gathered[0])
        for first, sent in swapped[1:]:
            dwv = (land_blocks(first, sent, *dwv),)
        dw = place_dw(2, gathered[2], place_dw(1, gathered[1], dw))
        db = gathered[1][:, PIECES[1][2]:].reshape(NDEV // S, S, R, G4).sum(axis=(0, 2))
        db = jnp.stack([db[gray(i)] for i in range(L)])
        return dw, db, dwv[0], jnp.swapaxes(dx, 0, 1)

    return jax.shard_map(local_grads, mesh=mesh, in_specs=(P('data'), P('data'), P(), P(), P()), out_specs=(P(), P(), P(), P('data')), check_vma=False)
```

```python
import functools

import jax
import jax.numpy as jnp
from jax import lax
from jax.experimental import pallas as pl
from jax.experimental.pallas import tpu as pltpu
from jax.sharding import PartitionSpec as P

T = 48
R = 8
S = 8
Q = S * R
H = 512
HB = 256
G4 = 4 * H
L = 8
V = 32000
LANE = 128
NDEV = 16
CO = 2
CH = 4
NR = 6
PIECES = ((0, 0, 256), (256, 384, 352), (608, 384, 32))
F32 = jnp.float32
BF16 = jnp.bfloat16
MESH = pl.DeviceIdType.MESH
MIB = 1024 * 1024
ANY = pl.BlockSpec(memory_space=pl.ANY)
VMEM = pl.BlockSpec(memory_space=pltpu.VMEM)
HBM = pl.BlockSpec(memory_space=pltpu.HBM)
DMA = pltpu.SemaphoreType.DMA


def dot(a, b):
    return jnp.dot(a, b, preferred_element_type=F32)


def dot_tt(a, b):
    return lax.dot_general(a, b, (((1,), (1,)), ((), ())), preferred_element_type=F32)


def gray(k):
    chip, core = k // 2, k % 2
    hi, lo = chip // 2, chip % 2
    return 2 * (chip + hi - 2 * hi * lo) + core


LAST = gray(S - 1)


def place():
    me = lax.axis_index("data")
    index = lax.rem(me, S)
    return me - index, index, gray(index)


def plane_signal(base, index):
    barrier = pltpu.get_barrier_semaphore()
    for i in range(1, S):
        pl.semaphore_signal(barrier, inc=1, device_id=(base + lax.rem(index + i, S),), device_id_type=MESH)


def plane_wait():
    pl.semaphore_wait(pltpu.get_barrier_semaphore(), S - 1)


def rows_of(v):
    return v.reshape(Q, v.shape[-1])


def groups_of(v):
    return v.reshape(S, R, v.shape[-1])


def fwd_kernel(x_hbm, w_hbm, b_ref, gates_hbm, cp_hbm, hp_hbm, xs_hbm, xl_hbm,
               w, xbuf, xout, gates, cprev, hprev, wsem, insem, recv, send, lastsem, osem):
    base, index, stage = place()
    first, last = stage == 0, stage == S - 1
    nxt = base + gray(lax.rem(stage + 1, S))
    plane_signal(base, index)
    wcopy = pltpu.make_async_copy(w_hbm.at[stage], w, wsem.at[0])
    wcopy.start()
    plane_wait()

    def feed(k):
        ts = pl.ds(k * CO, CO)

        @pl.when(first)
        def _():
            pltpu.make_async_copy(x_hbm.at[ts], xbuf.at[ts, 0], recv.at[k * CO]).start()

        @pl.when(jnp.logical_not(first))
        def _():
            pltpu.make_async_remote_copy(x_hbm.at[ts], xbuf.at[ts, index], insem, recv.at[k * CO],
                                         device_id=(base,), device_id_type=MESH).start()

        return 0

    def step_out(t):
        return pltpu.make_async_remote_copy(xout.at[t], xbuf.at[t], send, recv.at[t], device_id=(nxt,), device_id_type=MESH)

    def final_out(t, i):
        ts = pl.ds(t, CO)
        if i == LAST:
            return pltpu.make_async_copy(xout.at[ts, i], xl_hbm.at[ts], lastsem)
        return pltpu.make_async_remote_copy(xout.at[ts, i], xl_hbm.at[ts], send, lastsem, device_id=(base + i,), device_id_type=MESH)

    def arrived(t):
        @pl.when(jnp.logical_not(first))
        def _():
            step_out(t).wait_recv()

        @pl.when(first & (lax.rem(t, CO) == 0))
        def _():
            ts = pl.ds(t, CO)
            pltpu.make_async_remote_copy(xout.at[ts], xbuf.at[ts], send, recv.at[t], device_id=(nxt,), device_id_type=MESH).wait_recv()

    def pass_on(t):
        @pl.when(jnp.logical_not(last))
        def _():
            step_out(t).start()

        @pl.when(last & (lax.rem(t, CO) == CO - 1))
        def _():
            for i in range(S):
                final_out(t - CO + 1, i).start()

    lax.fori_loop(0, T // CO, lambda k, _: feed(k), 0)
    bias = b_ref[pl.ds(stage, 1), :]

    wcopy.wait()

    kept = ((gates, gates_hbm), (cprev, cp_hbm), (hprev, hp_hbm), (xbuf, xs_hbm))

    def save(t):
        for i, (src, dst) in enumerate(kept):
            pltpu.make_async_copy(src.at[t], dst.at[t], osem.at[i]).start()

    def two(p, state):
        for u in range(2):
            t = 2 * p + u

            @pl.when(t > 0)
            def _():
                pass_on(t - 1)
                save(t - 1)

            arrived(t)
            ha, hc, ca, cc = state
            xt = rows_of(xbuf[t].astype(F32))
            xlow = xt.astype(BF16)
            hlow = jnp.concatenate([ha, hc], axis=1).astype(BF16)
            hprev[t] = hlow
            cprev[t, :, 0:HB] = ca
            cprev[t, :, HB:H] = cc
            nh, nc = [], []
            for q in range(2):
                zz = []
                for g in range(4):
                    cols = slice(g * H + q * HB, g * H + q * HB + HB)
                    zz.append(dot(xlow, w[0:H, cols]) + dot(hlow, w[H:2 * H, cols]) + bias[:, cols])
                gi, gf, gg, go = jax.nn.sigmoid(zz[0]), jax.nn.sigmoid(zz[1]), jnp.tanh(zz[2]), jax.nn.sigmoid(zz[3])
                cn = gf * (ca, cc)[q] + gi * gg
                nh.append(go * jnp.tanh(cn))
                nc.append(cn)
                for g, val in enumerate((gi, gf, gg, go)):
                    gates[t, :, g * H + q * HB:g * H + q * HB + HB] = val
            xout[t] = groups_of(xt + jnp.concatenate(nh, axis=1)).astype(BF16)
            state = (nh[0], nh[1], nc[0], nc[1])
        return state

    zero = jnp.zeros((Q, HB), F32)
    lax.fori_loop(0, T // 2, two, (zero,) * 4)
    pass_on(jnp.int32(T - 1))
    save(T - 1)
    for i, (src, dst) in enumerate(kept):
        pltpu.make_async_copy(src, dst, osem.at[i]).wait()

    @pl.when(jnp.logical_not(first))
    def _():
        pltpu.make_async_remote_copy(x_hbm, xl_hbm, insem, lastsem, device_id=(base,), device_id_type=MESH).wait_send()

    @pl.when(jnp.logical_not(last))
    def _():
        pltpu.make_async_remote_copy(xout, xbuf, send, recv.at[0], device_id=(nxt,), device_id_type=MESH).wait_send()

    @pl.when(last)
    def _():
        others = (slice(None), slice(0, S - 1))
        pltpu.make_async_remote_copy(xout.at[others], xbuf.at[others], send, recv.at[0], device_id=(nxt,), device_id_type=MESH).wait_send()

    pltpu.make_async_copy(x_hbm, xl_hbm, lastsem).wait()


def forward(x, w, b):
    return pl.pallas_call(
        fwd_kernel,
        out_shape=(jax.ShapeDtypeStruct((T, Q, G4), F32), jax.ShapeDtypeStruct((T, Q, H), F32),
                   jax.ShapeDtypeStruct((T, Q, H), BF16), jax.ShapeDtypeStruct((T, S, R, H), BF16),
                   jax.ShapeDtypeStruct((T, R, H), BF16)),
        in_specs=[ANY, ANY, VMEM],
        out_specs=(HBM,) * 5,
        scratch_shapes=[pltpu.VMEM((2 * H, G4), BF16), pltpu.VMEM((T, S, R, H), BF16), pltpu.VMEM((T, S, R, H), BF16),
                        pltpu.VMEM((T, Q, G4), F32), pltpu.VMEM((T, Q, H), F32), pltpu.VMEM((T, Q, H), BF16)]
        + [DMA((1,)), DMA, DMA((T,)), DMA, DMA, DMA((4,))],
        compiler_params=pltpu.CompilerParams(vmem_limit_bytes=52 * MIB, collective_id=0, has_side_effects=True),
        cost_estimate=pl.CostEstimate(flops=60_000_000_000, bytes_accessed=80_000_000, transcendentals=0),
        name="lstm_fwd",
    )(x, w, b)


def bwd_kernel(d_hbm, gates_hbm, cp_hbm, hp_hbm, xs_hbm, w_hbm, both, own1, own2, give1, give2, db_ref, dx_hbm,
               w, wt, dbuf, dout, dall, ut, acc, gin, cin, hin, xin,
               wsem, insem, recv, send, lastsem, isem, osem):
    base, index, stage = place()
    plane = base // S
    first, last = stage == 0, stage == S - 1
    prv = base + gray(lax.rem(stage + S - 1, S))
    top = base + LAST
    plane_signal(base, index)
    wcopy = pltpu.make_async_copy(w_hbm.at[stage], w, wsem.at[0])
    wcopy.start()

    def feed(k):
        t = T - CO - k * CO
        ts = pl.ds(t, CO)

        @pl.when(last)
        def _():
            pltpu.make_async_copy(d_hbm.at[ts], dbuf.at[ts, LAST], recv.at[t]).start()

        @pl.when(jnp.logical_not(last))
        def _():
            pltpu.make_async_remote_copy(d_hbm.at[ts], dbuf.at[ts, index], insem, recv.at[t],
                                         device_id=(top,), device_id_type=MESH).start()

        return 0

    def step_out(t):
        return pltpu.make_async_remote_copy(dout.at[t], dbuf.at[t], send, recv.at[t], device_id=(prv,), device_id_type=MESH)

    def final_out(t, i):
        ts = pl.ds(t, CO)
        if i == 0:
            return pltpu.make_async_copy(dout.at[ts, i], dx_hbm.at[ts], lastsem)
        return pltpu.make_async_remote_copy(dout.at[ts, i], dx_hbm.at[ts], send, lastsem, device_id=(base + i,), device_id_type=MESH)

    def arrived(t):
        @pl.when(jnp.logical_not(last))
        def _():
            step_out(t).wait_recv()

        @pl.when(last & (lax.rem(t, CO) == CO - 1))
        def _():
            ts = pl.ds(t - CO + 1, CO)
            pltpu.make_async_remote_copy(dout.at[ts], dbuf.at[ts], send, recv.at[t - CO + 1], device_id=(prv,), device_id_type=MESH).wait_recv()

    def pass_on(t):
        @pl.when(jnp.logical_not(first))
        def _():
            step_out(t).start()

        @pl.when(first & (lax.rem(t, CO) == 0))
        def _():
            for i in range(S):
                final_out(t, i).start()

    def loads(t):
        k = lax.rem(t, NR)
        return [pltpu.make_async_copy(src.at[t], dst.at[k], isem.at[k, i])
                for i, (src, dst) in enumerate(((gates_hbm, gin), (cp_hbm, cin), (hp_hbm, hin), (xs_hbm, xin)))]

    for t in range(T - NR, T):
        for cp in loads(t):
            cp.start()
    plane_wait()
    lax.fori_loop(0, T // CO, lambda k, _: feed(k), 0)
    db_ref[...] = jnp.zeros(db_ref.shape, F32)
    acc[...] = jnp.zeros(acc.shape, F32)
    wcopy.wait()

    def turn(n, _):
        cols = pl.ds(pl.multiple_of(n * HB, HB), HB)
        wt[cols, :] = w[:, cols].T
        return 0

    lax.fori_loop(0, G4 // HB, turn, 0)

    def weight(buf, part):
        for n in range(0, G4 // CH, HB):
            cols = pl.ds(pl.multiple_of(part * (G4 // CH) + n, HB), HB)
            acc[:, cols] += dot(ut[buf], dall[buf, :, cols])

    def two(n, state):
        p = T // 2 - 1 - n
        us = []
        for u in (1, 0):
            t = 2 * p + u
            k = lax.rem(t, NR)
            for cp in loads(t):
                cp.wait()

            @pl.when(t < T - 1)
            def _():
                pass_on(t + 1)

            buf = lax.rem(t // CH, 2)

            @pl.when(t < T - CH)
            def _():
                weight(1 - buf, lax.rem(t, CH))

            arrived(t)
            ea, ec, da, dc_ = state
            dext = rows_of(dbuf[t])
            parts = [[None, None] for _ in range(4)]
            nd = []
            for q in range(2):
                gi, gf, gg, go = (gin[k, :, g * H + q * HB:g * H + q * HB + HB] for g in range(4))
                hq = slice(q * HB, q * HB + HB)
                cprev = cin[k, :, hq]
                th = jnp.tanh(gf * cprev + gi * gg)
                e = dext[:, hq] + (ea, ec)[q]
                dc = (da, dc_)[q] + e * (go * (1.0 - th * th))
                parts[0][q] = dc * (gg * gi * (1.0 - gi))
                parts[1][q] = dc * (cprev * gf * (1.0 - gf))
                parts[2][q] = dc * (gi * (1.0 - gg * gg))
                parts[3][q] = e * (th * go * (1.0 - go))
                nd.append(dc * gf)
            trows = pl.ds(pl.multiple_of(lax.rem(t, CH) * Q, Q), Q)
            lows = []
            for i, v in enumerate(v for ps in parts for v in ps):
                cols = slice(i * HB, i * HB + HB)
                low = v.astype(BF16)
                dall[buf, trows, cols] = low
                lows.append(low)
                db_ref[:, cols] += jnp.sum(v.reshape(Q // R, R, HB), axis=0)
            lowz = jnp.concatenate(lows, axis=1)
            ne = [dot(lowz, wt[:, H + q * HB:H + q * HB + HB]) for q in range(2)]
            for q in range(2):
                hq = slice(q * HB, q * HB + HB)
                dout[t, :, :, hq] = groups_of(dext[:, hq] + dot(lowz, wt[:, hq]))
            state = (ne[0], ne[1], nd[0], nd[1])
            us.append((rows_of(xin[k].astype(F32)), hin[k].astype(F32)))

            @pl.when(t >= NR)
            def _():
                for cp in loads(t - NR):
                    cp.start()

        tcols = pl.ds(pl.multiple_of(lax.rem(p, CH // 2) * 2 * Q, 2 * Q), 2 * Q)
        for j in range(2):
            ut[buf, j * H:j * H + H, tcols] = jnp.concatenate([us[1][j], us[0][j]], axis=0).T.astype(BF16)

        return state

    zero = jnp.zeros((Q, HB), F32)
    lax.fori_loop(0, T // 2, two, (zero,) * 4)
    pass_on(jnp.int32(0))

    lax.fori_loop(0, CH, lambda k, _: (weight(0, k), 0)[1], 0)
    outs = []
    for i, (dst, (row, step, rows), at) in enumerate(((both, PIECES[0], 0), (give1, PIECES[1], 1 - plane), (give2, PIECES[2], 1 - plane),
                                                      (own1, PIECES[1], plane), (own2, PIECES[2], plane))):
        outs.append(pltpu.make_async_copy(acc.at[pl.ds(pl.multiple_of(row + at * step, R), rows)], dst, osem.at[i]))
        outs[i].start()
    for out in outs:
        out.wait()

    @pl.when(jnp.logical_not(last))
    def _():
        pltpu.make_async_remote_copy(d_hbm, dx_hbm, insem, lastsem, device_id=(top,), device_id_type=MESH).wait_send()

    @pl.when(jnp.logical_not(first))
    def _():
        pltpu.make_async_remote_copy(dout, dbuf, send, recv.at[0], device_id=(prv,), device_id_type=MESH).wait_send()

    @pl.when(first)
    def _():
        others = (slice(None), slice(1, S))
        pltpu.make_async_remote_copy(dout.at[others], dbuf.at[others], send, recv.at[0], device_id=(prv,), device_id_type=MESH).wait_send()

    pltpu.make_async_copy(d_hbm, dx_hbm, lastsem).wait()


def backward(d_top, gates, cprev, hprev, xs, w):
    return pl.pallas_call(
        bwd_kernel,
        out_shape=tuple(jax.ShapeDtypeStruct((rows, G4), F32) for _, _, rows in PIECES + PIECES[1:]) + (jax.ShapeDtypeStruct((R, G4), F32), jax.ShapeDtypeStruct((T, R, H), F32)),
        in_specs=[ANY] * 6,
        out_specs=(HBM,) * 5 + (VMEM, HBM),
        scratch_shapes=[pltpu.VMEM((2 * H, G4), BF16), pltpu.VMEM((G4, 2 * H), BF16), pltpu.VMEM((T, S, R, H), F32),
                        pltpu.VMEM((T, S, R, H), F32), pltpu.VMEM((2, CH * Q, G4), BF16), pltpu.VMEM((2, 2 * H, CH * Q), BF16), pltpu.VMEM((2 * H, G4), F32)]
        + [pltpu.VMEM((NR, Q, G4), F32), pltpu.VMEM((NR, Q, H), F32), pltpu.VMEM((NR, Q, H), BF16), pltpu.VMEM((NR, S, R, H), BF16)]
        + [DMA((1,)), DMA, DMA((T,)), DMA, DMA, DMA((NR, 4)), DMA((5,))],
        compiler_params=pltpu.CompilerParams(vmem_limit_bytes=56 * MIB, collective_id=1, has_side_effects=True),
        cost_estimate=pl.CostEstimate(flops=110_000_000_000, bytes_accessed=80_000_000, transcendentals=0),
        name="lstm_bwd",
    )(d_top, gates, cprev, hprev, xs, w)


VB = 1280
NVB = V // VB
N = T * R
CHUNKS = ((0, 512), (512, 512), (1024, 256))
NW = 4
RB = 64


def head_kernel(x_ref, t_ref, w_hbm, dx_ref, stats_ref, lg, g0, g1, wv, mx, sm, tb, wsem):
    def wcopy(b):
        buf = lax.rem(b, NW)
        return pltpu.make_async_copy(w_hbm.at[:, pl.ds(pl.multiple_of(lax.rem(b, NVB) * VB, VB), VB)], wv.at[buf], wsem.at[buf])

    for b in range(NW - 1):
        wcopy(b).start()

    def ready(b):
        for i in range(2):
            wcopy(b + i).wait()
            wcopy(b + i + 2).start()

    mx[...] = jnp.full(mx.shape, -jnp.inf, F32)
    sm[...] = jnp.zeros(sm.shape, F32)
    dx_ref[...] = jnp.zeros(dx_ref.shape, F32)

    def logits(b, c, size):
        part = dot(x_ref[...], wv[lax.rem(b, NW), :, c:c + size])
        lg[b, :, c:c + size] = part
        for r in range(0, N, RB):
            rows = slice(r, r + RB)
            vals = [part[rows, h:h + LANE] for h in range(0, size, LANE)]
            m_old = mx[rows, :]
            m_new = functools.reduce(jnp.maximum, vals, m_old)
            mx[rows, :] = m_new
            sm[rows, :] = functools.reduce(jnp.add, [jnp.exp(v - m_new) for v in vals], sm[rows, :] * jnp.exp(m_old - m_new))

    def block(b):
        for c, size in CHUNKS:
            logits(b, c, size)

    wcopy(0).wait()
    block(0)

    def first(h, _):
        b = 2 * h + 1
        ready(b)
        for i in range(2):
            block(b + i)
        return 0

    lax.fori_loop(0, NVB // 2, first, 0)

    def finish(r):
        rows = slice(r, r + LANE)
        top = jnp.max(mx[rows, :], axis=1, keepdims=True)
        tot = jnp.sum(sm[rows, :] * jnp.exp(mx[rows, :] - top), axis=1, keepdims=True)
        lse = top + jnp.log(tot)
        mx[rows, :] = jnp.broadcast_to(lse, (LANE, LANE))
        tb[rows, :] = jnp.broadcast_to(t_ref[rows, :], (LANE, LANE))
        lane = lax.broadcasted_iota(jnp.int32, (LANE, LANE), 1)
        stats_ref[rows, :] = jnp.where(lane < LANE // 2, mx[rows, :], tb[rows, :].astype(F32))

    for r in range(0, N, LANE):
        finish(r)

    def grads(b, gb, c):
        ids = [b * VB + c + h + lax.broadcasted_iota(jnp.int32, (RB, LANE), 1) for h in (0, LANE)]
        for r in range(0, N, RB):
            rows = slice(r, r + RB)
            lse = mx[rows, :]
            for h in (0, LANE):
                cols = pl.ds(c + h, LANE)
                p = jnp.exp(lg[b, rows, cols] - lse)
                gb[rows, cols] = jnp.where(tb[rows, :] == ids[h // LANE], p - 1.0, p).astype(BF16)

    def apply(b, gb, cols):
        return dot_tt(gb[:, cols], wv[lax.rem(b + NVB, NW), :, cols])

    for c in range(0, VB, HB):
        grads(0, g0, c)

    def second(h, _):
        for i in range(2):
            b = 2 * h + NVB + i
            wcopy(b).wait()

            @pl.when(b + 2 < 2 * NVB)
            def _():
                wcopy(b + 2).start()

        for b, gb, gn in ((2 * h, g0, g1), (2 * h + 1, g1, g0)):
            total = jnp.zeros((N, H), F32)
            for c in range(0, VB, HB):
                total = total + apply(b, gb, slice(c, c + HB))
                grads(b + 1, gn, c)
            dx_ref[...] += total
        return 0

    lax.fori_loop(0, NVB // 2, second, 0)
    wcopy(2 * NVB - 1).wait()
    for c in range(0, VB, HB):
        dx_ref[...] += apply(NVB - 1, g0, slice(c, c + HB))


def head(x, tgt, w_vocab):
    return pl.pallas_call(
        head_kernel,
        out_shape=(jax.ShapeDtypeStruct((N, H), F32), jax.ShapeDtypeStruct((N, LANE), F32)),
        in_specs=[VMEM, VMEM, ANY],
        out_specs=(VMEM, VMEM),
        scratch_shapes=[pltpu.VMEM((NVB, N, VB), F32), pltpu.VMEM((N, VB), BF16), pltpu.VMEM((N, VB), BF16), pltpu.VMEM((NW, H, VB), BF16),
                        pltpu.VMEM((N, LANE), F32), pltpu.VMEM((N, LANE), F32), pltpu.VMEM((N, LANE), jnp.int32), DMA((NW,))],
        compiler_params=pltpu.CompilerParams(vmem_limit_bytes=60 * MIB),
        cost_estimate=pl.CostEstimate(flops=40_000_000_000, bytes_accessed=70_000_000, transcendentals=0),
        name="head",
    )(x, tgt, w_vocab)


TB = 768
NTOK = NDEV * N
NK = NTOK // TB
UN = 2
NOWN = (NVB + 1) // 2


def block_of(j, side):
    return j + side * (NVB - 1 - 2 * j)


def dwv_kernel(lo, hi, came, x_hbm, st_ref, w_hbm, *rest):
    nshared = min(hi, NOWN - 1) - lo
    arrived = rest[len(rest) - 15 - 1 - (nshared > 0) - len(came):]
    dw_hbm = arrived[len(came)]
    give_hbm = arrived[len(came) + 1]
    xv, xtv, wv, g0, g1, acc, lse, tgt, box, wsem, xsem, osem, gsem, isem, psem = rest[-15:]
    core = lax.rem(lax.axis_index("data"), 2)

    def cols(b):
        return pl.ds(pl.multiple_of(b * VB, VB), VB)

    def wcopy(i):
        buf = lax.rem(i, 2)
        return pltpu.make_async_copy(w_hbm.at[:, cols(block_of(lo + i, core))], wv.at[buf], wsem.at[buf])

    def keep(i):
        buf = lax.rem(i, 2)
        return pltpu.make_async_copy(acc.at[buf], dw_hbm.at[:, cols(block_of(lo + i, core))], osem.at[buf])

    def give(i):
        buf = lax.rem(i, 2)
        return pltpu.make_async_copy(acc.at[buf], give_hbm.at[i], gsem.at[buf])

    def done(i):
        keep(i).start()

        @pl.when(i < nshared)
        def _():
            give(i).start()

    def drained(i):
        keep(i).wait()

        @pl.when(i < nshared)
        def _():
            give(i).wait()

    pieces = [(src, first, i, r) for src, (first, count) in zip(arrived, came) for i in range(count) for r in range(0, H, LANE)]
    per = -(-len(pieces) // ((hi - lo) * NK // UN))

    def fetch(src, i, r, k, slot):
        return pltpu.make_async_copy(src.at[i, pl.ds(r, LANE)], box.at[k, slot], isem.at[k, slot])

    def put(first, i, r, k, slot):
        return pltpu.make_async_copy(box.at[k, slot], dw_hbm.at[pl.ds(r, LANE), cols(block_of(first + i, 1 - core))], psem.at[k, slot])

    def pieces_of(h, act):
        at = 0
        for src, (first, count) in zip(arrived, came):
            total = count * H // LANE
            for slot in range(per):
                c = h * per + slot - at
                i, r = c // (H // LANE), pl.multiple_of(lax.rem(c, H // LANE) * LANE, LANE)

                @pl.when((c >= 0) & (c < total))
                def _():
                    act(src, first, i, r, lax.rem(h, 2), slot)

            at += total

    def land(src, first, i, r, k, slot):
        fetch(src, i, r, k, slot).wait()
        put(first, i, r, k, slot).start()

    def move(h):
        if came:
            pieces_of(h, land)
            pieces_of(h - 1 + 2 * (h == 0) * len(pieces), lambda src, first, i, r, k, slot: put(first, i, r, k, slot).wait())
            pieces_of(h + 1, lambda src, first, i, r, k, slot: fetch(src, i, r, k, slot).start())

    n = hi - lo
    wcopy(0).start()

    def xcopy(k):
        rows = pl.ds(k * TB, TB)
        return pltpu.make_async_copy(x_hbm.at[rows], xv.at[rows], xsem.at[k])

    for k in range(NK):
        xcopy(k).start()

    def turn(k, _):
        xcopy(k).wait()
        for c in range(0, TB, HB):
            rows = pl.ds(pl.multiple_of(k * TB + c, HB), HB)
            xtv[k, :, c:c + HB] = xv[rows, :].T
            lse[rows, :] = jnp.broadcast_to(st_ref[rows, 0:1], (HB, LANE))
            tgt[rows, :] = jnp.broadcast_to(st_ref[rows, LANE - 1:LANE], (HB, LANE))
        return 0

    lax.fori_loop(0, NK, turn, 0)
    if came:
        pieces_of(jnp.int32(0), lambda src, first, i, r, k, slot: fetch(src, i, r, k, slot).start())

    def weight(it, gold, cols, reset=False):
        k, i = lax.rem(it + NK, NK), jnp.maximum(it, 0) // NK
        acc_c = acc.at[lax.rem(i, 2), :, cols]
        old = acc_c[...]
        acc_c[...] = (jnp.where(k == 0, 0.0, old) if reset else old) + dot(xtv[k], gold[:, cols])

    def step(it, u):
        gnew, gold = ((g0, g1), (g1, g0))[u % 2]
        k, i = lax.rem(it, NK) + u, it // NK
        base = pl.multiple_of(k * TB, TB)
        lane = lax.broadcasted_iota(jnp.int32, (R, LANE), 1) + block_of(lo + i, core) * VB
        for c in range(0, VB, HB):
            lgt = dot(xv[pl.ds(base, TB), :], wv[lax.rem(i, 2), :, c:c + HB])
            weight(it + u - 1, gold, slice(c, c + HB), u == 1)
            ids = [jnp.tile((lane + (c + h)).astype(F32), (RB // R, 1)) for h in (0, LANE)]
            for r in range(0, TB, RB):
                here = pl.ds(pl.multiple_of(base + r, RB), RB)
                for h in (0, LANE):
                    p = jnp.exp(lgt[r:r + RB, h:h + LANE] - lse[here, :])
                    gnew[r:r + RB, c + h:c + h + LANE] = jnp.where(tgt[here, :] == ids[h // LANE], p - 1.0, p).astype(BF16)

    def body(h, _):
        it = UN * h
        i0, k0 = it // NK, lax.rem(it, NK)
        move(h)

        @pl.when(k0 == 0)
        def _():
            wcopy(i0).wait()

            @pl.when(i0 < n - 1)
            def _():
                wcopy(i0 + 1).start()

        @pl.when((k0 == 0) & (i0 >= 2))
        def _():
            drained(i0 - 2)

        for u in range(UN):
            step(it, u)

        @pl.when((k0 == UN) & (i0 >= 1))
        def _():
            done(i0 - 1)

        return 0

    lax.fori_loop(0, n * NK // UN, body, 0)

    def last(c, _):
        weight(jnp.int32(n * NK - 1), g1, pl.ds(pl.multiple_of(c * HB, HB), HB))
        return 0

    lax.fori_loop(0, VB // HB, last, 0)
    if n > 1:
        drained(n - 2)
    done(n - 1)
    if came:
        pieces_of(jnp.int32(n * NK // UN - 1), lambda src, first, i, r, k, slot: put(first, i, r, k, slot).wait())
    drained(n - 1)


def grad_vocab(lo, hi, x_all, stats, w_vocab, before=(), came=()):
    counts = tuple((first, v.shape[0]) for first, v in came)
    nshared = min(hi, NOWN - 1) - lo
    out = (jax.ShapeDtypeStruct((H, V), F32), jax.ShapeDtypeStruct((nshared, H, VB), F32))[:1 + (nshared > 0)]
    per = max(1, -(-sum(c for _, c in counts) * (H // LANE) // ((hi - lo) * NK // UN)))
    return pl.pallas_call(
        functools.partial(dwv_kernel, lo, hi, counts),
        out_shape=out,
        in_specs=[ANY, VMEM, ANY] + [HBM] * (len(before) + len(came)),
        out_specs=(HBM,) * len(out),
        input_output_aliases={3: 0} if before else {},
        scratch_shapes=[pltpu.VMEM((NTOK, H), BF16), pltpu.VMEM((NK, H, TB), BF16), pltpu.VMEM((2, H, VB), BF16)]
        + [pltpu.VMEM((TB, VB), BF16)] * 2
        + [pltpu.VMEM((2, H, VB), F32)] + [pltpu.VMEM((NTOK, LANE), F32)] * 2 + [pltpu.VMEM((2, per, LANE, VB), F32)]
        + [DMA((2,)), DMA((NK,)), DMA((2,)), DMA((2,)), DMA((2, per)), DMA((2, per))],
        compiler_params=pltpu.CompilerParams(vmem_limit_bytes=62 * MIB),
        cost_estimate=pl.CostEstimate(flops=(hi - lo) * 20_000_000_000, bytes_accessed=100_000_000, transcendentals=0),
        name="dwv",
    )(x_all, stats, w_vocab, *before, *(v for _, v in came))


NC = 8


def copy_ring(n, src, dst, buf, isem, osem):
    def fetch(i):
        k = lax.rem(i, NC)
        return pltpu.make_async_copy(src(i), buf.at[k], isem.at[k])

    def put(i):
        k = lax.rem(i, NC)
        return pltpu.make_async_copy(buf.at[k], dst(i), osem.at[k])

    for i in range(NC // 2):
        fetch(i).start()

    def body(i, _):
        fetch(i).wait()
        put(i).start()

        @pl.when(i >= NC // 2)
        def _():
            put(i - NC // 2).wait()

        @pl.when(i + NC // 2 < n)
        def _():
            fetch(i + NC // 2).start()

        return 0

    lax.fori_loop(0, n, body, 0)
    for i in range(n - NC // 2, n):
        put(i).wait()


def copy_call(kernel, out, block, args):
    return pl.pallas_call(
        kernel,
        out_shape=jax.ShapeDtypeStruct(out, F32),
        in_specs=[HBM] * len(args),
        out_specs=HBM,
        input_output_aliases={1: 0} if len(args) > 1 else {},
        scratch_shapes=[pltpu.VMEM((NC,) + block, F32), DMA((NC,)), DMA((NC,))],
        compiler_params=pltpu.CompilerParams(vmem_limit_bytes=24 * MIB),
        cost_estimate=pl.CostEstimate(flops=20_000_000_000, bytes_accessed=130_000_000, transcendentals=0),
    )(*args)


def land_blocks(first, sent, dwv):
    per = H // LANE

    def kernel(src, _, dst, *scratch):
        other = 1 - lax.rem(lax.axis_index("data"), 2)

        def rows(i):
            return pl.ds(pl.multiple_of(lax.rem(i, per) * LANE, LANE), LANE)

        def target(i):
            return dst.at[rows(i), pl.ds(pl.multiple_of(block_of(first + i // per, other) * VB, VB), VB)]

        copy_ring(sent.shape[0] * per, lambda i: src.at[i // per, rows(i)], target, *scratch)

    return copy_call(kernel, (H, V), (LANE, VB), (sent, dwv))


def place_dw(piece, parts, *before):
    row, step, rows = PIECES[piece]

    def kernel(src, *rest):
        dst, scratch = rest[-4], rest[-3:]

        def target(i):
            return dst.at[gray(lax.rem(i, S)), pl.ds(pl.multiple_of(row + i // S * step, R), rows)]

        copy_ring(parts.shape[0], lambda i: src.at[i, 0:rows], target, *scratch)

    return copy_call(kernel, (L, 2 * H, G4), (rows, G4), (parts,) + before)


SPLITS = (0, 2, 6, NOWN)


def solution(mesh):
    def local_grads(x_rows, tgt_rows, w_lstm, b_lstm, w_vocab):
        tgt = jnp.swapaxes(tgt_rows, 0, 1).reshape(N, 1)
        gates, cprev, hprev, xs, top = forward(jnp.swapaxes(x_rows, 0, 1), w_lstm, b_lstm)
        top = top.reshape(N, H)
        d_top, stats = head(top, tgt, w_vocab)
        x_all = lax.all_gather(top, 'data', axis=0, tiled=True)
        stats = lax.all_gather(stats, 'data', axis=0, tiled=True)
        d_top, x_all = lax.optimization_barrier((d_top, x_all))
        both, *owns, give1, give2, db, dx = backward(d_top.reshape(T, R, H), gates, cprev, hprev, xs, w_lstm)
        other_plane = [(i, (i + S) % NDEV) for i in range(NDEV)]
        other_core = [(i, i + 1 - 2 * (i % 2)) for i in range(NDEV)]
        planes = [list(range(S)), list(range(S, NDEV))]
        dwv, part, gathered, swapped = (), both, [], []
        for i, (own, give) in enumerate(((both, both), (owns[0], give1), (owns[1], give2))):
            if i:
                give, part = lax.optimization_barrier((give, part))
            got = lax.ppermute(give, 'data', other_plane)
            dwv, sent = grad_vocab(SPLITS[i], SPLITS[i + 1], x_all, stats, w_vocab, dwv, swapped[:1] if i == 2 else ())
            own, dwv = lax.optimization_barrier((own, dwv))
            part = own + got if i != 1 else jnp.concatenate([own + got, db], axis=0)
            part, dwv = lax.optimization_barrier((part, dwv))
            gathered.append(lax.all_gather(part, 'data', axis=0, axis_index_groups=None if i else planes))
            swapped.append((SPLITS[i], lax.ppermute(sent, 'data', other_core)))
            dwv = (dwv,)
        dw = place_dw(0, gathered[0])
        for first, sent in swapped[1:]:
            dwv = (land_blocks(first, sent, *dwv),)
        dw = place_dw(2, gathered[2], place_dw(1, gathered[1], dw))
        db = gathered[1][:, PIECES[1][2]:].reshape(NDEV // S, S, R, G4).sum(axis=(0, 2))
        db = jnp.stack([db[gray(i)] for i in range(L)])
        return dw, db, dwv[0], jnp.swapaxes(dx, 0, 1)

    return jax.shard_map(local_grads, mesh=mesh, in_specs=(P('data'), P('data'), P(), P(), P()), out_specs=(P(), P(), P(), P('data')), check_vma=False)
```

```python
import functools

import jax
import jax.numpy as jnp
from jax import lax
from jax.experimental import pallas as pl
from jax.experimental.pallas import tpu as pltpu
from jax.sharding import PartitionSpec as P

T = 48
R = 8
S = 8
Q = S * R
H = 512
HB = 256
G4 = 4 * H
L = 8
V = 32000
LANE = 128
NDEV = 16
CH = 4
NR = 6
PIECES = ((0, 0, 256), (256, 384, 352), (608, 384, 32))
F32 = jnp.float32
BF16 = jnp.bfloat16
MESH = pl.DeviceIdType.MESH
MIB = 1024 * 1024
ANY = pl.BlockSpec(memory_space=pl.ANY)
VMEM = pl.BlockSpec(memory_space=pltpu.VMEM)
HBM = pl.BlockSpec(memory_space=pltpu.HBM)
DMA = pltpu.SemaphoreType.DMA


def dot(a, b):
    return jnp.dot(a, b, preferred_element_type=F32)


def dot_tt(a, b):
    return lax.dot_general(a, b, (((1,), (1,)), ((), ())), preferred_element_type=F32)


def gray(k):
    chip, core = k // 2, k % 2
    hi, lo = chip // 2, chip % 2
    return 2 * (chip + hi - 2 * hi * lo) + core


LAST = gray(S - 1)


def place():
    me = lax.axis_index("data")
    index = lax.rem(me, S)
    return me - index, index, gray(index)


def plane_signal(base, index):
    barrier = pltpu.get_barrier_semaphore()
    for i in range(1, S):
        pl.semaphore_signal(barrier, inc=1, device_id=(base + lax.rem(index + i, S),), device_id_type=MESH)


def plane_wait():
    pl.semaphore_wait(pltpu.get_barrier_semaphore(), S - 1)


def rows_of(v):
    return v.reshape(Q, v.shape[-1])


def groups_of(v):
    return v.reshape(S, R, v.shape[-1])


def fwd_kernel(x_hbm, w_hbm, b_ref, gates_hbm, cp_hbm, hp_hbm, xs_hbm, xl_hbm,
               w, xbuf, xout, gates, cprev, hprev, wsem, insem, recv, send, lastsem, osem):
    base, index, stage = place()
    first, last = stage == 0, stage == S - 1
    nxt = base + gray(lax.rem(stage + 1, S))
    plane_signal(base, index)
    wcopy = pltpu.make_async_copy(w_hbm.at[stage], w, wsem.at[0])
    wcopy.start()
    plane_wait()

    def feed(k):
        ts = pl.ds(k * CH, CH)

        @pl.when(first)
        def _():
            pltpu.make_async_copy(x_hbm.at[ts], xbuf.at[ts, 0], recv.at[k * CH]).start()

        @pl.when(jnp.logical_not(first))
        def _():
            pltpu.make_async_remote_copy(x_hbm.at[ts], xbuf.at[ts, index], insem, recv.at[k * CH],
                                         device_id=(base,), device_id_type=MESH).start()

        return 0

    def step_out(t):
        return pltpu.make_async_remote_copy(xout.at[t], xbuf.at[t], send, recv.at[t], device_id=(nxt,), device_id_type=MESH)

    def final_out(t, i):
        ts = pl.ds(t, CH)
        if i == LAST:
            return pltpu.make_async_copy(xout.at[ts, i], xl_hbm.at[ts], lastsem)
        return pltpu.make_async_remote_copy(xout.at[ts, i], xl_hbm.at[ts], send, lastsem, device_id=(base + i,), device_id_type=MESH)

    def arrived(t):
        @pl.when(jnp.logical_not(first))
        def _():
            step_out(t).wait_recv()

        @pl.when(first & (lax.rem(t, CH) == 0))
        def _():
            ts = pl.ds(t, CH)
            pltpu.make_async_remote_copy(xout.at[ts], xbuf.at[ts], send, recv.at[t], device_id=(nxt,), device_id_type=MESH).wait_recv()

    def pass_on(t):
        @pl.when(jnp.logical_not(last))
        def _():
            step_out(t).start()

        @pl.when(last & (lax.rem(t, CH) == CH - 1))
        def _():
            for i in range(S):
                final_out(t - CH + 1, i).start()

    lax.fori_loop(0, T // CH, lambda k, _: feed(k), 0)
    bias = b_ref[pl.ds(stage, 1), :]

    wcopy.wait()

    kept = ((gates, gates_hbm), (cprev, cp_hbm), (hprev, hp_hbm), (xbuf, xs_hbm))

    def save(t):
        for i, (src, dst) in enumerate(kept):
            pltpu.make_async_copy(src.at[t], dst.at[t], osem.at[i]).start()

    def two(p, state):
        for u in range(2):
            t = 2 * p + u

            @pl.when(t > 0)
            def _():
                pass_on(t - 1)
                save(t - 1)

            arrived(t)
            ha, hc, ca, cc = state
            xt = rows_of(xbuf[t].astype(F32))
            xlow = xt.astype(BF16)
            hlow = jnp.concatenate([ha, hc], axis=1).astype(BF16)
            hprev[t] = hlow
            cprev[t, :, 0:HB] = ca
            cprev[t, :, HB:H] = cc
            nh, nc = [], []
            for q in range(2):
                zz = []
                for g in range(4):
                    cols = slice(g * H + q * HB, g * H + q * HB + HB)
                    zz.append(dot(xlow, w[0:H, cols]) + dot(hlow, w[H:2 * H, cols]) + bias[:, cols])
                gi, gf, gg, go = jax.nn.sigmoid(zz[0]), jax.nn.sigmoid(zz[1]), jnp.tanh(zz[2]), jax.nn.sigmoid(zz[3])
                cn = gf * (ca, cc)[q] + gi * gg
                nh.append(go * jnp.tanh(cn))
                nc.append(cn)
                for g, val in enumerate((gi, gf, gg, go)):
                    gates[t, :, g * H + q * HB:g * H + q * HB + HB] = val
            xout[t] = groups_of(xt + jnp.concatenate(nh, axis=1)).astype(BF16)
            state = (nh[0], nh[1], nc[0], nc[1])
        return state

    zero = jnp.zeros((Q, HB), F32)
    lax.fori_loop(0, T // 2, two, (zero,) * 4)
    pass_on(jnp.int32(T - 1))
    save(T - 1)
    for i, (src, dst) in enumerate(kept):
        pltpu.make_async_copy(src, dst, osem.at[i]).wait()

    @pl.when(jnp.logical_not(first))
    def _():
        pltpu.make_async_remote_copy(x_hbm, xl_hbm, insem, lastsem, device_id=(base,), device_id_type=MESH).wait_send()

    @pl.when(jnp.logical_not(last))
    def _():
        pltpu.make_async_remote_copy(xout, xbuf, send, recv.at[0], device_id=(nxt,), device_id_type=MESH).wait_send()

    @pl.when(last)
    def _():
        others = (slice(None), slice(0, S - 1))
        pltpu.make_async_remote_copy(xout.at[others], xbuf.at[others], send, recv.at[0], device_id=(nxt,), device_id_type=MESH).wait_send()

    pltpu.make_async_copy(x_hbm, xl_hbm, lastsem).wait()


def forward(x, w, b):
    return pl.pallas_call(
        fwd_kernel,
        out_shape=(jax.ShapeDtypeStruct((T, Q, G4), F32), jax.ShapeDtypeStruct((T, Q, H), F32),
                   jax.ShapeDtypeStruct((T, Q, H), BF16), jax.ShapeDtypeStruct((T, S, R, H), BF16),
                   jax.ShapeDtypeStruct((T, R, H), BF16)),
        in_specs=[ANY, ANY, VMEM],
        out_specs=(HBM,) * 5,
        scratch_shapes=[pltpu.VMEM((2 * H, G4), BF16), pltpu.VMEM((T, S, R, H), BF16), pltpu.VMEM((T, S, R, H), BF16),
                        pltpu.VMEM((T, Q, G4), F32), pltpu.VMEM((T, Q, H), F32), pltpu.VMEM((T, Q, H), BF16)]
        + [DMA((1,)), DMA, DMA((T,)), DMA, DMA, DMA((4,))],
        compiler_params=pltpu.CompilerParams(vmem_limit_bytes=52 * MIB, collective_id=0, has_side_effects=True),
        cost_estimate=pl.CostEstimate(flops=60_000_000_000, bytes_accessed=80_000_000, transcendentals=0),
        name="lstm_fwd",
    )(x, w, b)


def bwd_kernel(d_hbm, gates_hbm, cp_hbm, hp_hbm, xs_hbm, w_hbm, both, own1, own2, give1, give2, db_ref, dx_hbm,
               w, wt, dbuf, dout, dall, ut, acc, gin, cin, hin, xin,
               wsem, insem, recv, send, lastsem, isem, osem):
    base, index, stage = place()
    plane = base // S
    first, last = stage == 0, stage == S - 1
    prv = base + gray(lax.rem(stage + S - 1, S))
    top = base + LAST
    plane_signal(base, index)
    wcopy = pltpu.make_async_copy(w_hbm.at[stage], w, wsem.at[0])
    wcopy.start()

    def feed(k):
        t = T - CH - k * CH
        ts = pl.ds(t, CH)

        @pl.when(last)
        def _():
            pltpu.make_async_copy(d_hbm.at[ts], dbuf.at[ts, LAST], recv.at[t]).start()

        @pl.when(jnp.logical_not(last))
        def _():
            pltpu.make_async_remote_copy(d_hbm.at[ts], dbuf.at[ts, index], insem, recv.at[t],
                                         device_id=(top,), device_id_type=MESH).start()

        return 0

    def step_out(t):
        return pltpu.make_async_remote_copy(dout.at[t], dbuf.at[t], send, recv.at[t], device_id=(prv,), device_id_type=MESH)

    def final_out(t, i):
        ts = pl.ds(t, CH)
        if i == 0:
            return pltpu.make_async_copy(dout.at[ts, i], dx_hbm.at[ts], lastsem)
        return pltpu.make_async_remote_copy(dout.at[ts, i], dx_hbm.at[ts], send, lastsem, device_id=(base + i,), device_id_type=MESH)

    def arrived(t):
        @pl.when(jnp.logical_not(last))
        def _():
            step_out(t).wait_recv()

        @pl.when(last & (lax.rem(t, CH) == CH - 1))
        def _():
            ts = pl.ds(t - CH + 1, CH)
            pltpu.make_async_remote_copy(dout.at[ts], dbuf.at[ts], send, recv.at[t - CH + 1], device_id=(prv,), device_id_type=MESH).wait_recv()

    def pass_on(t):
        @pl.when(jnp.logical_not(first))
        def _():
            step_out(t).start()

        @pl.when(first & (lax.rem(t, CH) == 0))
        def _():
            for i in range(S):
                final_out(t, i).start()

    def loads(t):
        k = lax.rem(t, NR)
        return [pltpu.make_async_copy(src.at[t], dst.at[k], isem.at[k, i])
                for i, (src, dst) in enumerate(((gates_hbm, gin), (cp_hbm, cin), (hp_hbm, hin), (xs_hbm, xin)))]

    for t in range(T - NR, T):
        for cp in loads(t):
            cp.start()
    plane_wait()
    lax.fori_loop(0, T // CH, lambda k, _: feed(k), 0)
    db_ref[...] = jnp.zeros(db_ref.shape, F32)
    acc[...] = jnp.zeros(acc.shape, F32)
    wcopy.wait()

    def turn(n, _):
        cols = pl.ds(pl.multiple_of(n * HB, HB), HB)
        wt[cols, :] = w[:, cols].T
        return 0

    lax.fori_loop(0, G4 // HB, turn, 0)

    def weight():
        for n in range(0, G4, HB):
            acc[:, n:n + HB] += dot(ut[...], dall[:, n:n + HB])

    def two(n, state):
        p = T // 2 - 1 - n
        us = []
        for u in (1, 0):
            t = 2 * p + u
            k = lax.rem(t, NR)
            for cp in loads(t):
                cp.wait()

            @pl.when(t < T - 1)
            def _():
                pass_on(t + 1)

            if u == 1:
                @pl.when((p < T // 2 - 1) & (lax.rem(p, CH // 2) == CH // 2 - 1))
                def _():
                    weight()

            arrived(t)
            ea, ec, da, dc_ = state
            dext = rows_of(dbuf[t])
            parts = [[None, None] for _ in range(4)]
            nd = []
            for q in range(2):
                gi, gf, gg, go = (gin[k, :, g * H + q * HB:g * H + q * HB + HB] for g in range(4))
                hq = slice(q * HB, q * HB + HB)
                cprev = cin[k, :, hq]
                th = jnp.tanh(gf * cprev + gi * gg)
                e = dext[:, hq] + (ea, ec)[q]
                dc = (da, dc_)[q] + e * (go * (1.0 - th * th))
                parts[0][q] = dc * (gg * gi * (1.0 - gi))
                parts[1][q] = dc * (cprev * gf * (1.0 - gf))
                parts[2][q] = dc * (gi * (1.0 - gg * gg))
                parts[3][q] = e * (th * go * (1.0 - go))
                nd.append(dc * gf)
            trows = pl.ds(pl.multiple_of(lax.rem(t, CH) * Q, Q), Q)
            lows = []
            for i, v in enumerate(v for ps in parts for v in ps):
                cols = slice(i * HB, i * HB + HB)
                low = v.astype(BF16)
                dall[trows, cols] = low
                lows.append(low)
                db_ref[:, cols] += jnp.sum(v.reshape(Q // R, R, HB), axis=0)
            lowz = jnp.concatenate(lows, axis=1)
            ne = [dot(lowz, wt[:, H + q * HB:H + q * HB + HB]) for q in range(2)]
            for q in range(2):
                hq = slice(q * HB, q * HB + HB)
                dout[t, :, :, hq] = groups_of(dext[:, hq] + dot(lowz, wt[:, hq]))
            state = (ne[0], ne[1], nd[0], nd[1])
            us.append((rows_of(xin[k].astype(F32)).astype(BF16), hin[k]))

            @pl.when(t >= NR)
            def _():
                for cp in loads(t - NR):
                    cp.start()

        tcols = pl.ds(pl.multiple_of(lax.rem(p, CH // 2) * 2 * Q, 2 * Q), 2 * Q)
        for j in range(2):
            ut[j * H:j * H + H, tcols] = jnp.concatenate([us[1][j], us[0][j]], axis=0).T

        return state

    zero = jnp.zeros((Q, HB), F32)
    lax.fori_loop(0, T // 2, two, (zero,) * 4)
    pass_on(jnp.int32(0))

    weight()
    outs = []
    for i, (dst, (row, step, rows), at) in enumerate(((both, PIECES[0], 0), (give1, PIECES[1], 1 - plane), (give2, PIECES[2], 1 - plane),
                                                      (own1, PIECES[1], plane), (own2, PIECES[2], plane))):
        outs.append(pltpu.make_async_copy(acc.at[pl.ds(pl.multiple_of(row + at * step, R), rows)], dst, osem.at[i]))
        outs[i].start()
    for out in outs:
        out.wait()

    @pl.when(jnp.logical_not(last))
    def _():
        pltpu.make_async_remote_copy(d_hbm, dx_hbm, insem, lastsem, device_id=(top,), device_id_type=MESH).wait_send()

    @pl.when(jnp.logical_not(first))
    def _():
        pltpu.make_async_remote_copy(dout, dbuf, send, recv.at[0], device_id=(prv,), device_id_type=MESH).wait_send()

    @pl.when(first)
    def _():
        others = (slice(None), slice(1, S))
        pltpu.make_async_remote_copy(dout.at[others], dbuf.at[others], send, recv.at[0], device_id=(prv,), device_id_type=MESH).wait_send()

    pltpu.make_async_copy(d_hbm, dx_hbm, lastsem).wait()


def backward(d_top, gates, cprev, hprev, xs, w):
    return pl.pallas_call(
        bwd_kernel,
        out_shape=tuple(jax.ShapeDtypeStruct((rows, G4), F32) for _, _, rows in PIECES + PIECES[1:]) + (jax.ShapeDtypeStruct((R, G4), F32), jax.ShapeDtypeStruct((T, R, H), F32)),
        in_specs=[ANY] * 6,
        out_specs=(HBM,) * 5 + (VMEM, HBM),
        scratch_shapes=[pltpu.VMEM((2 * H, G4), BF16), pltpu.VMEM((G4, 2 * H), BF16), pltpu.VMEM((T, S, R, H), F32),
                        pltpu.VMEM((T, S, R, H), F32), pltpu.VMEM((CH * Q, G4), BF16), pltpu.VMEM((2 * H, CH * Q), BF16), pltpu.VMEM((2 * H, G4), F32)]
        + [pltpu.VMEM((NR, Q, G4), F32), pltpu.VMEM((NR, Q, H), F32), pltpu.VMEM((NR, Q, H), BF16), pltpu.VMEM((NR, S, R, H), BF16)]
        + [DMA((1,)), DMA, DMA((T,)), DMA, DMA, DMA((NR, 4)), DMA((5,))],
        compiler_params=pltpu.CompilerParams(vmem_limit_bytes=56 * MIB, collective_id=1, has_side_effects=True),
        cost_estimate=pl.CostEstimate(flops=110_000_000_000, bytes_accessed=80_000_000, transcendentals=0),
        name="lstm_bwd",
    )(d_top, gates, cprev, hprev, xs, w)


VB = 1280
NVB = V // VB
N = T * R
CHUNKS = ((0, 512), (512, 512), (1024, 256))
NW = 4
RB = 64


def head_kernel(x_ref, t_ref, w_hbm, dx_ref, stats_ref, lg, g0, g1, wv, mx, sm, tb, wsem):
    def wcopy(b):
        buf = lax.rem(b, NW)
        return pltpu.make_async_copy(w_hbm.at[:, pl.ds(pl.multiple_of(lax.rem(b, NVB) * VB, VB), VB)], wv.at[buf], wsem.at[buf])

    for b in range(NW - 1):
        wcopy(b).start()

    def ready(b):
        for i in range(2):
            wcopy(b + i).wait()
            wcopy(b + i + 2).start()

    mx[...] = jnp.full(mx.shape, -jnp.inf, F32)
    sm[...] = jnp.zeros(sm.shape, F32)
    dx_ref[...] = jnp.zeros(dx_ref.shape, F32)

    def logits(b, c, size):
        part = dot(x_ref[...], wv[lax.rem(b, NW), :, c:c + size])
        lg[b, :, c:c + size] = part
        for r in range(0, N, RB):
            rows = slice(r, r + RB)
            vals = [part[rows, h:h + LANE] for h in range(0, size, LANE)]
            m_old = mx[rows, :]
            m_new = functools.reduce(jnp.maximum, vals, m_old)
            mx[rows, :] = m_new
            sm[rows, :] = functools.reduce(jnp.add, [jnp.exp(v - m_new) for v in vals], sm[rows, :] * jnp.exp(m_old - m_new))

    def block(b):
        for c, size in CHUNKS:
            logits(b, c, size)

    wcopy(0).wait()
    block(0)

    def first(h, _):
        b = 2 * h + 1
        ready(b)
        for i in range(2):
            block(b + i)
        return 0

    lax.fori_loop(0, NVB // 2, first, 0)

    def finish(r):
        rows = slice(r, r + LANE)
        top = jnp.max(mx[rows, :], axis=1, keepdims=True)
        tot = jnp.sum(sm[rows, :] * jnp.exp(mx[rows, :] - top), axis=1, keepdims=True)
        lse = top + jnp.log(tot)
        mx[rows, :] = jnp.broadcast_to(lse, (LANE, LANE))
        tb[rows, :] = jnp.broadcast_to(t_ref[rows, :], (LANE, LANE))

    lane = lax.broadcasted_iota(jnp.int32, (LANE, LANE), 1)
    stats = jnp.zeros((LANE, LANE), F32)
    for j in range(N // LANE):
        finish(j * LANE)
        rows = slice(j * LANE, j * LANE + LANE)
        stats = jnp.where(lane == j, mx[rows, :], jnp.where(lane == LANE - 1 - j, tb[rows, :].astype(F32), stats))
    stats_ref[...] = stats

    def grads(b, gb, c):
        ids = [b * VB + c + h + lax.broadcasted_iota(jnp.int32, (RB, LANE), 1) for h in (0, LANE)]
        for r in range(0, N, RB):
            rows = slice(r, r + RB)
            lse = mx[rows, :]
            for h in (0, LANE):
                cols = pl.ds(c + h, LANE)
                p = jnp.exp(lg[b, rows, cols] - lse)
                gb[rows, cols] = jnp.where(tb[rows, :] == ids[h // LANE], p - 1.0, p).astype(BF16)

    def apply(b, gb, cols):
        return dot_tt(gb[:, cols], wv[lax.rem(b + NVB, NW), :, cols])

    for c in range(0, VB, HB):
        grads(0, g0, c)

    def second(h, _):
        for i in range(2):
            b = 2 * h + NVB + i
            wcopy(b).wait()

            @pl.when(b + 2 < 2 * NVB)
            def _():
                wcopy(b + 2).start()

        for b, gb, gn in ((2 * h, g0, g1), (2 * h + 1, g1, g0)):
            total = jnp.zeros((N, H), F32)
            for c in range(0, VB, HB):
                total = total + apply(b, gb, slice(c, c + HB))
                grads(b + 1, gn, c)
            dx_ref[...] += total
        return 0

    lax.fori_loop(0, NVB // 2, second, 0)
    wcopy(2 * NVB - 1).wait()
    for c in range(0, VB, HB):
        dx_ref[...] += apply(NVB - 1, g0, slice(c, c + HB))


def head(x, tgt, w_vocab):
    return pl.pallas_call(
        head_kernel,
        out_shape=(jax.ShapeDtypeStruct((N, H), F32), jax.ShapeDtypeStruct((LANE, LANE), F32)),
        in_specs=[VMEM, VMEM, ANY],
        out_specs=(VMEM, VMEM),
        scratch_shapes=[pltpu.VMEM((NVB, N, VB), F32), pltpu.VMEM((N, VB), BF16), pltpu.VMEM((N, VB), BF16), pltpu.VMEM((NW, H, VB), BF16),
                        pltpu.VMEM((N, LANE), F32), pltpu.VMEM((N, LANE), F32), pltpu.VMEM((N, LANE), jnp.int32), DMA((NW,))],
        compiler_params=pltpu.CompilerParams(vmem_limit_bytes=60 * MIB),
        cost_estimate=pl.CostEstimate(flops=40_000_000_000, bytes_accessed=70_000_000, transcendentals=0),
        name="head",
    )(x, tgt, w_vocab)


TB = 768
NTOK = NDEV * N
NK = NTOK // TB
UN = 2
NOWN = (NVB + 1) // 2


def block_of(j, side):
    return j + side * (NVB - 1 - 2 * j)


def dwv_kernel(lo, hi, came, x_hbm, st_ref, w_hbm, *rest):
    nshared = min(hi, NOWN - 1) - lo
    arrived = rest[len(rest) - 15 - 1 - (nshared > 0) - len(came):]
    dw_hbm = arrived[len(came)]
    give_hbm = arrived[len(came) + 1]
    xv, xtv, wv, g0, g1, acc, lse, tgt, box, wsem, xsem, osem, gsem, isem, psem = rest[-15:]
    core = lax.rem(lax.axis_index("data"), 2)

    def cols(b):
        return pl.ds(pl.multiple_of(b * VB, VB), VB)

    def wcopy(i):
        buf = lax.rem(i, 2)
        return pltpu.make_async_copy(w_hbm.at[:, cols(block_of(lo + i, core))], wv.at[buf], wsem.at[buf])

    def keep(i):
        buf = lax.rem(i, 2)
        return pltpu.make_async_copy(acc.at[buf], dw_hbm.at[:, cols(block_of(lo + i, core))], osem.at[buf])

    def give(i):
        buf = lax.rem(i, 2)
        return pltpu.make_async_copy(acc.at[buf], give_hbm.at[i], gsem.at[buf])

    def done(i):
        keep(i).start()

        @pl.when(i < nshared)
        def _():
            give(i).start()

    def drained(i):
        keep(i).wait()

        @pl.when(i < nshared)
        def _():
            give(i).wait()

    pieces = [(src, first, i, r) for src, (first, count) in zip(arrived, came) for i in range(count) for r in range(0, H, LANE)]
    per = -(-len(pieces) // ((hi - lo) * NK // UN))

    def fetch(src, i, r, k, slot):
        return pltpu.make_async_copy(src.at[i, pl.ds(r, LANE)], box.at[k, slot], isem.at[k, slot])

    def put(first, i, r, k, slot):
        return pltpu.make_async_copy(box.at[k, slot], dw_hbm.at[pl.ds(r, LANE), cols(block_of(first + i, 1 - core))], psem.at[k, slot])

    def pieces_of(h, act):
        at = 0
        for src, (first, count) in zip(arrived, came):
            total = count * H // LANE
            for slot in range(per):
                c = h * per + slot - at
                i, r = c // (H // LANE), pl.multiple_of(lax.rem(c, H // LANE) * LANE, LANE)

                @pl.when((c >= 0) & (c < total))
                def _():
                    act(src, first, i, r, lax.rem(h, 2), slot)

            at += total

    def land(src, first, i, r, k, slot):
        fetch(src, i, r, k, slot).wait()
        put(first, i, r, k, slot).start()

    def move(h):
        if came:
            pieces_of(h, land)
            pieces_of(h - 1 + 2 * (h == 0) * len(pieces), lambda src, first, i, r, k, slot: put(first, i, r, k, slot).wait())
            pieces_of(h + 1, lambda src, first, i, r, k, slot: fetch(src, i, r, k, slot).start())

    n = hi - lo
    wcopy(0).start()

    def xcopy(k):
        rows = pl.ds(k * TB, TB)
        return pltpu.make_async_copy(x_hbm.at[rows], xv.at[rows], xsem.at[k])

    for k in range(NK):
        xcopy(k).start()

    def turn(k, _):
        xcopy(k).wait()
        for c in range(0, TB, HB):
            rows = pl.ds(pl.multiple_of(k * TB + c, HB), HB)
            xtv[k, :, c:c + HB] = xv[rows, :].T
        for c in range(0, TB, LANE):
            j = c % N // LANE
            held = pl.ds(pl.multiple_of((k * (TB // N) + c // N) * LANE, LANE), LANE)
            rows = pl.ds(pl.multiple_of(k * TB + c, LANE), LANE)
            lse[rows, :] = jnp.broadcast_to(st_ref[held, j:j + 1], (LANE, LANE))
            tgt[rows, :] = jnp.broadcast_to(st_ref[held, LANE - 1 - j:LANE - j], (LANE, LANE))
        return 0

    lax.fori_loop(0, NK, turn, 0)
    if came:
        pieces_of(jnp.int32(0), lambda src, first, i, r, k, slot: fetch(src, i, r, k, slot).start())

    def weight(it, gold, cols, reset=False):
        k, i = lax.rem(it + NK, NK), jnp.maximum(it, 0) // NK
        acc_c = acc.at[lax.rem(i, 2), :, cols]
        old = acc_c[...]
        acc_c[...] = (jnp.where(k == 0, 0.0, old) if reset else old) + dot(xtv[k], gold[:, cols])

    def step(it, u):
        gnew, gold = ((g0, g1), (g1, g0))[u % 2]
        k, i = lax.rem(it, NK) + u, it // NK
        base = pl.multiple_of(k * TB, TB)
        lane = lax.broadcasted_iota(jnp.int32, (R, LANE), 1) + block_of(lo + i, core) * VB
        for c in range(0, VB, HB):
            lgt = dot(xv[pl.ds(base, TB), :], wv[lax.rem(i, 2), :, c:c + HB])
            weight(it + u - 1, gold, slice(c, c + HB), u == 1)
            ids = [jnp.tile((lane + (c + h)).astype(F32), (RB // R, 1)) for h in (0, LANE)]
            for r in range(0, TB, RB):
                here = pl.ds(pl.multiple_of(base + r, RB), RB)
                for h in (0, LANE):
                    p = jnp.exp(lgt[r:r + RB, h:h + LANE] - lse[here, :])
                    gnew[r:r + RB, c + h:c + h + LANE] = jnp.where(tgt[here, :] == ids[h // LANE], p - 1.0, p).astype(BF16)

    def body(h, _):
        it = UN * h
        i0, k0 = it // NK, lax.rem(it, NK)
        move(h)

        @pl.when(k0 == 0)
        def _():
            wcopy(i0).wait()

            @pl.when(i0 < n - 1)
            def _():
                wcopy(i0 + 1).start()

        @pl.when((k0 == 0) & (i0 >= 2))
        def _():
            drained(i0 - 2)

        for u in range(UN):
            step(it, u)

        @pl.when((k0 == UN) & (i0 >= 1))
        def _():
            done(i0 - 1)

        return 0

    lax.fori_loop(0, n * NK // UN, body, 0)

    def last(c, _):
        weight(jnp.int32(n * NK - 1), g1, pl.ds(pl.multiple_of(c * HB, HB), HB))
        return 0

    lax.fori_loop(0, VB // HB, last, 0)
    if n > 1:
        drained(n - 2)
    done(n - 1)
    if came:
        pieces_of(jnp.int32(n * NK // UN - 1), lambda src, first, i, r, k, slot: put(first, i, r, k, slot).wait())
    drained(n - 1)


def grad_vocab(lo, hi, x_all, stats, w_vocab, before=(), came=()):
    counts = tuple((first, v.shape[0]) for first, v in came)
    nshared = min(hi, NOWN - 1) - lo
    out = (jax.ShapeDtypeStruct((H, V), F32), jax.ShapeDtypeStruct((nshared, H, VB), F32))[:1 + (nshared > 0)]
    per = max(1, -(-sum(c for _, c in counts) * (H // LANE) // ((hi - lo) * NK // UN)))
    return pl.pallas_call(
        functools.partial(dwv_kernel, lo, hi, counts),
        out_shape=out,
        in_specs=[ANY, VMEM, ANY] + [HBM] * (len(before) + len(came)),
        out_specs=(HBM,) * len(out),
        input_output_aliases={3: 0} if before else {},
        scratch_shapes=[pltpu.VMEM((NTOK, H), BF16), pltpu.VMEM((NK, H, TB), BF16), pltpu.VMEM((2, H, VB), BF16)]
        + [pltpu.VMEM((TB, VB), BF16)] * 2
        + [pltpu.VMEM((2, H, VB), F32)] + [pltpu.VMEM((NTOK, LANE), F32)] * 2 + [pltpu.VMEM((2, per, LANE, VB), F32)]
        + [DMA((2,)), DMA((NK,)), DMA((2,)), DMA((2,)), DMA((2, per)), DMA((2, per))],
        compiler_params=pltpu.CompilerParams(vmem_limit_bytes=62 * MIB),
        cost_estimate=pl.CostEstimate(flops=(hi - lo) * 20_000_000_000, bytes_accessed=100_000_000, transcendentals=0),
        name="dwv",
    )(x_all, stats, w_vocab, *before, *(v for _, v in came))


NC = 8


def copy_ring(n, src, dst, buf, isem, osem):
    def fetch(i):
        k = lax.rem(i, NC)
        return pltpu.make_async_copy(src(i), buf.at[k], isem.at[k])

    def put(i):
        k = lax.rem(i, NC)
        return pltpu.make_async_copy(buf.at[k], dst(i), osem.at[k])

    for i in range(NC // 2):
        fetch(i).start()

    def body(i, _):
        fetch(i).wait()
        put(i).start()

        @pl.when(i >= NC // 2)
        def _():
            put(i - NC // 2).wait()

        @pl.when(i + NC // 2 < n)
        def _():
            fetch(i + NC // 2).start()

        return 0

    lax.fori_loop(0, n, body, 0)
    for i in range(n - NC // 2, n):
        put(i).wait()


def copy_call(kernel, out, block, args):
    return pl.pallas_call(
        kernel,
        out_shape=jax.ShapeDtypeStruct(out, F32),
        in_specs=[HBM] * len(args),
        out_specs=HBM,
        input_output_aliases={1: 0} if len(args) > 1 else {},
        scratch_shapes=[pltpu.VMEM((NC,) + block, F32), DMA((NC,)), DMA((NC,))],
        compiler_params=pltpu.CompilerParams(vmem_limit_bytes=62 * MIB),
        cost_estimate=pl.CostEstimate(flops=20_000_000_000, bytes_accessed=130_000_000, transcendentals=0),
    )(*args)


def land_blocks(first, sent, dwv):
    per = H // LANE

    def kernel(src, _, dst, *scratch):
        other = 1 - lax.rem(lax.axis_index("data"), 2)

        def rows(i):
            return pl.ds(pl.multiple_of(lax.rem(i, per) * LANE, LANE), LANE)

        def target(i):
            return dst.at[rows(i), pl.ds(pl.multiple_of(block_of(first + i // per, other) * VB, VB), VB)]

        copy_ring(sent.shape[0] * per, lambda i: src.at[i // per, rows(i)], target, *scratch)

    return copy_call(kernel, (H, V), (LANE, VB), (sent, dwv))


def place_dw(piece, parts, *before):
    row, step, rows = PIECES[piece]

    def kernel(src, *rest):
        dst, scratch = rest[-4], rest[-3:]

        def target(i):
            return dst.at[gray(lax.rem(i, S)), pl.ds(pl.multiple_of(row + i // S * step, R), rows)]

        copy_ring(parts.shape[0], lambda i: src.at[i, 0:rows], target, *scratch)

    return copy_call(kernel, (L, 2 * H, G4), (rows, G4), (parts,) + before)


SPLITS = (0, 2, 6, NOWN)


def solution(mesh):
    def local_grads(x_rows, tgt_rows, w_lstm, b_lstm, w_vocab):
        tgt = jnp.swapaxes(tgt_rows, 0, 1).reshape(N, 1)
        gates, cprev, hprev, xs, top = forward(jnp.swapaxes(x_rows, 0, 1), w_lstm, b_lstm)
        top = top.reshape(N, H)
        d_top, stats = head(top, tgt, w_vocab)
        x_all = lax.all_gather(top, 'data', axis=0, tiled=True)
        stats = lax.all_gather(stats, 'data', axis=0, tiled=True)
        d_top, x_all = lax.optimization_barrier((d_top, x_all))
        both, *owns, give1, give2, db, dx = backward(d_top.reshape(T, R, H), gates, cprev, hprev, xs, w_lstm)
        other_plane = [(i, (i + S) % NDEV) for i in range(NDEV)]
        other_core = [(i, i + 1 - 2 * (i % 2)) for i in range(NDEV)]
        planes = [list(range(S)), list(range(S, NDEV))]
        dwv, part, gathered, swapped = (), both, [], []
        for i, (own, give) in enumerate(((both, both), (owns[0], give1), (owns[1], give2))):
            if i:
                give, part = lax.optimization_barrier((give, part))
            got = lax.ppermute(give, 'data', other_plane)
            dwv, sent = grad_vocab(SPLITS[i], SPLITS[i + 1], x_all, stats, w_vocab, dwv, swapped[:1] if i == 2 else ())
            own, dwv = lax.optimization_barrier((own, dwv))
            part = own + got if i != 1 else jnp.concatenate([own + got, db], axis=0)
            part, dwv = lax.optimization_barrier((part, dwv))
            gathered.append(lax.all_gather(part, 'data', axis=0, axis_index_groups=None if i else planes))
            swapped.append((SPLITS[i], lax.ppermute(sent, 'data', other_core)))
            dwv = (dwv,)
        dw = place_dw(0, gathered[0])
        for first, sent in swapped[1:]:
            dwv = (land_blocks(first, sent, *dwv),)
        dw = place_dw(2, gathered[2], place_dw(1, gathered[1], dw))
        db = gathered[1][:, PIECES[1][2]:].reshape(NDEV // S, S, R, G4).sum(axis=(0, 2))
        db = jnp.stack([db[gray(i)] for i in range(L)])
        return dw, db, dwv[0], jnp.swapaxes(dx, 0, 1)

    return jax.shard_map(local_grads, mesh=mesh, in_specs=(P('data'), P('data'), P(), P(), P()), out_specs=(P(), P(), P(), P('data')), check_vma=False)
```

```python
import functools

import jax
import jax.numpy as jnp
from jax import lax
from jax.experimental import pallas as pl
from jax.experimental.pallas import tpu as pltpu
from jax.sharding import PartitionSpec as P

T = 48
R = 8
S = 8
Q = S * R
H = 512
HB = 256
G4 = 4 * H
L = 8
V = 32000
LANE = 128
NDEV = 16
CH = 4
NR = 6
PIECES = ((0, 0, 256), (256, 384, 352), (608, 384, 32))
F32 = jnp.float32
BF16 = jnp.bfloat16
MESH = pl.DeviceIdType.MESH
MIB = 1024 * 1024
ANY = pl.BlockSpec(memory_space=pl.ANY)
VMEM = pl.BlockSpec(memory_space=pltpu.VMEM)
HBM = pl.BlockSpec(memory_space=pltpu.HBM)
DMA = pltpu.SemaphoreType.DMA


def dot(a, b):
    return jnp.dot(a, b, preferred_element_type=F32)


def dot_tt(a, b):
    return lax.dot_general(a, b, (((1,), (1,)), ((), ())), preferred_element_type=F32)


def gray(k):
    chip, core = k // 2, k % 2
    hi, lo = chip // 2, chip % 2
    return 2 * (chip + hi - 2 * hi * lo) + core


LAST = gray(S - 1)


def place():
    me = lax.axis_index("data")
    index = lax.rem(me, S)
    return me - index, index, gray(index)


def plane_signal(base, index):
    barrier = pltpu.get_barrier_semaphore()
    for i in range(1, S):
        pl.semaphore_signal(barrier, inc=1, device_id=(base + lax.rem(index + i, S),), device_id_type=MESH)


def plane_wait():
    pl.semaphore_wait(pltpu.get_barrier_semaphore(), S - 1)


def rows_of(v):
    return v.reshape(Q, v.shape[-1])


def groups_of(v):
    return v.reshape(S, R, v.shape[-1])


def fwd_kernel(x_hbm, w_hbm, b_ref, gates_hbm, cp_hbm, hp_hbm, xs_hbm, xl_hbm,
               w, xbuf, xout, gates, cprev, hprev, wsem, insem, recv, send, lastsem, osem):
    base, index, stage = place()
    first, last = stage == 0, stage == S - 1
    nxt = base + gray(lax.rem(stage + 1, S))
    plane_signal(base, index)
    wcopy = pltpu.make_async_copy(w_hbm.at[stage], w, wsem.at[0])
    wcopy.start()
    plane_wait()

    def feed(k):
        ts = pl.ds(k * CH, CH)

        @pl.when(first)
        def _():
            pltpu.make_async_copy(x_hbm.at[ts], xbuf.at[ts, 0], recv.at[k * CH]).start()

        @pl.when(jnp.logical_not(first))
        def _():
            pltpu.make_async_remote_copy(x_hbm.at[ts], xbuf.at[ts, index], insem, recv.at[k * CH],
                                         device_id=(base,), device_id_type=MESH).start()

        return 0

    def step_out(t):
        return pltpu.make_async_remote_copy(xout.at[t], xbuf.at[t], send, recv.at[t], device_id=(nxt,), device_id_type=MESH)

    def final_out(t, i):
        ts = pl.ds(t, CH)
        if i == LAST:
            return pltpu.make_async_copy(xout.at[ts, i], xl_hbm.at[ts], lastsem)
        return pltpu.make_async_remote_copy(xout.at[ts, i], xl_hbm.at[ts], send, lastsem, device_id=(base + i,), device_id_type=MESH)

    def arrived(t):
        @pl.when(jnp.logical_not(first))
        def _():
            step_out(t).wait_recv()

        @pl.when(first & (lax.rem(t, CH) == 0))
        def _():
            ts = pl.ds(t, CH)
            pltpu.make_async_remote_copy(xout.at[ts], xbuf.at[ts], send, recv.at[t], device_id=(nxt,), device_id_type=MESH).wait_recv()

    def pass_on(t):
        @pl.when(jnp.logical_not(last))
        def _():
            step_out(t).start()

        @pl.when(last & (lax.rem(t, CH) == CH - 1))
        def _():
            for i in range(S):
                final_out(t - CH + 1, i).start()

    lax.fori_loop(0, T // CH, lambda k, _: feed(k), 0)
    bias = b_ref[pl.ds(stage, 1), :]

    wcopy.wait()

    kept = ((gates, gates_hbm), (cprev, cp_hbm), (hprev, hp_hbm), (xbuf, xs_hbm))

    def save(t):
        for i, (src, dst) in enumerate(kept):
            pltpu.make_async_copy(src.at[t], dst.at[t], osem.at[i]).start()

    def two(p, state):
        for u in range(2):
            t = 2 * p + u

            @pl.when(t > 0)
            def _():
                pass_on(t - 1)
                save(t - 1)

            arrived(t)
            ha, hc, ca, cc = state
            xt = rows_of(xbuf[t].astype(F32))
            xlow = xt.astype(BF16)
            hlow = jnp.concatenate([ha, hc], axis=1).astype(BF16)
            hprev[t] = hlow
            cprev[t, :, 0:HB] = ca
            cprev[t, :, HB:H] = cc
            nh, nc = [], []
            for q in range(2):
                zz = []
                for g in range(4):
                    cols = slice(g * H + q * HB, g * H + q * HB + HB)
                    zz.append(dot(xlow, w[0:H, cols]) + dot(hlow, w[H:2 * H, cols]) + bias[:, cols])
                gi, gf, gg, go = jax.nn.sigmoid(zz[0]), jax.nn.sigmoid(zz[1]), jnp.tanh(zz[2]), jax.nn.sigmoid(zz[3])
                cn = gf * (ca, cc)[q] + gi * gg
                nh.append(go * jnp.tanh(cn))
                nc.append(cn)
                for g, val in enumerate((gi, gf, gg, go)):
                    gates[t, :, g * H + q * HB:g * H + q * HB + HB] = val
            xout[t] = groups_of(xt + jnp.concatenate(nh, axis=1)).astype(BF16)
            state = (nh[0], nh[1], nc[0], nc[1])
        return state

    zero = jnp.zeros((Q, HB), F32)
    lax.fori_loop(0, T // 2, two, (zero,) * 4)
    pass_on(jnp.int32(T - 1))
    save(T - 1)
    for i, (src, dst) in enumerate(kept):
        pltpu.make_async_copy(src, dst, osem.at[i]).wait()

    @pl.when(jnp.logical_not(first))
    def _():
        pltpu.make_async_remote_copy(x_hbm, xl_hbm, insem, lastsem, device_id=(base,), device_id_type=MESH).wait_send()

    @pl.when(jnp.logical_not(last))
    def _():
        pltpu.make_async_remote_copy(xout, xbuf, send, recv.at[0], device_id=(nxt,), device_id_type=MESH).wait_send()

    @pl.when(last)
    def _():
        others = (slice(None), slice(0, S - 1))
        pltpu.make_async_remote_copy(xout.at[others], xbuf.at[others], send, recv.at[0], device_id=(nxt,), device_id_type=MESH).wait_send()

    pltpu.make_async_copy(x_hbm, xl_hbm, lastsem).wait()


def forward(x, w, b):
    return pl.pallas_call(
        fwd_kernel,
        out_shape=(jax.ShapeDtypeStruct((T, Q, G4), F32), jax.ShapeDtypeStruct((T, Q, H), F32),
                   jax.ShapeDtypeStruct((T, Q, H), BF16), jax.ShapeDtypeStruct((T, S, R, H), BF16),
                   jax.ShapeDtypeStruct((T, R, H), BF16)),
        in_specs=[ANY, ANY, VMEM],
        out_specs=(HBM,) * 5,
        scratch_shapes=[pltpu.VMEM((2 * H, G4), BF16), pltpu.VMEM((T, S, R, H), BF16), pltpu.VMEM((T, S, R, H), BF16),
                        pltpu.VMEM((T, Q, G4), F32), pltpu.VMEM((T, Q, H), F32), pltpu.VMEM((T, Q, H), BF16)]
        + [DMA((1,)), DMA, DMA((T,)), DMA, DMA, DMA((4,))],
        compiler_params=pltpu.CompilerParams(vmem_limit_bytes=52 * MIB, collective_id=0, has_side_effects=True),
        cost_estimate=pl.CostEstimate(flops=60_000_000_000, bytes_accessed=80_000_000, transcendentals=0),
        name="lstm_fwd",
    )(x, w, b)


def bwd_kernel(d_hbm, gates_hbm, cp_hbm, hp_hbm, xs_hbm, w_hbm, both, own1, own2, give1, give2, db_ref, dx_hbm,
               w, wt, dbuf, dout, dall, ut, acc, gin, cin, hin, xin,
               wsem, insem, recv, send, lastsem, isem, osem):
    base, index, stage = place()
    plane = base // S
    first, last = stage == 0, stage == S - 1
    prv = base + gray(lax.rem(stage + S - 1, S))
    top = base + LAST
    plane_signal(base, index)
    wcopy = pltpu.make_async_copy(w_hbm.at[stage], w, wsem.at[0])
    wcopy.start()

    def feed(k):
        t = T - CH - k * CH
        ts = pl.ds(t, CH)

        @pl.when(last)
        def _():
            pltpu.make_async_copy(d_hbm.at[ts], dbuf.at[ts, LAST], recv.at[t]).start()

        @pl.when(jnp.logical_not(last))
        def _():
            pltpu.make_async_remote_copy(d_hbm.at[ts], dbuf.at[ts, index], insem, recv.at[t],
                                         device_id=(top,), device_id_type=MESH).start()

        return 0

    def step_out(t):
        return pltpu.make_async_remote_copy(dout.at[t], dbuf.at[t], send, recv.at[t], device_id=(prv,), device_id_type=MESH)

    def final_out(t, i):
        ts = pl.ds(t, CH)
        if i == 0:
            return pltpu.make_async_copy(dout.at[ts, i], dx_hbm.at[ts], lastsem)
        return pltpu.make_async_remote_copy(dout.at[ts, i], dx_hbm.at[ts], send, lastsem, device_id=(base + i,), device_id_type=MESH)

    def arrived(t):
        @pl.when(jnp.logical_not(last))
        def _():
            step_out(t).wait_recv()

        @pl.when(last & (lax.rem(t, CH) == CH - 1))
        def _():
            ts = pl.ds(t - CH + 1, CH)
            pltpu.make_async_remote_copy(dout.at[ts], dbuf.at[ts], send, recv.at[t - CH + 1], device_id=(prv,), device_id_type=MESH).wait_recv()

    def pass_on(t):
        @pl.when(jnp.logical_not(first))
        def _():
            step_out(t).start()

        @pl.when(first & (lax.rem(t, CH) == 0))
        def _():
            for i in range(S):
                final_out(t, i).start()

    def loads(t):
        k = lax.rem(t, NR)
        return [pltpu.make_async_copy(src.at[t], dst.at[k], isem.at[k, i])
                for i, (src, dst) in enumerate(((gates_hbm, gin), (cp_hbm, cin), (hp_hbm, hin), (xs_hbm, xin)))]

    for t in range(T - NR, T):
        for cp in loads(t):
            cp.start()
    plane_wait()
    lax.fori_loop(0, T // CH, lambda k, _: feed(k), 0)
    db_ref[...] = jnp.zeros(db_ref.shape, F32)
    acc[...] = jnp.zeros(acc.shape, F32)
    wcopy.wait()

    def turn(n, _):
        cols = pl.ds(pl.multiple_of(n * HB, HB), HB)
        wt[cols, :] = w[:, cols].T
        return 0

    lax.fori_loop(0, G4 // HB, turn, 0)

    def weight():
        for n in range(0, G4, HB):
            acc[:, n:n + HB] += dot(ut[...], dall[:, n:n + HB])

    def two(n, state):
        p = T // 2 - 1 - n
        us = []
        for u in (1, 0):
            t = 2 * p + u
            k = lax.rem(t, NR)
            for cp in loads(t):
                cp.wait()

            @pl.when(t < T - 1)
            def _():
                pass_on(t + 1)

            if u == 1:
                @pl.when((p < T // 2 - 1) & (lax.rem(p, CH // 2) == CH // 2 - 1))
                def _():
                    weight()

            arrived(t)
            ea, ec, da, dc_ = state
            dext = rows_of(dbuf[t])
            parts = [[None, None] for _ in range(4)]
            nd = []
            for q in range(2):
                gi, gf, gg, go = (gin[k, :, g * H + q * HB:g * H + q * HB + HB] for g in range(4))
                hq = slice(q * HB, q * HB + HB)
                cprev = cin[k, :, hq]
                th = jnp.tanh(gf * cprev + gi * gg)
                e = dext[:, hq] + (ea, ec)[q]
                dc = (da, dc_)[q] + e * (go * (1.0 - th * th))
                parts[0][q] = dc * (gg * gi * (1.0 - gi))
                parts[1][q] = dc * (cprev * gf * (1.0 - gf))
                parts[2][q] = dc * (gi * (1.0 - gg * gg))
                parts[3][q] = e * (th * go * (1.0 - go))
                nd.append(dc * gf)
            trows = pl.ds(pl.multiple_of(lax.rem(t, CH) * Q, Q), Q)
            lows = []
            for i, v in enumerate(v for ps in parts for v in ps):
                cols = slice(i * HB, i * HB + HB)
                low = v.astype(BF16)
                dall[trows, cols] = low
                lows.append(low)
                db_ref[:, cols] += jnp.sum(v.reshape(Q // R, R, HB), axis=0)
            lowz = jnp.concatenate(lows, axis=1)
            ne = [dot(lowz, wt[:, H + q * HB:H + q * HB + HB]) for q in range(2)]
            for q in range(2):
                hq = slice(q * HB, q * HB + HB)
                dout[t, :, :, hq] = groups_of(dext[:, hq] + dot(lowz, wt[:, hq]))
            state = (ne[0], ne[1], nd[0], nd[1])
            us.append((rows_of(xin[k].astype(F32)).astype(BF16), hin[k]))

            @pl.when(t >= NR)
            def _():
                for cp in loads(t - NR):
                    cp.start()

        tcols = pl.ds(pl.multiple_of(lax.rem(p, CH // 2) * 2 * Q, 2 * Q), 2 * Q)
        for j in range(2):
            ut[j * H:j * H + H, tcols] = jnp.concatenate([us[1][j], us[0][j]], axis=0).T

        return state

    zero = jnp.zeros((Q, HB), F32)
    lax.fori_loop(0, T // 2, two, (zero,) * 4)
    pass_on(jnp.int32(0))

    weight()
    outs = []
    for i, (dst, (row, step, rows), at) in enumerate(((both, PIECES[0], 0), (give1, PIECES[1], 1 - plane), (give2, PIECES[2], 1 - plane),
                                                      (own1, PIECES[1], plane), (own2, PIECES[2], plane))):
        outs.append(pltpu.make_async_copy(acc.at[pl.ds(pl.multiple_of(row + at * step, R), rows)], dst, osem.at[i]))
        outs[i].start()
    for out in outs:
        out.wait()

    @pl.when(jnp.logical_not(last))
    def _():
        pltpu.make_async_remote_copy(d_hbm, dx_hbm, insem, lastsem, device_id=(top,), device_id_type=MESH).wait_send()

    @pl.when(jnp.logical_not(first))
    def _():
        pltpu.make_async_remote_copy(dout, dbuf, send, recv.at[0], device_id=(prv,), device_id_type=MESH).wait_send()

    @pl.when(first)
    def _():
        others = (slice(None), slice(1, S))
        pltpu.make_async_remote_copy(dout.at[others], dbuf.at[others], send, recv.at[0], device_id=(prv,), device_id_type=MESH).wait_send()

    pltpu.make_async_copy(d_hbm, dx_hbm, lastsem).wait()


def backward(d_top, gates, cprev, hprev, xs, w):
    return pl.pallas_call(
        bwd_kernel,
        out_shape=tuple(jax.ShapeDtypeStruct((rows, G4), F32) for _, _, rows in PIECES + PIECES[1:]) + (jax.ShapeDtypeStruct((R, G4), F32), jax.ShapeDtypeStruct((T, R, H), F32)),
        in_specs=[ANY] * 6,
        out_specs=(HBM,) * 5 + (VMEM, HBM),
        scratch_shapes=[pltpu.VMEM((2 * H, G4), BF16), pltpu.VMEM((G4, 2 * H), BF16), pltpu.VMEM((T, S, R, H), F32),
                        pltpu.VMEM((T, S, R, H), F32), pltpu.VMEM((CH * Q, G4), BF16), pltpu.VMEM((2 * H, CH * Q), BF16), pltpu.VMEM((2 * H, G4), F32)]
        + [pltpu.VMEM((NR, Q, G4), F32), pltpu.VMEM((NR, Q, H), F32), pltpu.VMEM((NR, Q, H), BF16), pltpu.VMEM((NR, S, R, H), BF16)]
        + [DMA((1,)), DMA, DMA((T,)), DMA, DMA, DMA((NR, 4)), DMA((5,))],
        compiler_params=pltpu.CompilerParams(vmem_limit_bytes=56 * MIB, collective_id=1, has_side_effects=True),
        cost_estimate=pl.CostEstimate(flops=110_000_000_000, bytes_accessed=80_000_000, transcendentals=0),
        name="lstm_bwd",
    )(d_top, gates, cprev, hprev, xs, w)


VB = 1280
NVB = V // VB
N = T * R
CHUNKS = ((0, 512), (512, 512), (1024, 256))
NW = 4
RB = 64


def head_kernel(x_ref, t_ref, w_hbm, dx_ref, stats_ref, lg, g0, g1, wv, mx, sm, tb, wsem):
    def wcopy(b):
        buf = lax.rem(b, NW)
        return pltpu.make_async_copy(w_hbm.at[:, pl.ds(pl.multiple_of(lax.rem(b, NVB) * VB, VB), VB)], wv.at[buf], wsem.at[buf])

    for b in range(NW - 1):
        wcopy(b).start()

    def ready(b):
        for i in range(2):
            wcopy(b + i).wait()
            wcopy(b + i + 2).start()

    mx[...] = jnp.full(mx.shape, -jnp.inf, F32)
    sm[...] = jnp.zeros(sm.shape, F32)
    dx_ref[...] = jnp.zeros(dx_ref.shape, F32)

    def logits(b, c, size):
        part = dot(x_ref[...], wv[lax.rem(b, NW), :, c:c + size])
        lg[b, :, c:c + size] = part
        for r in range(0, N, RB):
            rows = slice(r, r + RB)
            vals = [part[rows, h:h + LANE] for h in range(0, size, LANE)]
            m_old = mx[rows, :]
            m_new = functools.reduce(jnp.maximum, vals, m_old)
            mx[rows, :] = m_new
            sm[rows, :] = functools.reduce(jnp.add, [jnp.exp(v - m_new) for v in vals], sm[rows, :] * jnp.exp(m_old - m_new))

    def block(b):
        for c, size in CHUNKS:
            logits(b, c, size)

    wcopy(0).wait()
    block(0)

    def first(h, _):
        b = 2 * h + 1
        ready(b)
        for i in range(2):
            block(b + i)
        return 0

    lax.fori_loop(0, NVB // 2, first, 0)

    def finish(r):
        rows = slice(r, r + LANE)
        top = jnp.max(mx[rows, :], axis=1, keepdims=True)
        tot = jnp.sum(sm[rows, :] * jnp.exp(mx[rows, :] - top), axis=1, keepdims=True)
        lse = top + jnp.log(tot)
        mx[rows, :] = jnp.broadcast_to(lse, (LANE, LANE))
        tb[rows, :] = jnp.broadcast_to(t_ref[rows, :], (LANE, LANE))

    lane = lax.broadcasted_iota(jnp.int32, (LANE, LANE), 1)
    stats = jnp.zeros((LANE, LANE), F32)
    for j in range(N // LANE):
        finish(j * LANE)
        rows = slice(j * LANE, j * LANE + LANE)
        stats = jnp.where(lane == j, mx[rows, :], jnp.where(lane == LANE - 1 - j, tb[rows, :].astype(F32), stats))
    stats_ref[...] = stats

    def grads(b, gb, c):
        ids = [b * VB + c + h + lax.broadcasted_iota(jnp.int32, (RB, LANE), 1) for h in (0, LANE)]
        for r in range(0, N, RB):
            rows = slice(r, r + RB)
            lse = mx[rows, :]
            for h in (0, LANE):
                cols = pl.ds(c + h, LANE)
                p = jnp.exp(lg[b, rows, cols] - lse)
                gb[rows, cols] = jnp.where(tb[rows, :] == ids[h // LANE], p - 1.0, p).astype(BF16)

    def apply(b, gb, cols):
        return dot_tt(gb[:, cols], wv[lax.rem(b + NVB, NW), :, cols])

    for c in range(0, VB, HB):
        grads(0, g0, c)

    def second(h, _):
        for i in range(2):
            b = 2 * h + NVB + i
            wcopy(b).wait()

            @pl.when(b + 2 < 2 * NVB)
            def _():
                wcopy(b + 2).start()

        for b, gb, gn in ((2 * h, g0, g1), (2 * h + 1, g1, g0)):
            total = jnp.zeros((N, H), F32)
            for c in range(0, VB, HB):
                total = total + apply(b, gb, slice(c, c + HB))
                grads(b + 1, gn, c)
            dx_ref[...] += total
        return 0

    lax.fori_loop(0, NVB // 2, second, 0)
    wcopy(2 * NVB - 1).wait()
    for c in range(0, VB, HB):
        dx_ref[...] += apply(NVB - 1, g0, slice(c, c + HB))


def head(x, tgt, w_vocab):
    return pl.pallas_call(
        head_kernel,
        out_shape=(jax.ShapeDtypeStruct((N, H), F32), jax.ShapeDtypeStruct((LANE, LANE), F32)),
        in_specs=[VMEM, VMEM, ANY],
        out_specs=(VMEM, VMEM),
        scratch_shapes=[pltpu.VMEM((NVB, N, VB), F32), pltpu.VMEM((N, VB), BF16), pltpu.VMEM((N, VB), BF16), pltpu.VMEM((NW, H, VB), BF16),
                        pltpu.VMEM((N, LANE), F32), pltpu.VMEM((N, LANE), F32), pltpu.VMEM((N, LANE), jnp.int32), DMA((NW,))],
        compiler_params=pltpu.CompilerParams(vmem_limit_bytes=60 * MIB),
        cost_estimate=pl.CostEstimate(flops=40_000_000_000, bytes_accessed=70_000_000, transcendentals=0),
        name="head",
    )(x, tgt, w_vocab)


TB = 768
NTOK = NDEV * N
NK = NTOK // TB
UN = 2
NOWN = (NVB + 1) // 2


def block_of(j, side):
    return j + side * (NVB - 1 - 2 * j)


def dwv_kernel(lo, hi, came, x_hbm, st_ref, w_hbm, *rest):
    nshared = min(hi, NOWN - 1) - lo
    arrived = rest[len(rest) - 15 - 1 - (nshared > 0) - len(came):]
    dw_hbm = arrived[len(came)]
    give_hbm = arrived[len(came) + 1]
    xv, xtv, wv, g0, g1, acc, lse, tgt, box, wsem, xsem, osem, gsem, isem, psem = rest[-15:]
    core = lax.rem(lax.axis_index("data"), 2)

    def cols(b):
        return pl.ds(pl.multiple_of(b * VB, VB), VB)

    def wcopy(i):
        buf = lax.rem(i, 2)
        return pltpu.make_async_copy(w_hbm.at[:, cols(block_of(lo + i, core))], wv.at[buf], wsem.at[buf])

    def keep(i):
        buf = lax.rem(i, 2)
        return pltpu.make_async_copy(acc.at[buf], dw_hbm.at[:, cols(block_of(lo + i, core))], osem.at[buf])

    def give(i):
        buf = lax.rem(i, 2)
        return pltpu.make_async_copy(acc.at[buf], give_hbm.at[i], gsem.at[buf])

    def done(i):
        keep(i).start()

        @pl.when(i < nshared)
        def _():
            give(i).start()

    def drained(i):
        keep(i).wait()

        @pl.when(i < nshared)
        def _():
            give(i).wait()

    pieces = [(src, first, i, r) for src, (first, count) in zip(arrived, came) for i in range(count) for r in range(0, H, LANE)]
    per = -(-len(pieces) // ((hi - lo) * NK // UN))

    def fetch(src, i, r, k, slot):
        return pltpu.make_async_copy(src.at[i, pl.ds(r, LANE)], box.at[k, slot], isem.at[k, slot])

    def put(first, i, r, k, slot):
        return pltpu.make_async_copy(box.at[k, slot], dw_hbm.at[pl.ds(r, LANE), cols(block_of(first + i, 1 - core))], psem.at[k, slot])

    def pieces_of(h, act):
        at = 0
        for src, (first, count) in zip(arrived, came):
            total = count * H // LANE
            for slot in range(per):
                c = h * per + slot - at
                i, r = c // (H // LANE), pl.multiple_of(lax.rem(c, H // LANE) * LANE, LANE)

                @pl.when((c >= 0) & (c < total))
                def _():
                    act(src, first, i, r, lax.rem(h, 2), slot)

            at += total

    def land(src, first, i, r, k, slot):
        fetch(src, i, r, k, slot).wait()
        put(first, i, r, k, slot).start()

    def move(h):
        if came:
            pieces_of(h, land)
            pieces_of(h - 1 + 2 * (h == 0) * len(pieces), lambda src, first, i, r, k, slot: put(first, i, r, k, slot).wait())
            pieces_of(h + 1, lambda src, first, i, r, k, slot: fetch(src, i, r, k, slot).start())

    n = hi - lo
    wcopy(0).start()

    def xcopy(k):
        rows = pl.ds(k * TB, TB)
        return pltpu.make_async_copy(x_hbm.at[rows], xv.at[rows], xsem.at[k])

    for k in range(NK):
        xcopy(k).start()

    def turn(k, _):
        xcopy(k).wait()
        for c in range(0, TB, HB):
            rows = pl.ds(pl.multiple_of(k * TB + c, HB), HB)
            xtv[k, :, c:c + HB] = xv[rows, :].T
        for c in range(0, TB, LANE):
            j = c % N // LANE
            held = pl.ds(pl.multiple_of((k * (TB // N) + c // N) * LANE, LANE), LANE)
            rows = pl.ds(pl.multiple_of(k * TB + c, LANE), LANE)
            lse[rows, :] = jnp.broadcast_to(st_ref[held, j:j + 1], (LANE, LANE))
            tgt[rows, :] = jnp.broadcast_to(st_ref[held, LANE - 1 - j:LANE - j], (LANE, LANE))
        return 0

    lax.fori_loop(0, NK, turn, 0)
    if came:
        pieces_of(jnp.int32(0), lambda src, first, i, r, k, slot: fetch(src, i, r, k, slot).start())

    def weight(it, gold, cols, reset=False):
        k, i = lax.rem(it + NK, NK), jnp.maximum(it, 0) // NK
        acc_c = acc.at[lax.rem(i, 2), :, cols]
        old = acc_c[...]
        acc_c[...] = (jnp.where(k == 0, 0.0, old) if reset else old) + dot(xtv[k], gold[:, cols])

    def step(it, u):
        gnew, gold = ((g0, g1), (g1, g0))[u % 2]
        k, i = lax.rem(it, NK) + u, it // NK
        base = pl.multiple_of(k * TB, TB)
        lane = lax.broadcasted_iota(jnp.int32, (R, LANE), 1) + block_of(lo + i, core) * VB
        for c in range(0, VB, HB):
            lgt = dot(xv[pl.ds(base, TB), :], wv[lax.rem(i, 2), :, c:c + HB])
            weight(it + u - 1, gold, slice(c, c + HB), u == 1)
            ids = [jnp.tile((lane + (c + h)).astype(F32), (RB // R, 1)) for h in (0, LANE)]
            for r in range(0, TB, RB):
                here = pl.ds(pl.multiple_of(base + r, RB), RB)
                for h in (0, LANE):
                    p = jnp.exp(lgt[r:r + RB, h:h + LANE] - lse[here, :])
                    gnew[r:r + RB, c + h:c + h + LANE] = jnp.where(tgt[here, :] == ids[h // LANE], p - 1.0, p).astype(BF16)

    def body(h, _):
        it = UN * h
        i0, k0 = it // NK, lax.rem(it, NK)
        move(h)

        @pl.when(k0 == 0)
        def _():
            wcopy(i0).wait()

            @pl.when(i0 < n - 1)
            def _():
                wcopy(i0 + 1).start()

        @pl.when((k0 == 0) & (i0 >= 2))
        def _():
            drained(i0 - 2)

        for u in range(UN):
            step(it, u)

        @pl.when((k0 == UN) & (i0 >= 1))
        def _():
            done(i0 - 1)

        return 0

    lax.fori_loop(0, n * NK // UN, body, 0)

    def last(c, _):
        weight(jnp.int32(n * NK - 1), g1, pl.ds(pl.multiple_of(c * HB, HB), HB))
        return 0

    lax.fori_loop(0, VB // HB, last, 0)
    if n > 1:
        drained(n - 2)
    done(n - 1)
    if came:
        pieces_of(jnp.int32(n * NK // UN - 1), lambda src, first, i, r, k, slot: put(first, i, r, k, slot).wait())
    drained(n - 1)


def grad_vocab(lo, hi, x_all, stats, w_vocab, before=(), came=()):
    counts = tuple((first, v.shape[0]) for first, v in came)
    nshared = min(hi, NOWN - 1) - lo
    out = (jax.ShapeDtypeStruct((H, V), F32), jax.ShapeDtypeStruct((nshared, H, VB), F32))[:1 + (nshared > 0)]
    per = max(1, -(-sum(c for _, c in counts) * (H // LANE) // ((hi - lo) * NK // UN)))
    return pl.pallas_call(
        functools.partial(dwv_kernel, lo, hi, counts),
        out_shape=out,
        in_specs=[ANY, VMEM, ANY] + [HBM] * (len(before) + len(came)),
        out_specs=(HBM,) * len(out),
        input_output_aliases={3: 0} if before else {},
        scratch_shapes=[pltpu.VMEM((NTOK, H), BF16), pltpu.VMEM((NK, H, TB), BF16), pltpu.VMEM((2, H, VB), BF16)]
        + [pltpu.VMEM((TB, VB), BF16)] * 2
        + [pltpu.VMEM((2, H, VB), F32)] + [pltpu.VMEM((NTOK, LANE), F32)] * 2 + [pltpu.VMEM((2, per, LANE, VB), F32)]
        + [DMA((2,)), DMA((NK,)), DMA((2,)), DMA((2,)), DMA((2, per)), DMA((2, per))],
        compiler_params=pltpu.CompilerParams(vmem_limit_bytes=62 * MIB),
        cost_estimate=pl.CostEstimate(flops=(hi - lo) * 20_000_000_000, bytes_accessed=100_000_000, transcendentals=0),
        name="dwv",
    )(x_all, stats, w_vocab, *before, *(v for _, v in came))


RING = 24 * MIB


def copy_ring(n, src, dst, buf, isem, osem):
    nbuf = buf.shape[0]
    ahead = nbuf // 2

    def fetch(i):
        k = lax.rem(i, nbuf)
        return pltpu.make_async_copy(src(i), buf.at[k], isem.at[k])

    def put(i):
        k = lax.rem(i, nbuf)
        return pltpu.make_async_copy(buf.at[k], dst(i), osem.at[k])

    for i in range(min(ahead, n)):
        fetch(i).start()

    def body(i, _):
        fetch(i).wait()
        put(i).start()

        @pl.when(i >= ahead)
        def _():
            put(i - ahead).wait()

        @pl.when(i + ahead < n)
        def _():
            fetch(i + ahead).start()

        return 0

    lax.fori_loop(0, n, body, 0)
    for i in range(max(n - ahead, 0), n):
        put(i).wait()


def copy_call(kernel, out, block, args):
    nbuf = min(RING // (block[0] * block[1] * 4), 2 * NDEV)
    return pl.pallas_call(
        kernel,
        out_shape=jax.ShapeDtypeStruct(out, F32),
        in_specs=[HBM] * len(args),
        out_specs=HBM,
        input_output_aliases={1: 0} if len(args) > 1 else {},
        scratch_shapes=[pltpu.VMEM((nbuf,) + block, F32), DMA((nbuf,)), DMA((nbuf,))],
        compiler_params=pltpu.CompilerParams(vmem_limit_bytes=62 * MIB),
        cost_estimate=pl.CostEstimate(flops=20_000_000_000, bytes_accessed=130_000_000, transcendentals=0),
    )(*args)


def land_blocks(first, sent, dwv):
    per = H // LANE

    def kernel(src, _, dst, *scratch):
        other = 1 - lax.rem(lax.axis_index("data"), 2)

        def rows(i):
            return pl.ds(pl.multiple_of(lax.rem(i, per) * LANE, LANE), LANE)

        def target(i):
            return dst.at[rows(i), pl.ds(pl.multiple_of(block_of(first + i // per, other) * VB, VB), VB)]

        copy_ring(sent.shape[0] * per, lambda i: src.at[i // per, rows(i)], target, *scratch)

    return copy_call(kernel, (H, V), (LANE, VB), (sent, dwv))


def place_dw(piece, parts, *before):
    row, step, rows = PIECES[piece]

    def kernel(src, *rest):
        dst, scratch = rest[-4], rest[-3:]

        def target(i):
            return dst.at[gray(lax.rem(i, S)), pl.ds(pl.multiple_of(row + i // S * step, R), rows)]

        copy_ring(parts.shape[0], lambda i: src.at[i, 0:rows], target, *scratch)

    return copy_call(kernel, (L, 2 * H, G4), (rows, G4), (parts,) + before)


SPLITS = (0, 2, 6, NOWN)


def solution(mesh):
    def local_grads(x_rows, tgt_rows, w_lstm, b_lstm, w_vocab):
        tgt = jnp.swapaxes(tgt_rows, 0, 1).reshape(N, 1)
        gates, cprev, hprev, xs, top = forward(jnp.swapaxes(x_rows, 0, 1), w_lstm, b_lstm)
        top = top.reshape(N, H)
        d_top, stats = head(top, tgt, w_vocab)
        x_all = lax.all_gather(top, 'data', axis=0, tiled=True)
        stats = lax.all_gather(stats, 'data', axis=0, tiled=True)
        d_top, x_all = lax.optimization_barrier((d_top, x_all))
        both, *owns, give1, give2, db, dx = backward(d_top.reshape(T, R, H), gates, cprev, hprev, xs, w_lstm)
        other_plane = [(i, (i + S) % NDEV) for i in range(NDEV)]
        other_core = [(i, i + 1 - 2 * (i % 2)) for i in range(NDEV)]
        planes = [list(range(S)), list(range(S, NDEV))]
        dwv, part, gathered, swapped = (), both, [], []
        for i, (own, give) in enumerate(((both, both), (owns[0], give1), (owns[1], give2))):
            if i:
                give, part = lax.optimization_barrier((give, part))
            got = lax.ppermute(give, 'data', other_plane)
            dwv, sent = grad_vocab(SPLITS[i], SPLITS[i + 1], x_all, stats, w_vocab, dwv, swapped[:1] if i == 2 else ())
            own, dwv = lax.optimization_barrier((own, dwv))
            part = own + got if i != 1 else jnp.concatenate([own + got, db], axis=0)
            part, dwv = lax.optimization_barrier((part, dwv))
            gathered.append(lax.all_gather(part, 'data', axis=0, axis_index_groups=None if i else planes))
            swapped.append((SPLITS[i], lax.ppermute(sent, 'data', other_core)))
            dwv = (dwv,)
        dw = place_dw(0, gathered[0])
        for first, sent in swapped[1:]:
            dwv = (land_blocks(first, sent, *dwv),)
        dw = place_dw(2, gathered[2], place_dw(1, gathered[1], dw))
        db = gathered[1][:, PIECES[1][2]:].reshape(NDEV // S, S, R, G4).sum(axis=(0, 2))
        db = jnp.stack([db[gray(i)] for i in range(L)])
        return dw, db, dwv[0], jnp.swapaxes(dx, 0, 1)

    return jax.shard_map(local_grads, mesh=mesh, in_specs=(P('data'), P('data'), P(), P(), P()), out_specs=(P(), P(), P(), P('data')), check_vma=False)
```
